32 devices in a mesh: cells: 16 (over z, y, x), faces: 2 (over core).
Axes of the slice: x: 2, y: 2, z: 4, core: 2. Of those that a mesh axis runs over, the one named last changes fastest.
Arguments:
- flow_state: float32 [4, 131072], P(None, 'cells'), may hold values from -6 to 6
- source_term: float32 [4, 131072], P(None, 'cells'), may hold values from -24 to 24
- volume_rate: float32 [131072], P('cells'), may hold values from 0.5 to 4
- face_normal: float32 [3, 393216], P(None, ('cells', 'faces')), may hold values from -3 to 3
- face_owner: int32 [393216], P(('cells', 'faces')), may hold values from 0 to 8191, as said below
- face_neighbour: int32 [393216], P(('cells', 'faces')), may hold values from 0 to 9727, as said below
- face_count: int32 [32], P(('cells', 'faces')), may hold values from 1536 to 12288, as said below
- send_list: int32 [96, 256], P('cells'), may hold values from 0 to 8191
- halo_count: int32 [96], P('cells'), may hold values from 64 to 256, as said below
Outputs:
- solution_field: float32 [4, 131072], P(None, 'cells')
- residual: float32 [4, 131072], P(None, 'cells')
The draws below stay inside these ranges and needn't reach their ends.
Inputs may be any that keep to these rules, and one draw needn't show every extreme that they name: `face_owner`: A local cell of the slot's partition; with s = g mod 12288 and t = s // 192, it lies in 128 * t to 128 * t + 127. `face_neighbour`: with s and t as for face_owner: below 8192 a local cell (128 * t + d) mod 8192 with d in 0 to 255; otherwise 8192 plus a halo slot of the slot's partition in (t mod (6)) * 256 to that plus 256 - 1. Live slots of a block are its first face_count slots; in every draw some block has all 12288 slots live. `send_list`: entries at or past the list's count are unused. `halo_count`: every partition has one list with exactly 256 entries.
All inputs are finite; a program needn't handle non-finite values.
Results may differ from the reference program's by a relative error of at most 0.0003.
Values sent between devices are 32-bit elements; how exact they have to be, the bound alone decides.
No kernel may reach another device: no remote copies, remote signals or barrier semaphores. Data moves between devices by JAX's collectives and lax.ppermute only.
A program may use at most 64 MiB of HBM per device.

```python
import math
import jax
import jax.numpy as jnp
from jax import lax

CELLS_DEV = 8192
HALO = 256
NEIGH = 3
ITERS = 2
BLOCK = 4
TILES = 64
HWIN = 256
PARTITIONS = 16
SPLIT = 2
GROUPS = 32
FACE_SLOTS = 12288
CELLS = 131072
FACES = 393216


def draw_face_count(key, part):
    drawn_counts = jax.random.randint(key, (GROUPS,), FACE_SLOTS // 8, FACE_SLOTS + 1)
    chosen = jax.random.randint(jax.random.fold_in(key, 7), (), 0, GROUPS)
    return jnp.where(jnp.arange(GROUPS) == chosen, FACE_SLOTS, drawn_counts).astype(jnp.int32)


def draw_halo_count(key, part):
    list_total = 2 * NEIGH
    drawn_counts = jax.random.randint(key, (PARTITIONS, list_total), HALO // 4, HALO + 1)
    chosen = jax.random.randint(jax.random.fold_in(key, 11), (PARTITIONS, 1), 0, list_total)
    filled = jnp.where(jnp.arange(list_total)[None, :] == chosen, HALO, drawn_counts)
    return filled.reshape(PARTITIONS * list_total).astype(jnp.int32)


def tile_of_slot():
    slot_ids = jnp.arange(FACES, dtype=jnp.int32) % FACE_SLOTS
    return slot_ids // (FACE_SLOTS // TILES)


def draw_face_owner(key, part):
    tile_ids = tile_of_slot()
    offset = jax.random.randint(jax.random.fold_in(key, 21), (FACES,), 0, 128)
    return (tile_ids * 128 + offset).astype(jnp.int32)


def draw_face_neighbour(key, part):
    tile_ids = tile_of_slot()
    window_count = 2 * NEIGH * HALO // HWIN
    local_offset = jax.random.randint(jax.random.fold_in(key, 31), (FACES,), 0, 256)
    local_cell = (tile_ids * 128 + local_offset) % CELLS_DEV
    halo_offset = jax.random.randint(jax.random.fold_in(key, 37), (FACES,), 0, HWIN)
    halo_cell = CELLS_DEV + tile_ids % window_count * HWIN + halo_offset
    pick = jax.random.randint(jax.random.fold_in(key, 41), (FACES,), 0, 10)
    return jnp.where(pick < 3, halo_cell, local_cell).astype(jnp.int32)


def with_ends(values, key, least, high):
    place = [jax.random.randint(jax.random.fold_in(key, axis), (), 0, length) for axis, length in enumerate(values.shape)]
    main_axis = values.shape.index(max(values.shape))
    next_to = place[:main_axis] + [(place[main_axis] + 1) % values.shape[main_axis]] + place[main_axis + 1:]
    return values.at[tuple(place)].set(least).at[tuple(next_to)].set(high)


def shard_levels(stream_key, shape, shards, low, largest):
    loudness = 1.0
    for position, shards_of in shards:
        heights = jax.random.uniform(jax.random.fold_in(jax.random.fold_in(stream_key, 6), position), (shards_of,), jnp.float32, low / len(shards), largest / len(shards))
        loudness = loudness * jnp.repeat(jnp.exp(heights), shape[position] // shards_of).reshape((-1,) + (1,) * (len(shape) - 1 - position))
    return loudness


def bell_draw(stream_key, extent, width, limit, shards=(), kind=jnp.bfloat16):
    drawn = jax.random.normal(stream_key, extent, jnp.float32) * width
    if len(shards) > 0:
        drawn = shard_levels(stream_key, extent, shards, -0.22, 0.18) * drawn
    return jnp.clip(drawn, min=-limit, max=limit).astype(kind)


def setup_inputs(seed: int = 0) -> dict:
    key_list = jax.random.split(jax.random.key(seed), 10)
    return {
        "flow_state": bell_draw(key_list[0], (BLOCK, CELLS), 1.0, 6.0, ((1, 16),), jnp.float32),
        "source_term": bell_draw(key_list[1], (BLOCK, CELLS), 4.0, 24.0, ((1, 16),), jnp.float32),
        "volume_rate": jnp.clip(jnp.exp(math.log(4.0) - 2.0794415 * jax.random.uniform(key_list[2], (CELLS,), jnp.float32) ** shard_levels(key_list[2], (CELLS,), ((0, 16),), -0.2, 0.2)), 0.5, 4.0),
        "face_normal": bell_draw(key_list[3], (3, FACES), 0.5, 3.0, ((1, 32),), jnp.float32),
        "face_owner": draw_face_owner(jax.random.fold_in(key_list[9], 71), 0),
        "face_neighbour": draw_face_neighbour(jax.random.fold_in(key_list[9], 71), 0),
        "face_count": draw_face_count(jax.random.fold_in(key_list[9], 71), 0),
        "send_list": with_ends(jax.random.randint(key_list[7], (PARTITIONS * 2 * NEIGH, HALO), 0, CELLS_DEV), jax.random.fold_in(key_list[7], 1), 0, CELLS_DEV - 1).astype(jnp.int32),
        "halo_count": draw_halo_count(jax.random.fold_in(key_list[9], 71), 0),
    }


def shift_table():
    return jnp.array([which + 1 for which in range(NEIGH)] + [-(which + 1) for which in range(NEIGH)], jnp.int32)

def reference(flow_state, source_term, volume_rate, face_normal, face_owner, face_neighbour, face_count, send_list, halo_count):
    list_total = 2 * NEIGH
    face_ids = jnp.arange(FACES, dtype=jnp.int32)
    partition = face_ids // (FACE_SLOTS * SPLIT)
    is_live = (face_ids % FACE_SLOTS < face_count[face_ids // FACE_SLOTS]).astype(jnp.float32)
    owner_global = partition * CELLS_DEV + face_owner
    is_local = face_neighbour < CELLS_DEV
    halo_pos = jnp.maximum(face_neighbour - CELLS_DEV, 0)
    which_list = halo_pos // HALO
    which_slot = halo_pos % HALO
    sender = (partition - shift_table()[which_list]) % PARTITIONS
    list_row = sender * list_total + which_list
    sent_cell = send_list[list_row, which_slot]
    halo_live = which_slot < halo_count[list_row]
    neighbour_global = jnp.where(is_local, partition * CELLS_DEV + face_neighbour, sender * CELLS_DEV + sent_cell)
    neighbour_weight = jnp.where(is_local | halo_live, 1.0, 0.0).astype(jnp.float32)
    local_weight = is_local.astype(jnp.float32)
    sink_index = jnp.where(is_local, neighbour_global, CELLS)
    index_both = jnp.concatenate([owner_global, sink_index])

    def to_cells(owner_values, neighbour_values):
        stacked = jnp.concatenate([owner_values, neighbour_values], axis=1).T
        summed = jax.ops.segment_sum(stacked, index_both, num_segments=CELLS + 1)
        return summed[:CELLS].T
    left_state = flow_state[:, owner_global]
    right_state = flow_state[:, neighbour_global] * neighbour_weight
    normal_speed = 0.5 * lax.optimization_barrier(jnp.sum(face_normal * (left_state[:3] + right_state[:3]), axis=0))
    normal_size = jnp.sqrt(lax.optimization_barrier(jnp.sum(face_normal * face_normal, axis=0)))
    wave_speed = jnp.abs(normal_speed) + 2.0 * normal_size
    owner_terms = 0.5 * jnp.concatenate([normal_speed[None], face_normal, wave_speed[None]], axis=0) * is_live
    neighbour_terms = jnp.concatenate([-0.5 * normal_speed[None], -0.5 * face_normal, 0.5 * wave_speed[None]], axis=0) * (is_live * local_weight)
    block_terms = to_cells(owner_terms, neighbour_terms)
    velocity_diag = volume_rate + block_terms[0] + block_terms[4]
    pressure_diag = volume_rate + block_terms[4]
    coupling = block_terms[1:4]
    schur = pressure_diag - lax.optimization_barrier(jnp.sum(coupling * coupling, axis=0)) / velocity_diag

    def precondition(vector_in):
        pressure = (vector_in[3] - lax.optimization_barrier(jnp.sum(coupling * vector_in[:3], axis=0)) / velocity_diag) / schur
        velocity = (vector_in[:3] - coupling * pressure) / velocity_diag
        return jnp.concatenate([velocity, pressure[None]], axis=0)

    def apply_matrix(vector_in):
        left_side = vector_in[:, owner_global]
        right_side = vector_in[:, neighbour_global] * neighbour_weight
        face_sum = left_side + right_side
        central = jnp.concatenate([normal_speed * face_sum[:3] + face_normal * face_sum[3], lax.optimization_barrier(jnp.sum(face_normal * face_sum[:3], axis=0))[None]], axis=0)
        face_flux = (0.5 * central - 0.5 * wave_speed * (right_side - left_side)) * is_live
        return volume_rate * vector_in + to_cells(face_flux, -face_flux * local_weight)
    solution_field = jnp.zeros_like(source_term)
    residual = source_term
    shadow = source_term
    direction = source_term
    rho_now = jnp.sum(shadow * residual)
    for iteration in range(ITERS):
        pre_dir = precondition(direction)
        image = apply_matrix(pre_dir)
        step_alpha = rho_now / jnp.sum(shadow * image)
        middle = residual - step_alpha * image
        pre_mid = precondition(middle)
        second = apply_matrix(pre_mid)
        step_omega = jnp.sum(second * middle) / jnp.sum(second * second)
        solution_field = solution_field + step_alpha * pre_dir + step_omega * pre_mid
        residual = middle - step_omega * second
        if iteration + 1 < ITERS:
            rho_next = jnp.sum(shadow * residual)
            ratio_beta = rho_next / rho_now * (step_alpha / step_omega)
            direction = residual + ratio_beta * (direction - step_omega * image)
            rho_now = rho_next
    return (solution_field, residual)
```

```python
import functools

import jax
import jax.numpy as jnp
from jax import lax
from jax.experimental import pallas as pl
from jax.experimental.pallas import tpu as pltpu
from jax.sharding import PartitionSpec as P

F32 = jnp.float32
I32 = jnp.int32
LANES = 128
SUB = 8
BLOCK = 4


def offsets(count):
    return [which + 1 for which in range(count)] + [-(which + 1) for which in range(count)]


def pick(values, index):
    return jnp.take_along_axis(values, index, axis=1, mode="promise_in_bounds")


def lane_ids(shape=(SUB, LANES)):
    return lax.broadcasted_iota(I32, shape, 1)


def sub_ids(shape=(SUB, LANES)):
    return lax.broadcasted_iota(I32, shape, 0)


def ring_place(distance, count):
    here = lax.axis_index("cells")
    return lax.rem(here + distance + count, count)


def in_groups(tiles):
    return range(tiles // SUB)


def rows8(g):
    return slice(g * SUB, g * SUB + SUB)


def listed(cell_ref, send_ref):
    tiles = cell_ref.shape[1]
    halves = send_ref.shape[0] // 2
    row_at = [send_ref[h] for h in range(halves)]
    lane_at = [send_ref[halves + h] for h in range(halves)]
    found = [[jnp.zeros((SUB, LANES), F32) for _ in range(halves)] for _ in range(BLOCK)]
    for t in range(tiles):
        here = [row_at[h] == t for h in range(halves)]
        for c in range(BLOCK):
            row = jnp.broadcast_to(cell_ref[c, t : t + 1, :], (SUB, LANES))
            for h in range(halves):
                found[c][h] = jnp.where(here[h], pick(row, lane_at[h]), found[c][h])
    return found


def send_halo(found, stage_ref, out_ref, shifts):
    count = out_ref.shape[0]
    halves = len(found[0])
    for c in range(BLOCK):
        for h in range(halves):
            at = (c * halves + h) * SUB
            stage_ref[at : at + SUB, :] = found[c][h]
    for which, shift in enumerate(shifts):
        place = ring_place(shift, count)
        out_ref[place, 0:SUB, :] = stage_ref[pl.ds(which, SUB, stride=SUB), :]


def got_halo(in_ref, shifts):
    count = in_ref.shape[0]
    return [in_ref[ring_place(-shift, count), 0:SUB, :] for shift in shifts]


def lay_halo(lists, halo_ref):
    total = len(lists)
    span = halo_ref.shape[0] // SUB
    for j in range(total + SUB - 1):
        halo_ref[pl.ds(j, SUB, stride=span), :] = lists[j % total]


def send_sums(sums, out_ref):
    rows = jnp.zeros((SUB, LANES), F32)
    sub = sub_ids()
    for i, acc in enumerate(sums):
        row = jnp.sum(acc, axis=0, keepdims=True)
        rows = jnp.where(sub == i, jnp.broadcast_to(row, (SUB, LANES)), rows)
    first = out_ref.shape[1] - SUB
    for d in range(out_ref.shape[0]):
        out_ref[d, first : first + SUB, :] = rows


def got_sums(in_ref):
    first = in_ref.shape[1] - SUB
    parts = [in_ref[d, first : first + SUB, :] for d in range(in_ref.shape[0])]
    while len(parts) > 1:
        parts = [a + b for a, b in zip(parts[::2], parts[1::2])] + parts[len(parts) & ~1 :]
    return jnp.sum(parts[0], axis=1, keepdims=True)


def spread(column, i):
    return jnp.broadcast_to(column[i : i + 1, :], (SUB, LANES))


def row_of(ref, i):
    return jnp.broadcast_to(ref[i : i + 1, :], (SUB, LANES))


def prefix_matrix():
    shape = (3 * LANES, LANES)
    upto = (lax.broadcasted_iota(I32, shape, 0) % LANES) <= lax.broadcasted_iota(I32, shape, 1)
    return jnp.where(upto, 1.0, 0.0).astype(jnp.bfloat16)


def prefix_sums(blocks, matrix):
    values = jnp.concatenate(blocks, axis=0)
    high = values.astype(jnp.bfloat16)
    rest = values - high.astype(F32)
    middle = rest.astype(jnp.bfloat16)
    low = (rest - middle.astype(F32)).astype(jnp.bfloat16)
    split = jnp.concatenate([high, middle, low], axis=1)
    sums = jnp.dot(split, matrix, preferred_element_type=F32)
    return [sums[i * SUB : (i + 1) * SUB, :] for i in range(len(blocks))]


def to_cells(fluxes, tables, g, matrix, signs):
    rows, parts = len(fluxes), len(fluxes[0])
    order_ref, last_ref = tables
    blocks = []
    for side in range(2):
        for r in range(rows):
            order = order_ref[side, r, rows8(g), :]
            blocks += [pick(fluxes[r][c], order) for c in range(parts)]
    sums = prefix_sums(blocks, matrix)
    totals = []
    for side, of in ((0, 0), (1, 1), (1, 2)):
        acc = None
        for r in range(rows):
            last = last_ref[of, r, rows8(g), :]
            some = last >= 0
            at = jnp.maximum(last, 0)
            got = [
                jnp.where(some, pick(sums[(side * rows + r) * parts + c], at), 0.0)
                for c in range(parts)
            ]
            acc = got if acc is None else [a + b for a, b in zip(acc, got)]
        totals.append(acc)
    lane = lane_ids()
    here, beside = [], []
    for c in range(parts):
        owned, near, far = totals[0][c], totals[1][c], totals[2][c]
        both = owned + near if signs[c] > 0 else owned - near
        here.append(both - jnp.where(lane == 0, 0.0, pltpu.roll(both, 1, 1)))
        before = pltpu.roll(jnp.where(lane == LANES - 1, near, far), 1, 1)
        beside.append(far - before)
    return here, beside


def face_values(wide_ref, halo_ref, owner, code, g, lists, parts):
    span = halo_ref.shape[0] // SUB
    halves = SUB // BLOCK
    at = code & (LANES - 1)
    source = code >> 7
    first = (g * SUB) % lists
    left, right = [], []
    for c in range(parts):
        own = wide_ref[c, rows8(g), :]
        left.append(pick(own, owner))
        got = pick(own, at)
        got = jnp.where(source == 1, pick(wide_ref[c, g * SUB + 1 : g * SUB + 1 + SUB, :], at), got)
        for h in range(halves):
            base = (c * halves + h) * span + first
            got = jnp.where(source == 2 + h, pick(halo_ref[base : base + SUB, :], at), got)
        right.append(got)
    return left, right


def widen(wide_ref, tiles):
    for c in range(BLOCK):
        wide_ref[c, tiles : tiles + 1, :] = wide_ref[c, 0:1, :]


def wrap_beside(beside_ref, tiles):
    for c in range(beside_ref.shape[0]):
        beside_ref[c, 0:1, :] = beside_ref[c, tiles : tiles + 1, :]


def face_part(wide_ref, halo_ref, face_ref, link_ref, tables, here_ref, beside_ref, lists):
    tiles = here_ref.shape[1]
    rows = face_ref.shape[1]
    matrix = prefix_matrix()
    for g in in_groups(tiles):
        fluxes = []
        for r in range(rows):
            owner, code = link_ref[0, r, rows8(g), :], link_ref[1, r, rows8(g), :]
            left, right = face_values(wide_ref, halo_ref, owner, code, g, lists, BLOCK)
            speed, n0, n1, n2, wave = [face_ref[i, r, rows8(g), :] for i in range(5)]
            both = [a + b for a, b in zip(left, right)]
            gap = [a - b for a, b in zip(left, right)]
            normal = (n0, n1, n2)
            flux = [speed * both[i] + normal[i] * both[3] + wave * gap[i] for i in range(3)]
            flux.append(n0 * both[0] + n1 * both[1] + n2 * both[2] + wave * gap[3])
            fluxes.append(flux)
        here, beside = to_cells(fluxes, tables, g, matrix, (-1,) * BLOCK)
        for c in range(BLOCK):
            here_ref[c, rows8(g), :] = here[c]
            beside_ref[c, g * SUB + 1 : g * SUB + 1 + SUB, :] = beside[c]
    wrap_beside(beside_ref, tiles)


def precondition(vector, diag_ref, g):
    inverse, n0, n1, n2, schur = [diag_ref[i, rows8(g), :] for i in range(5)]
    coupled = n0 * vector[0] + n1 * vector[1] + n2 * vector[2]
    pressure = (vector[3] - coupled * inverse) * schur
    return [(vector[i] - n * pressure) * inverse for i, n in enumerate((n0, n1, n2))] + [pressure]


def applied(g, volume_ref, wide_ref, here_ref, beside_ref):
    volume = volume_ref[rows8(g), :]
    return [
        volume * wide_ref[c, rows8(g), :] + (here_ref[c, rows8(g), :] - beside_ref[c, rows8(g), :])
        for c in range(BLOCK)
    ]


def cell(ref, g):
    return [ref[c, rows8(g), :] for c in range(BLOCK)]


def put(ref, g, vector):
    for c in range(BLOCK):
        ref[c, rows8(g), :] = vector[c]


def added(acc, a, b):
    for x, y in zip(a, b):
        acc = acc + x * y
    return acc


def zero():
    return jnp.zeros((SUB, LANES), F32)


def start_kernel(
    count_ref, used_ref, normal_ref, owner_ref, neighbour_ref, flow_ref, list_ref,
    pack_ref, out_ref, flow_out, send_ref,
    stage_ref, *, shifts, cells_here,
):
    lists, width = list_ref.shape
    halves = width // LANES
    tiles = cells_here // LANES
    pairs = tiles // 2
    shape = (pairs, LANES)
    pair, lane = sub_ids(shape), lane_ids(shape)
    for i in range(3 * pairs):
        for c in range(3):
            at = (i % 3) * pairs + i // 3
            pack_ref[c, at : at + 1, :] = normal_ref[c : c + 1, i * LANES : (i + 1) * LANES]
    for q in range(3):
        at = slice(q * pairs, (q + 1) * pairs)
        tile = 2 * pair + (0, jnp.where(lane >= LANES // 2, 1, 0), 1)[q]
        live = (3 * pair + q) * LANES + lane < count_ref[0]
        owner = owner_ref[pl.ds(q, pairs, stride=3), :] - tile * LANES
        neighbour = neighbour_ref[pl.ds(q, pairs, stride=3), :]
        near = (neighbour - tile * LANES) & (cells_here - 1)
        far = neighbour - cells_here - lax.rem(tile, lists) * width + 2 * LANES
        code = jnp.where(neighbour < cells_here, near, far)
        pack_ref[3, at, :] = (owner * 512 + code).astype(F32)
        for c in range(3):
            pack_ref[c, at, :] = jnp.where(live, pack_ref[c, at, :], 0.0)
    for t in range(tiles):
        for c in range(BLOCK):
            flow_out[c, t : t + 1, :] = flow_ref[c : c + 1, t * LANES : (t + 1) * LANES]
    sub = sub_ids()
    used = jnp.zeros((SUB, LANES), I32)
    for k in range(lists):
        used = jnp.where(sub == k, used_ref[k], used)
    for h in range(halves):
        for k in range(lists):
            stage_ref[k : k + 1, :] = list_ref[k : k + 1, h * LANES : (h + 1) * LANES].astype(F32)
        listed_cell = stage_ref[0:SUB, :].astype(I32)
        alive = (lane_ids() + h * LANES < used) & (sub < lists)
        send_ref[h] = jnp.where(alive, listed_cell >> 7, -1)
        send_ref[halves + h] = jnp.where(alive, listed_cell & (LANES - 1), 0)
    send_halo(listed(flow_out, send_ref), stage_ref, out_ref, shifts)


def sorted_columns(x):
    sub = sub_ids()
    for k in range(1, 8):
        flip = None
        if 4 <= k <= 6:
            flip = ((sub >> (k - 4)) & 1) == 1
            x = [jnp.where(flip, -a, a) for a in x]
        for j in range(k - 1, -1, -1):
            if j < 4:
                new = list(x)
                for v in range(16):
                    w = v | (1 << j)
                    if w != v:
                        low, high = jnp.minimum(x[v], x[w]), jnp.maximum(x[v], x[w])
                        down = k < 4 and (v >> k) & 1
                        new[v], new[w] = (high, low) if down else (low, high)
                x = new
            else:
                d = 1 << (j - 4)
                first = ((sub >> (j - 4)) & 1) == 0
                x = [
                    jnp.where(
                        first,
                        jnp.minimum(a, pltpu.roll(a, SUB - d, 0)),
                        jnp.maximum(a, pltpu.roll(a, d, 0)),
                    )
                    for a in x
                ]
        if flip is not None:
            x = [jnp.where(flip, -a, a) for a in x]
    return x


def sort_rows(key_ref):
    lane = lane_ids()
    back = 8 * (lane & 15) + (lane >> 4)
    for b in range(key_ref.shape[0] // LANES):
        at = slice(b * LANES, (b + 1) * LANES)
        turned = jnp.transpose(key_ref[at, :])
        x = sorted_columns([turned[v * SUB : (v + 1) * SUB, :] for v in range(16)])
        turned = jnp.transpose(jnp.concatenate(x, axis=0))
        for v in range(16):
            row = b * LANES + v * SUB
            key_ref[row : row + SUB, :] = pick(turned[v * SUB : (v + 1) * SUB, :], back)


def last_below(keys, bound):
    at = jnp.zeros((SUB, LANES), I32)
    for step in (64, 32, 16, 8, 4, 2, 1):
        at = jnp.where(pick(keys, at + (step - 1)) < bound, at + step, at)
    return jnp.where(pick(keys, at) < bound, at, at - 1)


def setup_kernel(
    mine_ref, peer_ref, in_ref, flow_ref, source_ref, volume_ref, send_ref,
    face_ref, link_ref, order_ref, last_ref, diag_ref, source_out, pre_ref, out_ref,
    stage_ref, halo_ref, wide_ref, key_ref, here_ref, beside_ref, tile_ref, *, shifts,
):
    lists = len(shifts)
    tiles = volume_ref.shape[0]
    pairs = tiles // 2
    for t in range(tiles):
        for c in range(BLOCK):
            source_out[c, t : t + 1, :] = source_ref[c : c + 1, t * LANES : (t + 1) * LANES]
    swapped = lax.axis_index("faces") == 1
    lane = lane_ids((pairs, LANES))
    half = LANES // 2
    for i in range(4):
        part = []
        for q in range(3):
            mine = mine_ref[i, q * pairs : (q + 1) * pairs, :]
            peer = peer_ref[i, q * pairs : (q + 1) * pairs, :]
            part.append((jnp.where(swapped, peer, mine), jnp.where(swapped, mine, peer)))
        (a0, b0), (a1, b1), (a2, b2) = part
        even = (a0, b0, jnp.where(lane < half, a1, pltpu.roll(b1, half, 1)))
        odd = (a2, b2, jnp.where(lane < half, pltpu.roll(a1, half, 1), b1))
        for r in range(3):
            tile_ref[i * 3 + r, pl.ds(0, pairs, stride=2), :] = even[r]
            tile_ref[i * 3 + r, pl.ds(1, pairs, stride=2), :] = odd[r]
    lane = lane_ids()
    for r in range(3):
        for g in in_groups(tiles):
            joint = tile_ref[9 + r, rows8(g), :].astype(I32)
            owner, code = joint >> 9, joint & 511
            link_ref[0, r, rows8(g), :] = owner
            link_ref[1, r, rows8(g), :] = code
            at = r * tiles + g * SUB
            key_ref[at : at + SUB, :] = (owner * LANES + lane).astype(F32)
            at += 3 * tiles
            key_ref[at : at + SUB, :] = (jnp.minimum(code, 256) * LANES + lane).astype(F32)
    sort_rows(key_ref)
    for r in range(3):
        for g in in_groups(tiles):
            at = r * tiles + g * SUB
            owned = key_ref[at : at + SUB, :]
            near = key_ref[at + 3 * tiles : at + 3 * tiles + SUB, :]
            order_ref[0, r, rows8(g), :] = owned.astype(I32) & (LANES - 1)
            order_ref[1, r, rows8(g), :] = near.astype(I32) & (LANES - 1)
            bound = ((lane + 1) * LANES).astype(F32)
            last_ref[0, r, rows8(g), :] = last_below(owned, bound)
            last_ref[1, r, rows8(g), :] = last_below(near, bound)
            last_ref[2, r, rows8(g), :] = last_below(near, bound + float(LANES * LANES))
    for g in in_groups(tiles):
        put(wide_ref, g, cell(flow_ref, g))
    widen(wide_ref, tiles)
    lay_halo(got_halo(in_ref, shifts), halo_ref)
    matrix = prefix_matrix()
    for g in in_groups(tiles):
        terms = []
        for r in range(3):
            owner, code = link_ref[0, r, rows8(g), :], link_ref[1, r, rows8(g), :]
            left, right = face_values(wide_ref, halo_ref, owner, code, g, lists, 3)
            normal = [tile_ref[i * 3 + r, rows8(g), :] for i in range(3)]
            speed = zero()
            size = zero()
            for i in range(3):
                speed = speed + normal[i] * (left[i] + right[i])
                size = size + normal[i] * normal[i]
            speed = 0.5 * speed
            wave = jnp.abs(speed) + 2.0 * jnp.sqrt(size)
            term = [0.5 * speed] + [0.5 * n for n in normal] + [0.5 * wave]
            for i in range(5):
                face_ref[i, r, rows8(g), :] = term[i]
            terms.append(term)
        here, beside = to_cells(terms, (order_ref, last_ref), g, matrix, (-1, -1, -1, -1, 1))
        for i in range(5):
            here_ref[i, rows8(g), :] = here[i]
            beside_ref[i, g * SUB + 1 : g * SUB + 1 + SUB, :] = beside[i]
    wrap_beside(beside_ref, tiles)
    for g in in_groups(tiles):
        volume = volume_ref[rows8(g), :]
        own = [here_ref[i, rows8(g), :] for i in range(5)]
        other = [beside_ref[i, rows8(g), :] for i in range(5)]
        speed, n0, n1, n2 = [own[i] - other[i] for i in range(4)]
        pressure_diag = volume + (own[4] + other[4])
        inverse = 1.0 / (pressure_diag + speed)
        schur = pressure_diag - (n0 * n0 + n1 * n1 + n2 * n2) * inverse
        for i, value in enumerate((inverse, n0, n1, n2, 1.0 / schur)):
            diag_ref[i, rows8(g), :] = value
        put(pre_ref, g, precondition(cell(source_out, g), diag_ref, g))
    send_halo(listed(pre_ref, send_ref), stage_ref, out_ref, shifts)


def combine(scales, vectors):
    out = []
    for parts in zip(*vectors):
        acc = None
        for scale, part in zip(scales, parts):
            term = part if scale is None else scale * part
            acc = term if acc is None else acc + term
        out.append(acc)
    return out


def first_kernel(
    in_ref, pre_ref, source_ref, volume_ref, face_ref, link_ref, order_ref, last_ref, diag_ref, send_ref,
    image_ref, mimage_ref, out_ref,
    stage_ref, halo_ref, wide_ref, here_ref, beside_ref, *, shifts,
):
    tiles = volume_ref.shape[0]
    groups = in_groups(tiles)
    for g in groups:
        put(wide_ref, g, cell(pre_ref, g))
    widen(wide_ref, tiles)
    lay_halo(got_halo(in_ref, shifts), halo_ref)
    face_part(wide_ref, halo_ref, face_ref, link_ref, (order_ref, last_ref), here_ref, beside_ref, len(shifts))
    product, rho = zero(), zero()
    for g in groups:
        image = applied(g, volume_ref, wide_ref, here_ref, beside_ref)
        source = cell(source_ref, g)
        product = added(product, source, image)
        rho = added(rho, source, source)
        put(image_ref, g, image)
        put(mimage_ref, g, precondition(image, diag_ref, g))
    send_sums((product, rho), out_ref)
    send_halo(listed(mimage_ref, send_ref), stage_ref, out_ref, shifts)


def second_kernel(
    in1_ref, in2_ref, pre_ref, mimage_ref, image_ref, source_ref,
    volume_ref, face_ref, link_ref, order_ref, last_ref, diag_ref, send_ref,
    middle_ref, premid_ref, second_ref, msecond_ref, scale_ref, out_ref,
    stage_ref, halo_ref, wide_ref, here_ref, beside_ref, *, shifts,
):
    tiles = volume_ref.shape[0]
    groups = in_groups(tiles)
    sums = got_sums(in2_ref)
    rho = spread(sums, 1)
    alpha = rho / spread(sums, 0)
    scale_ref[0:1, :] = alpha[0:1, :]
    scale_ref[1:2, :] = rho[0:1, :]
    for g in groups:
        premid = combine((None, -alpha), (cell(pre_ref, g), cell(mimage_ref, g)))
        put(wide_ref, g, premid)
        put(premid_ref, g, premid)
    widen(wide_ref, tiles)
    lay_halo(combine((None, -alpha), (got_halo(in1_ref, shifts), got_halo(in2_ref, shifts))), halo_ref)
    face_part(wide_ref, halo_ref, face_ref, link_ref, (order_ref, last_ref), here_ref, beside_ref, len(shifts))
    products = [zero() for _ in range(4)]
    for g in groups:
        second = applied(g, volume_ref, wide_ref, here_ref, beside_ref)
        source = cell(source_ref, g)
        middle = combine((None, -alpha), (source, cell(image_ref, g)))
        put(middle_ref, g, middle)
        put(second_ref, g, second)
        put(msecond_ref, g, precondition(second, diag_ref, g))
        for i, (a, b) in enumerate(((second, middle), (second, second), (source, middle), (source, second))):
            products[i] = added(products[i], a, b)
    send_sums(products, out_ref)
    send_halo(listed(msecond_ref, send_ref), stage_ref, out_ref, shifts)


def third_kernel(
    in1_ref, in2_ref, in3_ref, scale_ref, pre_ref, mimage_ref, premid_ref, msecond_ref, middle_ref, second_ref, source_ref,
    volume_ref, face_ref, link_ref, order_ref, last_ref, diag_ref, send_ref,
    field_ref, residual_ref, preres_ref, predir_ref, image_ref, mimage_out, scale_out, ghost_ref, out_ref,
    stage_ref, halo_ref, wide_ref, here_ref, beside_ref, *, shifts,
):
    tiles = volume_ref.shape[0]
    groups = in_groups(tiles)
    sums = got_sums(in3_ref)
    alpha, rho = row_of(scale_ref, 0), row_of(scale_ref, 1)
    omega = spread(sums, 0) / spread(sums, 1)
    rho_next = spread(sums, 2) - omega * spread(sums, 3)
    beta = rho_next / rho * (alpha / omega)
    scale_out[0:1, :] = rho_next[0:1, :]
    drop = -beta * omega
    for g in groups:
        predir, mimage, premid = cell(pre_ref, g), cell(mimage_ref, g), cell(premid_ref, g)
        put(field_ref, g, combine((alpha, omega), (predir, premid)))
        put(residual_ref, g, combine((None, -omega), (cell(middle_ref, g), cell(second_ref, g))))
        preres = combine((None, -omega), (premid, cell(msecond_ref, g)))
        put(preres_ref, g, preres)
        predir = combine((None, beta, drop), (preres, predir, mimage))
        put(predir_ref, g, predir)
        put(wide_ref, g, predir)
    widen(wide_ref, tiles)
    ghost1, ghost2, ghost3 = [got_halo(ref, shifts) for ref in (in1_ref, in2_ref, in3_ref)]
    preres = combine((None, -alpha, -omega), (ghost1, ghost2, ghost3))
    for k in range(len(shifts)):
        ghost_ref[k] = preres[k]
    lay_halo(combine((None, beta, drop), (preres, ghost1, ghost2)), halo_ref)
    face_part(wide_ref, halo_ref, face_ref, link_ref, (order_ref, last_ref), here_ref, beside_ref, len(shifts))
    product = zero()
    for g in groups:
        image = applied(g, volume_ref, wide_ref, here_ref, beside_ref)
        product = added(product, cell(source_ref, g), image)
        put(image_ref, g, image)
        put(mimage_out, g, precondition(image, diag_ref, g))
    send_sums((product,), out_ref)
    send_halo(listed(mimage_out, send_ref), stage_ref, out_ref, shifts)


def fourth_kernel(
    in4_ref, scale_ref, ghost_ref, field_ref, residual_ref, preres_ref, predir_ref, image_ref, mimage_ref,
    volume_ref, face_ref, link_ref, order_ref, last_ref,
    field_out, premid_ref, middle_ref, second_ref, out_ref,
    halo_ref, wide_ref, here_ref, beside_ref, *, shifts,
):
    tiles = volume_ref.shape[0]
    groups = in_groups(tiles)
    alpha = row_of(scale_ref, 0) / spread(got_sums(in4_ref), 0)
    for g in groups:
        premid = combine((None, -alpha), (cell(preres_ref, g), cell(mimage_ref, g)))
        put(wide_ref, g, premid)
        put(premid_ref, g, premid)
        put(field_out, g, combine((None, alpha), (cell(field_ref, g), cell(predir_ref, g))))
        put(middle_ref, g, combine((None, -alpha), (cell(residual_ref, g), cell(image_ref, g))))
    widen(wide_ref, tiles)
    ghosts = [ghost_ref[k] for k in range(len(shifts))]
    lay_halo(combine((None, -alpha), (ghosts, got_halo(in4_ref, shifts))), halo_ref)
    face_part(wide_ref, halo_ref, face_ref, link_ref, (order_ref, last_ref), here_ref, beside_ref, len(shifts))
    cross, square = zero(), zero()
    for g in groups:
        second = applied(g, volume_ref, wide_ref, here_ref, beside_ref)
        put(second_ref, g, second)
        cross = added(cross, second, cell(middle_ref, g))
        square = added(square, second, second)
    send_sums((cross, square), out_ref)


def last_kernel(in_ref, field_ref, premid_ref, middle_ref, second_ref, field_out, residual_out, stage_ref):
    tiles = field_ref.shape[1]
    sums = got_sums(in_ref)
    omega = spread(sums, 0) / spread(sums, 1)
    for g in in_groups(tiles):
        field = combine((None, omega), (cell(field_ref, g), cell(premid_ref, g)))
        residual = combine((None, -omega), (cell(middle_ref, g), cell(second_ref, g)))
        put(stage_ref.at[0], g, field)
        put(stage_ref.at[1], g, residual)
        for i, out in enumerate((field_out, residual_out)):
            for t in range(g * SUB, g * SUB + SUB):
                for c in range(BLOCK):
                    out[c : c + 1, t * LANES : (t + 1) * LANES] = stage_ref[i, c, t : t + 1, :]


def run(kernel, outs, scratch, args, scalars=0):
    vmem = pl.BlockSpec(memory_space=pltpu.VMEM)
    smem = pl.BlockSpec(memory_space=pltpu.SMEM)
    return pl.pallas_call(
        kernel,
        out_shape=[jax.ShapeDtypeStruct(shape, dtype) for shape, dtype in outs],
        in_specs=[smem] * scalars + [vmem] * (len(args) - scalars),
        out_specs=[vmem] * len(outs),
        scratch_shapes=[pltpu.VMEM(shape, F32) for shape in scratch],
        compiler_params=pltpu.CompilerParams(vmem_limit_bytes=24 << 20),
    )(*args)


def exchange(block):
    return lax.all_to_all(block, "cells", 0, 0)


def body(
    flow_state,
    source_term,
    volume_rate,
    face_normal,
    face_owner,
    face_neighbour,
    face_count,
    send_list,
    halo_count,
):
    count = lax.axis_size("cells")
    cells_here = flow_state.shape[1]
    lists, width = send_list.shape
    tiles = cells_here // LANES
    per_tile = face_owner.shape[0] // tiles
    shifts = offsets(lists // 2)
    halves = width // LANES
    assert per_tile * 2 == 3 * LANES and lax.axis_size("faces") == 2
    assert width == 2 * LANES and count > lists and lists <= SUB
    assert tiles % SUB == 0 and cells_here & (cells_here - 1) == 0
    rows = 3
    span = -(-(lists + SUB - 1) // SUB) * SUB
    vector = (BLOCK, tiles, LANES)
    vec = (vector, F32)
    faces = (rows, tiles, LANES)
    scale = ((SUB, LANES), F32)
    halo_block = ((count, SUB, LANES), F32)
    full_block = ((count, 2 * SUB, LANES), F32)
    wide = (BLOCK, tiles + SUB, LANES)
    stage = (SUB * SUB, LANES)
    halo = (SUB * span, LANES)
    flat = face_owner.shape[0] // LANES
    volume = volume_rate.reshape(tiles, LANES)

    pack, out0, flow, send = run(
        functools.partial(start_kernel, shifts=shifts, cells_here=cells_here),
        [((4, flat, LANES), F32), halo_block, vec, ((2 * halves, SUB, LANES), I32)],
        [stage],
        (
            face_count, halo_count, face_normal, face_owner.reshape(flat, LANES),
            face_neighbour.reshape(flat, LANES), flow_state, send_list,
        ),
        scalars=2,
    )
    peer = lax.ppermute(pack, "faces", [(0, 1), (1, 0)])
    in0 = exchange(out0)
    face, link, order, last, diag, source, predir, out1 = run(
        functools.partial(setup_kernel, shifts=shifts),
        [
            ((5,) + faces, F32), ((2,) + faces, I32), ((2,) + faces, I32), ((3,) + faces, I32),
            ((5, tiles, LANES), F32), vec, vec, halo_block,
        ],
        [stage, halo, wide, (6 * tiles, LANES), (5, tiles, LANES), (5, tiles + SUB, LANES), (12, tiles, LANES)],
        (pack, peer, in0, flow, source_term, volume, send),
    )
    in1 = exchange(out1)
    work = [stage, halo, wide, vector, wide]
    fixed = (volume, face, link, order, last, diag, send)
    image, mimage, out2 = run(
        functools.partial(first_kernel, shifts=shifts), [vec, vec, full_block], work, (in1, predir, source) + fixed
    )
    in2 = exchange(out2)
    middle, premid, second, msecond, scales, out3 = run(
        functools.partial(second_kernel, shifts=shifts),
        [vec, vec, vec, vec, scale, full_block],
        work,
        (in1, in2, predir, mimage, image, source) + fixed,
    )
    in3 = exchange(out3)
    field, residual, preres, predir, image, mimage, scales, ghosts, out4 = run(
        functools.partial(third_kernel, shifts=shifts),
        [vec, vec, vec, vec, vec, vec, scale, ((lists, SUB, LANES), F32), full_block],
        work,
        (in1, in2, in3, scales, predir, mimage, premid, msecond, middle, second, source) + fixed,
    )
    in4 = exchange(out4)
    field, premid, middle, second, out5 = run(
        functools.partial(fourth_kernel, shifts=shifts),
        [vec, vec, vec, vec, halo_block],
        work[1:],
        (in4, scales, ghosts, field, residual, preres, predir, image, mimage) + fixed[:5],
    )
    in5 = exchange(out5)
    out = (flow_state.shape, F32)
    field, residual = run(last_kernel, [out, out], [(2,) + vector], (in5, field, premid, middle, second))
    return (field, residual)


def solution(mesh):
    in_specs = (
        P(None, "cells"),
        P(None, "cells"),
        P("cells"),
        P(None, ("cells", "faces")),
        P(("cells", "faces")),
        P(("cells", "faces")),
        P(("cells", "faces")),
        P("cells", None),
        P("cells"),
    )
    out_specs = (P(None, "cells"), P(None, "cells"))
    return jax.shard_map(body, mesh=mesh, in_specs=in_specs, out_specs=out_specs, check_vma=False)
```

```python
import functools

import jax
import jax.numpy as jnp
from jax import lax
from jax.experimental import pallas as pl
from jax.experimental.pallas import tpu as pltpu
from jax.sharding import PartitionSpec as P

F32 = jnp.float32
I32 = jnp.int32
LANES = 128
SUB = 8
BLOCK = 4


def offsets(count):
    return [which + 1 for which in range(count)] + [-(which + 1) for which in range(count)]


ALONG_LANES = lax.GatherDimensionNumbers(
    offset_dims=(),
    collapsed_slice_dims=(1,),
    start_index_map=(1,),
    operand_batching_dims=(0,),
    start_indices_batching_dims=(0,),
)

ALONG_ROWS = lax.GatherDimensionNumbers(
    offset_dims=(),
    collapsed_slice_dims=(0,),
    start_index_map=(0,),
    operand_batching_dims=(1,),
    start_indices_batching_dims=(1,),
)


def pick(values, index):
    mode = lax.GatherScatterMode.PROMISE_IN_BOUNDS
    return lax.gather(values, index[..., None], ALONG_LANES, slice_sizes=(1, 1), mode=mode)


def pick_row(values, index):
    mode = lax.GatherScatterMode.PROMISE_IN_BOUNDS
    return lax.gather(values, index[..., None], ALONG_ROWS, slice_sizes=(1, 1), mode=mode)


def lane_ids(shape=(SUB, LANES)):
    return lax.broadcasted_iota(I32, shape, 1)


def sub_ids(shape=(SUB, LANES)):
    return lax.broadcasted_iota(I32, shape, 0)


def partition(distance, count):
    return lax.rem(lax.axis_index("cells") + distance + count, count)


def in_groups(tiles):
    return range(tiles // SUB)


def rows8(g):
    return slice(g * SUB, g * SUB + SUB)


def listed(cell_ref, send_ref):
    row_at, lane_at = send_ref[0], send_ref[1]
    found = [jnp.zeros((SUB, LANES), F32) for _ in range(BLOCK)]
    for t in range(cell_ref.shape[1]):
        here = row_at == t
        for c in range(BLOCK):
            row = jnp.broadcast_to(cell_ref[c, t : t + 1, :], (SUB, LANES))
            found[c] = jnp.where(here, pick(row, lane_at), found[c])
    return found


def send_halo(found, stage_ref, out_ref, each):
    cores = lax.axis_size("faces")
    count = out_ref.shape[0] // cores
    halves = SUB // BLOCK
    for c in range(BLOCK):
        stage_ref[c * SUB : (c + 1) * SUB, :] = found[c]
    sign = 1 - 2 * lax.axis_index("faces")
    for j in range(each):
        place = partition(sign * (j + 1), count)
        for h in range(halves):
            rows = stage_ref[pl.ds(j * halves + h, BLOCK, stride=SUB), :]
            for core in range(cores):
                out_ref[place * cores + core, h * BLOCK : (h + 1) * BLOCK, :] = rows


def got_halo(in_ref, shifts):
    cores = lax.axis_size("faces")
    count = in_ref.shape[0] // cores
    each = len(shifts) // cores
    return [in_ref[partition(-shift, count) * cores + k // each] for k, shift in enumerate(shifts)]


def lay_halo(lists, halo_ref):
    total = len(lists)
    span = halo_ref.shape[0] // SUB
    for j in range(total + SUB - 1):
        halo_ref[pl.ds(j, SUB, stride=span), :] = lists[j % total]


def send_sums(sums, out_ref):
    rows = jnp.zeros((SUB, LANES), F32)
    sub = sub_ids()
    for i, acc in enumerate(sums):
        row = jnp.sum(acc, axis=0, keepdims=True)
        rows = jnp.where(sub == i, jnp.broadcast_to(row, (SUB, LANES)), rows)
    for d in range(out_ref.shape[0]):
        out_ref[d] = rows


def total_of(parts):
    while len(parts) > 1:
        parts = [a + b for a, b in zip(parts[::2], parts[1::2])] + parts[len(parts) & ~1 :]
    return jnp.sum(parts[0], axis=1, keepdims=True)


def got_sums(in_ref, each):
    cores = lax.axis_size("faces")
    count = in_ref.shape[0] // cores
    parts = []
    for q in range(count):
        ahead = partition(-q, count)
        core = jnp.where((ahead >= 1) & (ahead <= each), 1, 0)
        parts.append(in_ref[q * cores + core])
    return total_of(parts)


def spread(column, i):
    return jnp.broadcast_to(column[i : i + 1, :], (SUB, LANES))


def row_of(ref, i):
    return jnp.broadcast_to(ref[i : i + 1, :], (SUB, LANES))


def prefix_matrix():
    shape = (2 * LANES, LANES)
    upto = (lax.broadcasted_iota(I32, shape, 0) & (LANES - 1)) <= lax.broadcasted_iota(I32, shape, 1)
    return jnp.where(upto, 1.0, 0.0).astype(jnp.bfloat16)


def prefix_sums(values, matrix):
    high = values.astype(jnp.bfloat16)
    low = (values - high.astype(F32)).astype(jnp.bfloat16)
    return jnp.dot(jnp.concatenate([high, low], axis=1), matrix, preferred_element_type=F32)


def block_at(i):
    return slice(i * SUB, i * SUB + SUB)


def to_cells(flux_ref, order_ref, last_ref, here_ref, beside_ref, sort_ref, signs):
    parts = len(signs)
    tiles = here_ref.shape[1]
    rows = order_ref.shape[1]
    each = rows * parts
    matrix = prefix_matrix()
    for g in in_groups(tiles):
        for side in range(2):
            for r in range(rows):
                order = order_ref[side, r, rows8(g), :]
                for c in range(parts):
                    source = flux_ref[block_at(g * each + r * parts + c), :]
                    sort_ref[block_at((g * 2 + side) * each + r * parts + c), :] = pick(source, order)
    for g in in_groups(tiles):
        at = slice(g * 2 * each * SUB, (g + 1) * 2 * each * SUB)
        sort_ref[at, :] = prefix_sums(sort_ref[at, :], matrix)
    lane = lane_ids()
    for g in in_groups(tiles):
        totals = []
        for side, of in ((0, 0), (1, 1), (1, 2)):
            acc = None
            for r in range(rows):
                last = last_ref[of, r, rows8(g), :]
                some = last >= 0
                at = last & (LANES - 1)
                got = [
                    jnp.where(some, pick(sort_ref[block_at((g * 2 + side) * each + r * parts + c), :], at), 0.0)
                    for c in range(parts)
                ]
                acc = got if acc is None else [a + b for a, b in zip(acc, got)]
            totals.append(acc)
        for c in range(parts):
            owned, near, far = totals[0][c], totals[1][c], totals[2][c]
            here_ref[c, rows8(g), :] = owned + near if signs[c] > 0 else owned - near
            beside_ref[c, g * SUB + 1 : g * SUB + 1 + SUB, :] = jnp.where(lane == LANES - 1, near, far)
            sort_ref[block_at(g * 2 * each + c), :] = far
    for g in in_groups(tiles):
        for c in range(parts):
            both = here_ref[c, rows8(g), :]
            here_ref[c, rows8(g), :] = both - jnp.where(lane == 0, 0.0, pltpu.roll(both, 1, 1))
            at = slice(g * SUB + 1, g * SUB + 1 + SUB)
            before = pltpu.roll(beside_ref[c, at, :], 1, 1)
            beside_ref[c, at, :] = sort_ref[block_at(g * 2 * each + c), :] - before
    for c in range(parts):
        beside_ref[c, 0:1, :] = beside_ref[c, tiles : tiles + 1, :]


def face_values(wide_ref, halo_ref, owner, code, g, lists, parts):
    span = halo_ref.shape[0] // SUB
    halves = SUB // BLOCK
    at = code & (LANES - 1)
    source = code >> 7
    first = (g * SUB) % lists
    own = [wide_ref[c, rows8(g), :] for c in range(parts)]
    left = [pick(v, owner) for v in own]
    right = [pick(v, at) for v in own]
    masks = [source == i for i in range(1, 2 + halves)]
    for c in range(parts):
        others = [wide_ref[c, g * SUB + 1 : g * SUB + 1 + SUB, :]]
        for h in range(halves):
            base = (h * BLOCK + c) * span + first
            others.append(halo_ref[base : base + SUB, :])
        for mask, other in zip(masks, others):
            right[c] = jnp.where(mask, pick(other, at), right[c])
    return left, right


def widen(wide_ref, tiles):
    for c in range(BLOCK):
        wide_ref[c, tiles : tiles + 1, :] = wide_ref[c, 0:1, :]


def face_part(wide_ref, halo_ref, face_ref, link_ref, tables, here_ref, beside_ref, flux_ref, sort_ref, lists):
    tiles = here_ref.shape[1]
    rows = face_ref.shape[1]
    for g in in_groups(tiles):
        for r in range(rows):
            owner, code = link_ref[0, r, rows8(g), :], link_ref[1, r, rows8(g), :]
            left, right = face_values(wide_ref, halo_ref, owner, code, g, lists, BLOCK)
            speed, n0, n1, n2, wave = [face_ref[i, r, rows8(g), :] for i in range(5)]
            both = [a + b for a, b in zip(left, right)]
            gap = [a - b for a, b in zip(left, right)]
            normal = (n0, n1, n2)
            flux = [speed * both[i] + normal[i] * both[3] + wave * gap[i] for i in range(3)]
            flux.append(n0 * both[0] + n1 * both[1] + n2 * both[2] + wave * gap[3])
            for c in range(BLOCK):
                flux_ref[block_at((g * rows + r) * BLOCK + c), :] = flux[c]
    to_cells(flux_ref, *tables, here_ref, beside_ref, sort_ref, (-1,) * BLOCK)


def precondition(vector, diag_ref, g):
    inverse, n0, n1, n2, schur = [diag_ref[i, rows8(g), :] for i in range(5)]
    coupled = n0 * vector[0] + n1 * vector[1] + n2 * vector[2]
    pressure = (vector[3] - coupled * inverse) * schur
    return [(vector[i] - n * pressure) * inverse for i, n in enumerate((n0, n1, n2))] + [pressure]


def applied(g, volume_ref, wide_ref, here_ref, beside_ref):
    volume = volume_ref[rows8(g), :]
    return [
        volume * wide_ref[c, rows8(g), :] + (here_ref[c, rows8(g), :] - beside_ref[c, rows8(g), :])
        for c in range(BLOCK)
    ]


def cell(ref, g):
    return [ref[c, rows8(g), :] for c in range(BLOCK)]


def put(ref, g, vector):
    for c in range(BLOCK):
        ref[c, rows8(g), :] = vector[c]


def added(acc, a, b):
    for x, y in zip(a, b):
        acc = acc + x * y
    return acc


def zero():
    return jnp.zeros((SUB, LANES), F32)


def start_kernel(
    count_ref, used_ref, normal_ref, owner_ref, neighbour_ref, flow_ref, list_ref,
    pack_ref, out_ref, flow_out, send_ref,
    stage_ref, *, cells_here,
):
    lists, width = list_ref.shape
    each = lists // 2
    halves = width // LANES
    tiles = cells_here // LANES
    pairs = tiles // 2
    shape = (pairs, LANES)
    pair, lane = sub_ids(shape), lane_ids(shape)
    for i in range(3 * pairs):
        for c in range(3):
            at = (i % 3) * pairs + i // 3
            pack_ref[c, at : at + 1, :] = normal_ref[c : c + 1, i * LANES : (i + 1) * LANES]
    for q in range(3):
        at = slice(q * pairs, (q + 1) * pairs)
        tile = 2 * pair + (0, jnp.where(lane >= LANES // 2, 1, 0), 1)[q]
        live = (3 * pair + q) * LANES + lane < count_ref[0]
        owner = owner_ref[pl.ds(q, pairs, stride=3), :] - tile * LANES
        neighbour = neighbour_ref[pl.ds(q, pairs, stride=3), :]
        near = (neighbour - tile * LANES) & (cells_here - 1)
        far = neighbour - cells_here - lax.rem(tile, lists) * width + 2 * LANES
        code = jnp.where(neighbour < cells_here, near, far)
        pack_ref[3, at, :] = (owner * 512 + code).astype(F32)
        for c in range(3):
            pack_ref[c, at, :] = jnp.where(live, pack_ref[c, at, :], 0.0)
    for t in range(tiles):
        for c in range(BLOCK):
            flow_out[c, t : t + 1, :] = flow_ref[c : c + 1, t * LANES : (t + 1) * LANES]
    sub = sub_ids()
    core = lax.axis_index("faces")
    used = jnp.zeros((SUB, LANES), I32)
    for j in range(each):
        for h in range(halves):
            i = j * halves + h
            rows = [list_ref[k : k + 1, h * LANES : (h + 1) * LANES] for k in (j, each + j)]
            stage_ref[i : i + 1, :] = jnp.where(core == 0, *rows).astype(F32)
            used = jnp.where(sub == i, used_ref[core * each + j] - h * LANES, used)
    cells = stage_ref[0:SUB, :].astype(I32)
    alive = (lane_ids() < used) & (sub < each * halves)
    send_ref[0] = jnp.where(alive, cells >> 7, -1)
    send_ref[1] = jnp.where(alive, cells & (LANES - 1), 0)
    send_halo(listed(flow_out, send_ref), stage_ref, out_ref, each)


def sorted_columns(x):
    sub = sub_ids()
    for k in range(1, 8):
        flip = None
        if 4 <= k <= 6:
            flip = ((sub >> (k - 4)) & 1) == 1
            x = [jnp.where(flip, -a, a) for a in x]
        for j in range(k - 1, -1, -1):
            if j < 4:
                new = list(x)
                for v in range(16):
                    w = v | (1 << j)
                    if w != v:
                        low, high = jnp.minimum(x[v], x[w]), jnp.maximum(x[v], x[w])
                        down = k < 4 and (v >> k) & 1
                        new[v], new[w] = (high, low) if down else (low, high)
                x = new
            else:
                d = 1 << (j - 4)
                first = ((sub >> (j - 4)) & 1) == 0
                x = [
                    jnp.where(
                        first,
                        jnp.minimum(a, pltpu.roll(a, SUB - d, 0)),
                        jnp.maximum(a, pltpu.roll(a, d, 0)),
                    )
                    for a in x
                ]
        if flip is not None:
            x = [jnp.where(flip, -a, a) for a in x]
    return x


def counts_below(x, first):
    sub = sub_ids()
    rows = []
    heads = [jnp.broadcast_to(x[15][s : s + 1, :], (SUB, LANES)) for s in range(SUB)]
    for w in range(LANES // SUB):
        bound = ((sub + (first + w * SUB + 1)) * LANES).astype(F32)
        block = jnp.zeros((SUB, LANES), I32)
        for s in range(SUB):
            block = jnp.where(heads[s] < bound, s + 1, block)
        at = jnp.minimum(block, SUB - 1)
        inside = jnp.zeros((SUB, LANES), I32)
        for v in range(15):
            inside = jnp.where(pick_row(x[v], at) < bound, v + 1, inside)
        rows.append((block * 16 + jnp.where(block < SUB, inside, 0)).astype(F32))
    return rows


def sort_rows(key_ref, lower_ref, upper_ref):
    lane = lane_ids()
    back = 8 * (lane & 15) + (lane >> 4)
    skip = lower_ref.shape[0] - upper_ref.shape[0]
    for b in range(key_ref.shape[0] // LANES):
        at = slice(b * LANES, (b + 1) * LANES)
        turned = jnp.transpose(key_ref[at, :])
        x = sorted_columns([turned[v * SUB : (v + 1) * SUB, :] for v in range(16)])
        turned = jnp.transpose(jnp.concatenate(x, axis=0))
        for v in range(16):
            row = b * LANES + v * SUB
            key_ref[row : row + SUB, :] = pick(turned[v * SUB : (v + 1) * SUB, :], back)
        lower_ref[at, :] = jnp.transpose(jnp.concatenate(counts_below(x, 0), axis=0))
        if b * LANES >= skip:
            at = slice(b * LANES - skip, (b + 1) * LANES - skip)
            upper_ref[at, :] = jnp.transpose(jnp.concatenate(counts_below(x, LANES), axis=0))


def setup_kernel(
    mine_ref, peer_ref, in_ref, flow_ref, source_ref, volume_ref, send_ref,
    face_ref, link_ref, order_ref, last_ref, diag_ref, source_out, pre_ref, out_ref,
    stage_ref, halo_ref, wide_ref, key_ref, here_ref, beside_ref, tile_ref, flux_ref, sort_ref, lower_ref, upper_ref, *, shifts,
):
    lists = len(shifts)
    tiles = volume_ref.shape[0]
    pairs = tiles // 2
    for t in range(tiles):
        for c in range(BLOCK):
            source_out[c, t : t + 1, :] = source_ref[c : c + 1, t * LANES : (t + 1) * LANES]
    swapped = lax.axis_index("faces") == 1
    lane = lane_ids((pairs, LANES))
    half = LANES // 2
    for i in range(4):
        part = []
        for q in range(3):
            mine = mine_ref[i, q * pairs : (q + 1) * pairs, :]
            peer = peer_ref[i, q * pairs : (q + 1) * pairs, :]
            part.append((jnp.where(swapped, peer, mine), jnp.where(swapped, mine, peer)))
        (a0, b0), (a1, b1), (a2, b2) = part
        even = (a0, b0, jnp.where(lane < half, a1, pltpu.roll(b1, half, 1)))
        odd = (a2, b2, jnp.where(lane < half, pltpu.roll(a1, half, 1), b1))
        for r in range(3):
            tile_ref[i * 3 + r, pl.ds(0, pairs, stride=2), :] = even[r]
            tile_ref[i * 3 + r, pl.ds(1, pairs, stride=2), :] = odd[r]
    lane = lane_ids()
    for r in range(3):
        for g in in_groups(tiles):
            joint = tile_ref[9 + r, rows8(g), :].astype(I32)
            owner, code = joint >> 9, joint & 511
            link_ref[0, r, rows8(g), :] = owner
            link_ref[1, r, rows8(g), :] = code
            at = r * tiles + g * SUB
            key_ref[at : at + SUB, :] = (owner * LANES + lane).astype(F32)
            at += 3 * tiles
            key_ref[at : at + SUB, :] = (jnp.minimum(code, 256) * LANES + lane).astype(F32)
    sort_rows(key_ref, lower_ref, upper_ref)
    skip = lower_ref.shape[0] - upper_ref.shape[0]
    for r in range(3):
        for g in in_groups(tiles):
            at = r * tiles + g * SUB
            owned = key_ref[at : at + SUB, :]
            near = key_ref[at + 3 * tiles : at + 3 * tiles + SUB, :]
            order_ref[0, r, rows8(g), :] = owned.astype(I32) & (LANES - 1)
            order_ref[1, r, rows8(g), :] = near.astype(I32) & (LANES - 1)
            near = at + 3 * tiles
            for i, count in enumerate(
                (lower_ref[at : at + SUB, :], lower_ref[near : near + SUB, :], upper_ref[near - skip : near - skip + SUB, :])
            ):
                last_ref[i, r, rows8(g), :] = count.astype(I32) - 1
    for g in in_groups(tiles):
        put(wide_ref, g, cell(flow_ref, g))
    widen(wide_ref, tiles)
    lay_halo(got_halo(in_ref, shifts), halo_ref)
    for g in in_groups(tiles):
        for r in range(3):
            owner, code = link_ref[0, r, rows8(g), :], link_ref[1, r, rows8(g), :]
            left, right = face_values(wide_ref, halo_ref, owner, code, g, lists, 3)
            normal = [tile_ref[i * 3 + r, rows8(g), :] for i in range(3)]
            speed = zero()
            size = zero()
            for i in range(3):
                speed = speed + normal[i] * (left[i] + right[i])
                size = size + normal[i] * normal[i]
            speed = 0.5 * speed
            wave = jnp.abs(speed) + 2.0 * jnp.sqrt(size)
            term = [0.5 * speed] + [0.5 * n for n in normal] + [0.5 * wave]
            for i in range(5):
                face_ref[i, r, rows8(g), :] = term[i]
                flux_ref[block_at((g * 3 + r) * 5 + i), :] = term[i]
    to_cells(flux_ref, order_ref, last_ref, here_ref, beside_ref, sort_ref, (-1, -1, -1, -1, 1))
    for g in in_groups(tiles):
        volume = volume_ref[rows8(g), :]
        own = [here_ref[i, rows8(g), :] for i in range(5)]
        other = [beside_ref[i, rows8(g), :] for i in range(5)]
        speed, n0, n1, n2 = [own[i] - other[i] for i in range(4)]
        pressure_diag = volume + (own[4] + other[4])
        inverse = 1.0 / (pressure_diag + speed)
        schur = pressure_diag - (n0 * n0 + n1 * n1 + n2 * n2) * inverse
        for i, value in enumerate((inverse, n0, n1, n2, 1.0 / schur)):
            diag_ref[i, rows8(g), :] = value
        put(pre_ref, g, precondition(cell(source_out, g), diag_ref, g))
    send_halo(listed(pre_ref, send_ref), stage_ref, out_ref, len(shifts) // 2)


def combine(scales, vectors):
    out = []
    for parts in zip(*vectors):
        acc = None
        for scale, part in zip(scales, parts):
            term = part if scale is None else scale * part
            acc = term if acc is None else acc + term
        out.append(acc)
    return out


def first_kernel(
    in_ref, pre_ref, source_ref, volume_ref, face_ref, link_ref, order_ref, last_ref, diag_ref, send_ref,
    image_ref, mimage_ref, out_ref,
    stage_ref, halo_ref, wide_ref, here_ref, beside_ref, flux_ref, sort_ref, *, shifts,
):
    tiles = volume_ref.shape[0]
    groups = in_groups(tiles)
    for g in groups:
        put(wide_ref, g, cell(pre_ref, g))
    widen(wide_ref, tiles)
    lay_halo(got_halo(in_ref, shifts), halo_ref)
    face_part(wide_ref, halo_ref, face_ref, link_ref, (order_ref, last_ref), here_ref, beside_ref, flux_ref, sort_ref, len(shifts))
    product, rho = zero(), zero()
    for g in groups:
        image = applied(g, volume_ref, wide_ref, here_ref, beside_ref)
        source = cell(source_ref, g)
        product = added(product, source, image)
        rho = added(rho, source, source)
        put(image_ref, g, image)
        put(mimage_ref, g, precondition(image, diag_ref, g))
    send_sums((product, rho), out_ref)
    send_halo(listed(mimage_ref, send_ref), stage_ref, out_ref, len(shifts) // 2)


def second_kernel(
    in1_ref, in2_ref, pre_ref, mimage_ref, image_ref, source_ref,
    volume_ref, face_ref, link_ref, order_ref, last_ref, diag_ref, send_ref,
    middle_ref, premid_ref, second_ref, msecond_ref, scale_ref, out_ref,
    stage_ref, halo_ref, wide_ref, here_ref, beside_ref, flux_ref, sort_ref, *, shifts,
):
    tiles = volume_ref.shape[0]
    groups = in_groups(tiles)
    sums = got_sums(in2_ref, len(shifts) // 2)
    rho = spread(sums, 1)
    alpha = rho / spread(sums, 0)
    scale_ref[0:1, :] = alpha[0:1, :]
    scale_ref[1:2, :] = rho[0:1, :]
    for g in groups:
        premid = combine((None, -alpha), (cell(pre_ref, g), cell(mimage_ref, g)))
        put(wide_ref, g, premid)
        put(premid_ref, g, premid)
    widen(wide_ref, tiles)
    lay_halo(combine((None, -alpha), (got_halo(in1_ref, shifts), got_halo(in2_ref, shifts))), halo_ref)
    face_part(wide_ref, halo_ref, face_ref, link_ref, (order_ref, last_ref), here_ref, beside_ref, flux_ref, sort_ref, len(shifts))
    products = [zero() for _ in range(4)]
    for g in groups:
        second = applied(g, volume_ref, wide_ref, here_ref, beside_ref)
        source = cell(source_ref, g)
        middle = combine((None, -alpha), (source, cell(image_ref, g)))
        put(middle_ref, g, middle)
        put(second_ref, g, second)
        put(msecond_ref, g, precondition(second, diag_ref, g))
        for i, (a, b) in enumerate(((second, middle), (second, second), (source, middle), (source, second))):
            products[i] = added(products[i], a, b)
    send_sums(products, out_ref)
    send_halo(listed(msecond_ref, send_ref), stage_ref, out_ref, len(shifts) // 2)


def third_kernel(
    in1_ref, in2_ref, in3_ref, scale_ref, pre_ref, mimage_ref, premid_ref, msecond_ref, middle_ref, second_ref, source_ref,
    volume_ref, face_ref, link_ref, order_ref, last_ref, diag_ref, send_ref,
    field_ref, residual_ref, preres_ref, predir_ref, image_ref, mimage_out, scale_out, ghost_ref, out_ref,
    stage_ref, halo_ref, wide_ref, here_ref, beside_ref, flux_ref, sort_ref, *, shifts,
):
    tiles = volume_ref.shape[0]
    groups = in_groups(tiles)
    sums = got_sums(in3_ref, len(shifts) // 2)
    alpha, rho = row_of(scale_ref, 0), row_of(scale_ref, 1)
    omega = spread(sums, 0) / spread(sums, 1)
    rho_next = spread(sums, 2) - omega * spread(sums, 3)
    beta = rho_next / rho * (alpha / omega)
    scale_out[0:1, :] = rho_next[0:1, :]
    drop = -beta * omega
    for g in groups:
        predir, mimage, premid = cell(pre_ref, g), cell(mimage_ref, g), cell(premid_ref, g)
        put(field_ref, g, combine((alpha, omega), (predir, premid)))
        put(residual_ref, g, combine((None, -omega), (cell(middle_ref, g), cell(second_ref, g))))
        preres = combine((None, -omega), (premid, cell(msecond_ref, g)))
        put(preres_ref, g, preres)
        predir = combine((None, beta, drop), (preres, predir, mimage))
        put(predir_ref, g, predir)
        put(wide_ref, g, predir)
    widen(wide_ref, tiles)
    ghost1, ghost2, ghost3 = [got_halo(ref, shifts) for ref in (in1_ref, in2_ref, in3_ref)]
    preres = combine((None, -alpha, -omega), (ghost1, ghost2, ghost3))
    for k in range(len(shifts)):
        ghost_ref[k] = preres[k]
    lay_halo(combine((None, beta, drop), (preres, ghost1, ghost2)), halo_ref)
    face_part(wide_ref, halo_ref, face_ref, link_ref, (order_ref, last_ref), here_ref, beside_ref, flux_ref, sort_ref, len(shifts))
    product = zero()
    for g in groups:
        image = applied(g, volume_ref, wide_ref, here_ref, beside_ref)
        product = added(product, cell(source_ref, g), image)
        put(image_ref, g, image)
        put(mimage_out, g, precondition(image, diag_ref, g))
    send_sums((product,), out_ref)
    send_halo(listed(mimage_out, send_ref), stage_ref, out_ref, len(shifts) // 2)


def fourth_kernel(
    in4_ref, scale_ref, ghost_ref, field_ref, residual_ref, preres_ref, predir_ref, image_ref, mimage_ref,
    volume_ref, face_ref, link_ref, order_ref, last_ref,
    field_out, premid_ref, middle_ref, second_ref, out_ref,
    halo_ref, wide_ref, here_ref, beside_ref, flux_ref, sort_ref, *, shifts,
):
    tiles = volume_ref.shape[0]
    groups = in_groups(tiles)
    alpha = row_of(scale_ref, 0) / spread(got_sums(in4_ref, len(shifts) // 2), 0)
    for g in groups:
        premid = combine((None, -alpha), (cell(preres_ref, g), cell(mimage_ref, g)))
        put(wide_ref, g, premid)
        put(premid_ref, g, premid)
        put(field_out, g, combine((None, alpha), (cell(field_ref, g), cell(predir_ref, g))))
        put(middle_ref, g, combine((None, -alpha), (cell(residual_ref, g), cell(image_ref, g))))
    widen(wide_ref, tiles)
    ghosts = [ghost_ref[k] for k in range(len(shifts))]
    lay_halo(combine((None, -alpha), (ghosts, got_halo(in4_ref, shifts))), halo_ref)
    face_part(wide_ref, halo_ref, face_ref, link_ref, (order_ref, last_ref), here_ref, beside_ref, flux_ref, sort_ref, len(shifts))
    cross, square = zero(), zero()
    for g in groups:
        second = applied(g, volume_ref, wide_ref, here_ref, beside_ref)
        put(second_ref, g, second)
        cross = added(cross, second, cell(middle_ref, g))
        square = added(square, second, second)
    send_sums((cross, square), out_ref)


def last_kernel(in_ref, field_ref, premid_ref, middle_ref, second_ref, field_out, residual_out, stage_ref):
    tiles = field_ref.shape[1]
    sums = total_of([in_ref[d] for d in range(in_ref.shape[0])])
    omega = spread(sums, 0) / spread(sums, 1)
    for g in in_groups(tiles):
        field = combine((None, omega), (cell(field_ref, g), cell(premid_ref, g)))
        residual = combine((None, -omega), (cell(middle_ref, g), cell(second_ref, g)))
        put(stage_ref.at[0], g, field)
        put(stage_ref.at[1], g, residual)
        for i, out in enumerate((field_out, residual_out)):
            for t in range(g * SUB, g * SUB + SUB):
                for c in range(BLOCK):
                    out[c : c + 1, t * LANES : (t + 1) * LANES] = stage_ref[i, c, t : t + 1, :]


def run(kernel, outs, scratch, args, scalars=0):
    vmem = pl.BlockSpec(memory_space=pltpu.VMEM)
    smem = pl.BlockSpec(memory_space=pltpu.SMEM)
    return pl.pallas_call(
        kernel,
        out_shape=[jax.ShapeDtypeStruct(shape, dtype) for shape, dtype in outs],
        in_specs=[smem] * scalars + [vmem] * (len(args) - scalars),
        out_specs=[vmem] * len(outs),
        scratch_shapes=[pltpu.VMEM(shape, F32) for shape in scratch],
        compiler_params=pltpu.CompilerParams(vmem_limit_bytes=24 << 20),
    )(*args)


def exchange(block):
    return lax.all_to_all(block, ("cells", "faces"), 0, 0)


def body(
    flow_state,
    source_term,
    volume_rate,
    face_normal,
    face_owner,
    face_neighbour,
    face_count,
    send_list,
    halo_count,
):
    count = lax.axis_size("cells")
    cells_here = flow_state.shape[1]
    lists, width = send_list.shape
    tiles = cells_here // LANES
    per_tile = face_owner.shape[0] // tiles
    shifts = offsets(lists // 2)
    assert per_tile * 2 == 3 * LANES and lax.axis_size("faces") == 2
    assert width == 2 * LANES and count > lists and lists % 2 == 0 and lists <= SUB
    assert tiles % SUB == 0 and cells_here & (cells_here - 1) == 0
    rows = 3
    span = -(-(lists + SUB - 1) // SUB) * SUB
    vector = (BLOCK, tiles, LANES)
    vec = (vector, F32)
    faces = (rows, tiles, LANES)
    scale = ((SUB, LANES), F32)
    sum_block = ((count, SUB, LANES), F32)
    full_block = ((2 * count, SUB, LANES), F32)
    wide = (BLOCK, tiles + SUB, LANES)
    stage = (SUB * SUB, LANES)
    halo = (SUB * span, LANES)
    flat = face_owner.shape[0] // LANES
    volume = volume_rate.reshape(tiles, LANES)

    pack, out0, flow, send = run(
        functools.partial(start_kernel, cells_here=cells_here),
        [((4, flat, LANES), F32), full_block, vec, ((2, SUB, LANES), I32)],
        [stage],
        (
            face_count, halo_count, face_normal, face_owner.reshape(flat, LANES),
            face_neighbour.reshape(flat, LANES), flow_state, send_list,
        ),
        scalars=2,
    )
    peer = lax.ppermute(pack, "faces", [(0, 1), (1, 0)])
    in0 = exchange(out0)
    face, link, order, last, diag, source, predir, out1 = run(
        functools.partial(setup_kernel, shifts=shifts),
        [
            ((5,) + faces, F32), ((2,) + faces, I32), ((2,) + faces, I32), ((3,) + faces, I32),
            ((5, tiles, LANES), F32), vec, vec, full_block,
        ],
        [stage, halo, wide, (6 * tiles, LANES), (5, tiles, LANES), (5, tiles + SUB, LANES), (12, tiles, LANES), (rows * 5 * tiles, LANES), (2 * rows * 5 * tiles, LANES), (6 * tiles, LANES), (4 * tiles, LANES)],
        (pack, peer, in0, flow, source_term, volume, send),
    )
    in1 = exchange(out1)
    work = [stage, halo, wide, vector, wide, (rows * BLOCK * tiles, LANES), (2 * rows * BLOCK * tiles, LANES)]
    fixed = (volume, face, link, order, last, diag, send)
    image, mimage, out2 = run(
        functools.partial(first_kernel, shifts=shifts), [vec, vec, full_block], work, (in1, predir, source) + fixed
    )
    in2 = exchange(out2)
    middle, premid, second, msecond, scales, out3 = run(
        functools.partial(second_kernel, shifts=shifts),
        [vec, vec, vec, vec, scale, full_block],
        work,
        (in1, in2, predir, mimage, image, source) + fixed,
    )
    in3 = exchange(out3)
    field, residual, preres, predir, image, mimage, scales, ghosts, out4 = run(
        functools.partial(third_kernel, shifts=shifts),
        [vec, vec, vec, vec, vec, vec, scale, ((lists, SUB, LANES), F32), full_block],
        work,
        (in1, in2, in3, scales, predir, mimage, premid, msecond, middle, second, source) + fixed,
    )
    in4 = exchange(out4)
    field, premid, middle, second, out5 = run(
        functools.partial(fourth_kernel, shifts=shifts),
        [vec, vec, vec, vec, sum_block],
        work[1:],
        (in4, scales, ghosts, field, residual, preres, predir, image, mimage) + fixed[:5],
    )
    in5 = lax.all_to_all(out5, "cells", 0, 0)
    out = (flow_state.shape, F32)
    field, residual = run(last_kernel, [out, out], [(2,) + vector], (in5, field, premid, middle, second))
    return (field, residual)


def solution(mesh):
    in_specs = (
        P(None, "cells"),
        P(None, "cells"),
        P("cells"),
        P(None, ("cells", "faces")),
        P(("cells", "faces")),
        P(("cells", "faces")),
        P(("cells", "faces")),
        P("cells", None),
        P("cells"),
    )
    out_specs = (P(None, "cells"), P(None, "cells"))
    return jax.shard_map(body, mesh=mesh, in_specs=in_specs, out_specs=out_specs, check_vma=False)
```

```python
import functools

import jax
import jax.numpy as jnp
from jax import lax
from jax.experimental import pallas as pl
from jax.experimental.pallas import tpu as pltpu
from jax.sharding import PartitionSpec as P

F32 = jnp.float32
I32 = jnp.int32
LANES = 128
SUB = 8
BLOCK = 4


def offsets(count):
    return [which + 1 for which in range(count)] + [-(which + 1) for which in range(count)]


ALONG_LANES = lax.GatherDimensionNumbers(
    offset_dims=(),
    collapsed_slice_dims=(1,),
    start_index_map=(1,),
    operand_batching_dims=(0,),
    start_indices_batching_dims=(0,),
)

ALONG_ROWS = lax.GatherDimensionNumbers(
    offset_dims=(),
    collapsed_slice_dims=(0,),
    start_index_map=(0,),
    operand_batching_dims=(1,),
    start_indices_batching_dims=(1,),
)


def pick(values, index):
    mode = lax.GatherScatterMode.PROMISE_IN_BOUNDS
    return lax.gather(values, index[..., None], ALONG_LANES, slice_sizes=(1, 1), mode=mode)


def pick_row(values, index):
    mode = lax.GatherScatterMode.PROMISE_IN_BOUNDS
    return lax.gather(values, index[..., None], ALONG_ROWS, slice_sizes=(1, 1), mode=mode)


def lane_ids(shape=(SUB, LANES)):
    return lax.broadcasted_iota(I32, shape, 1)


def sub_ids(shape=(SUB, LANES)):
    return lax.broadcasted_iota(I32, shape, 0)


def partition(distance, count):
    return lax.rem(lax.axis_index("cells") + distance + count, count)


def in_groups(tiles):
    return range(tiles // SUB)


def rows8(g):
    return slice(g * SUB, g * SUB + SUB)


def listed(row_of_tile, tiles, send_ref):
    row_at, lane_at = send_ref[0], send_ref[1]
    found = [jnp.zeros((SUB, LANES), F32) for _ in range(BLOCK)]
    for t in range(tiles):
        here = row_at == t
        for c in range(BLOCK):
            row = jnp.broadcast_to(row_of_tile(c, t), (SUB, LANES))
            found[c] = jnp.where(here, pick(row, lane_at), found[c])
    return found


def tiled_rows(ref):
    return lambda c, t: ref[c, t : t + 1, :]


def flat_rows(ref):
    return lambda c, t: ref[c : c + 1, t * LANES : (t + 1) * LANES]


def send_halo(found, stage_ref, out_ref, each):
    cores = lax.axis_size("faces")
    count = out_ref.shape[0] // cores
    halves = SUB // BLOCK
    for c in range(BLOCK):
        stage_ref[c * SUB : (c + 1) * SUB, :] = found[c]
    sign = 1 - 2 * lax.axis_index("faces")
    for j in range(each):
        place = partition(sign * (j + 1), count)
        for h in range(halves):
            rows = stage_ref[pl.ds(j * halves + h, BLOCK, stride=SUB), :]
            for core in range(cores):
                out_ref[place * cores + core, h * BLOCK : (h + 1) * BLOCK, :] = rows


def got_halo(in_ref, shifts):
    cores = lax.axis_size("faces")
    count = in_ref.shape[0] // cores
    each = len(shifts) // cores
    return [in_ref[partition(-shift, count) * cores + k // each] for k, shift in enumerate(shifts)]


def lay_halo(lists, halo_ref):
    total = len(lists)
    span = halo_ref.shape[0] // SUB
    for j in range(total + SUB - 1):
        halo_ref[pl.ds(j, SUB, stride=span), :] = lists[j % total]


def send_sums(sums, out_ref):
    rows = jnp.zeros((SUB, LANES), F32)
    sub = sub_ids()
    for i, acc in enumerate(sums):
        row = jnp.sum(acc, axis=0, keepdims=True)
        rows = jnp.where(sub == i, jnp.broadcast_to(row, (SUB, LANES)), rows)
    for d in range(out_ref.shape[0]):
        out_ref[d] = rows


def total_of(parts):
    while len(parts) > 1:
        parts = [a + b for a, b in zip(parts[::2], parts[1::2])] + parts[len(parts) & ~1 :]
    return jnp.sum(parts[0], axis=1, keepdims=True)


def got_sums(in_ref, each):
    cores = lax.axis_size("faces")
    count = in_ref.shape[0] // cores
    parts = []
    for q in range(count):
        ahead = partition(-q, count)
        core = jnp.where((ahead >= 1) & (ahead <= each), 1, 0)
        parts.append(in_ref[q * cores + core])
    return total_of(parts)


def spread(column, i):
    return jnp.broadcast_to(column[i : i + 1, :], (SUB, LANES))


def row_of(ref, i):
    return jnp.broadcast_to(ref[i : i + 1, :], (SUB, LANES))


def prefix_matrix():
    shape = (2 * LANES, LANES)
    upto = (lax.broadcasted_iota(I32, shape, 0) & (LANES - 1)) <= lax.broadcasted_iota(I32, shape, 1)
    return jnp.where(upto, 1.0, 0.0).astype(jnp.bfloat16)


def prefix_sums(values, matrix):
    high = values.astype(jnp.bfloat16)
    low = (values - high.astype(F32)).astype(jnp.bfloat16)
    return jnp.dot(jnp.concatenate([high, low], axis=1), matrix, preferred_element_type=F32)


def block_at(i):
    return slice(i * SUB, i * SUB + SUB)


def to_cells(flux_ref, order_ref, last_ref, here_ref, beside_ref, sort_ref, signs):
    parts = len(signs)
    tiles = here_ref.shape[1]
    rows = order_ref.shape[1]
    each = rows * parts
    sides = 1 if beside_ref is None else 2
    matrix = prefix_matrix()
    for g in in_groups(tiles):
        for side in range(sides):
            for r in range(rows):
                order = order_ref[side, r, rows8(g), :]
                for c in range(parts):
                    source = flux_ref[block_at(g * each + r * parts + c), :]
                    sort_ref[block_at((g * sides + side) * each + r * parts + c), :] = pick(source, order)
    for g in in_groups(tiles):
        at = slice(g * sides * each * SUB, (g + 1) * sides * each * SUB)
        sort_ref[at, :] = prefix_sums(sort_ref[at, :], matrix)
    lane = lane_ids()
    for g in in_groups(tiles):
        totals = []
        for side, of in ((0, 0), (1, 1), (1, 2))[: 2 * sides - 1]:
            acc = None
            for r in range(rows):
                last = last_ref[of, r, rows8(g), :]
                some = last >= 0
                at = last & (LANES - 1)
                got = [
                    jnp.where(some, pick(sort_ref[block_at((g * sides + side) * each + r * parts + c), :], at), 0.0)
                    for c in range(parts)
                ]
                acc = got if acc is None else [a + b for a, b in zip(acc, got)]
            totals.append(acc)
        for c in range(parts):
            if sides == 1:
                here_ref[c, rows8(g), :] = totals[0][c]
                continue
            owned, near, far = totals[0][c], totals[1][c], totals[2][c]
            here_ref[c, rows8(g), :] = owned + near if signs[c] > 0 else owned - near
            beside_ref[c, g * SUB + 1 : g * SUB + 1 + SUB, :] = jnp.where(lane == LANES - 1, near, far)
            sort_ref[block_at(g * sides * each + c), :] = far
    for g in in_groups(tiles):
        for c in range(parts):
            both = here_ref[c, rows8(g), :]
            here_ref[c, rows8(g), :] = both - jnp.where(lane == 0, 0.0, pltpu.roll(both, 1, 1))
            if sides == 2:
                at = slice(g * SUB + 1, g * SUB + 1 + SUB)
                before = pltpu.roll(beside_ref[c, at, :], 1, 1)
                beside_ref[c, at, :] = sort_ref[block_at(g * sides * each + c), :] - before
    if sides == 2:
        for c in range(parts):
            beside_ref[c, 0:1, :] = beside_ref[c, tiles : tiles + 1, :]


def local_values(wide_ref, link_ref, g, r, parts):
    owner, code = link_ref[0, r, rows8(g), :], link_ref[1, r, rows8(g), :]
    at = code & (LANES - 1)
    source = code >> 7
    own = [wide_ref[c, rows8(g), :] for c in range(parts)]
    left = [pick(v, owner) for v in own]
    right = [jnp.where(source == 0, pick(v, at), 0.0) for v in own]
    for c in range(parts):
        other = wide_ref[c, g * SUB + 1 : g * SUB + 1 + SUB, :]
        right[c] = jnp.where(source == 1, pick(other, at), right[c])
    return left, right


def halo_values(right, halo_ref, link_ref, g, r, lists):
    span = halo_ref.shape[0] // SUB
    code = link_ref[1, r, rows8(g), :]
    at = code & (LANES - 1)
    source = code >> 7
    first = (g * SUB) % lists
    right = list(right)
    for h in range(SUB // BLOCK):
        for c in range(len(right)):
            base = (h * BLOCK + c) * span + first
            right[c] = jnp.where(source == 2 + h, pick(halo_ref[base : base + SUB, :], at), right[c])
    return right


def widen(wide_ref, tiles, parts=BLOCK):
    for c in range(parts):
        wide_ref[c, tiles : tiles + 1, :] = wide_ref[c, 0:1, :]


def face_terms(normal_ref, pair_ref, g, r):
    normal = [normal_ref[i, r, rows8(g), :] for i in range(3)]
    return normal, pair_ref[0, r, rows8(g), :], pair_ref[1, r, rows8(g), :]


def put_flux(flux_ref, first, normal, speed, wave, both, gap):
    for i in range(3):
        flux_ref[block_at(first + i), :] = speed * both[i] + normal[i] * both[3] + wave * gap[i]
    last = normal[0] * both[0] + normal[1] * both[1] + normal[2] * both[2] + wave * gap[3]
    flux_ref[block_at(first + 3), :] = last


def face_part(wide_ref, halo_ref, faces, here_ref, beside_ref, flux_ref, sort_ref, lists):
    normal_ref, pair_ref, link_ref, order_ref, last_ref = faces
    rows = link_ref.shape[1]
    for g in in_groups(here_ref.shape[1]):
        for r in range(rows):
            left, right = local_values(wide_ref, link_ref, g, r, BLOCK)
            right = halo_values(right, halo_ref, link_ref, g, r, lists)
            normal, speed, wave = face_terms(normal_ref, pair_ref, g, r)
            both = [a + b for a, b in zip(left, right)]
            gap = [a - b for a, b in zip(left, right)]
            put_flux(flux_ref, (g * rows + r) * BLOCK, normal, speed, wave, both, gap)
    to_cells(flux_ref, order_ref, last_ref, here_ref, beside_ref, sort_ref, (-1,) * BLOCK)


def precondition(vector, diag_ref, g):
    inverse, n0, n1, n2, schur = [diag_ref[i, rows8(g), :] for i in range(5)]
    coupled = n0 * vector[0] + n1 * vector[1] + n2 * vector[2]
    pressure = (vector[3] - coupled * inverse) * schur
    return [(vector[i] - n * pressure) * inverse for i, n in enumerate((n0, n1, n2))] + [pressure]


def applied(g, volume_ref, wide_ref, here_ref, beside_ref):
    volume = volume_ref[rows8(g), :]
    return [
        volume * wide_ref[c, rows8(g), :] + (here_ref[c, rows8(g), :] - beside_ref[c, rows8(g), :])
        for c in range(BLOCK)
    ]


def cell(ref, g):
    return [ref[c, rows8(g), :] for c in range(BLOCK)]


def put(ref, g, vector):
    for c in range(BLOCK):
        ref[c, rows8(g), :] = vector[c]


def added(acc, a, b):
    for x, y in zip(a, b):
        acc = acc + x * y
    return acc


def zero():
    return jnp.zeros((SUB, LANES), F32)


def start_kernel(
    used_any, flow_any, list_any, normal_any, owner_any, neighbour_any, source_any,
    out_ref, send_ref, flow_ref, normal_ref, owner_ref, neighbour_ref, source_ref,
    stage_ref, list_ref, used_ref, sems,
):
    pairs = (
        (used_any, used_ref), (flow_any, flow_ref), (list_any, list_ref), (normal_any, normal_ref),
        (owner_any, owner_ref), (neighbour_any, neighbour_ref), (source_any, source_ref),
    )
    copies = [pltpu.make_async_copy(a, b, sems.at[i]) for i, (a, b) in enumerate(pairs)]
    for copy in copies:
        copy.start()
    lists, width = list_ref.shape
    each = lists // 2
    halves = width // LANES
    sub = sub_ids()
    core = lax.axis_index("faces")
    used = jnp.zeros((SUB, LANES), I32)
    for copy in copies[:3]:
        copy.wait()
    for j in range(each):
        for h in range(halves):
            i = j * halves + h
            rows = [list_ref[k : k + 1, h * LANES : (h + 1) * LANES] for k in (j, each + j)]
            stage_ref[i : i + 1, :] = jnp.where(core == 0, *rows).astype(F32)
            used = jnp.where(sub == i, used_ref[core * each + j] - h * LANES, used)
    cells = stage_ref[0:SUB, :].astype(I32)
    alive = (lane_ids() < used) & (sub < each * halves)
    send_ref[0] = jnp.where(alive, cells >> 7, -1)
    send_ref[1] = jnp.where(alive, cells & (LANES - 1), 0)
    tiles = flow_ref.shape[1] // LANES
    send_halo(listed(flat_rows(flow_ref), tiles, send_ref), stage_ref, out_ref, each)
    for copy in copies[3:]:
        copy.wait()


def pack_kernel(count_ref, normal_ref, owner_ref, neighbour_ref, pack_ref, *, lists, width, cells_here):
    tiles = cells_here // LANES
    pairs = tiles // 2
    shape = (pairs, LANES)
    pair, lane = sub_ids(shape), lane_ids(shape)
    for i in range(3 * pairs):
        for c in range(3):
            at = (i % 3) * pairs + i // 3
            pack_ref[c, at : at + 1, :] = normal_ref[c : c + 1, i * LANES : (i + 1) * LANES]
    for q in range(3):
        at = slice(q * pairs, (q + 1) * pairs)
        tile = 2 * pair + (0, jnp.where(lane >= LANES // 2, 1, 0), 1)[q]
        live = (3 * pair + q) * LANES + lane < count_ref[0]
        owner = owner_ref[pl.ds(q, pairs, stride=3), :] - tile * LANES
        neighbour = neighbour_ref[pl.ds(q, pairs, stride=3), :]
        near = (neighbour - tile * LANES) & (cells_here - 1)
        far = neighbour - cells_here - lax.rem(tile, lists) * width + 2 * LANES
        code = jnp.where(neighbour < cells_here, near, far)
        pack_ref[3, at, :] = (owner * 512 + code).astype(F32)
        for c in range(3):
            pack_ref[c, at, :] = jnp.where(live, 0.5 * pack_ref[c, at, :], 0.0)


def sorted_columns(x):
    sub = sub_ids()
    for k in range(1, 8):
        flip = None
        if 4 <= k <= 6:
            flip = ((sub >> (k - 4)) & 1) == 1
            x = [jnp.where(flip, -a, a) for a in x]
        for j in range(k - 1, -1, -1):
            if j < 4:
                new = list(x)
                for v in range(16):
                    w = v | (1 << j)
                    if w != v:
                        low, high = jnp.minimum(x[v], x[w]), jnp.maximum(x[v], x[w])
                        down = k < 4 and (v >> k) & 1
                        new[v], new[w] = (high, low) if down else (low, high)
                x = new
            else:
                d = 1 << (j - 4)
                first = ((sub >> (j - 4)) & 1) == 0
                x = [
                    jnp.where(
                        first,
                        jnp.minimum(a, pltpu.roll(a, SUB - d, 0)),
                        jnp.maximum(a, pltpu.roll(a, d, 0)),
                    )
                    for a in x
                ]
        if flip is not None:
            x = [jnp.where(flip, -a, a) for a in x]
    return x


def counts_below(x, first):
    sub = sub_ids()
    rows = []
    heads = [jnp.broadcast_to(x[15][s : s + 1, :], (SUB, LANES)) for s in range(SUB)]
    for w in range(LANES // SUB):
        bound = ((sub + (first + w * SUB + 1)) * LANES).astype(F32)
        block = jnp.zeros((SUB, LANES), I32)
        for s in range(SUB):
            block = jnp.where(heads[s] < bound, s + 1, block)
        at = jnp.minimum(block, SUB - 1)
        inside = jnp.zeros((SUB, LANES), I32)
        for v in range(15):
            inside = jnp.where(pick_row(x[v], at) < bound, v + 1, inside)
        rows.append((block * 16 + jnp.where(block < SUB, inside, 0)).astype(F32))
    return rows


def sort_rows(key_ref, lower_ref, upper_ref):
    lane = lane_ids()
    back = 8 * (lane & 15) + (lane >> 4)
    skip = lower_ref.shape[0] - upper_ref.shape[0]
    for b in range(key_ref.shape[0] // LANES):
        at = slice(b * LANES, (b + 1) * LANES)
        turned = jnp.transpose(key_ref[at, :])
        x = sorted_columns([turned[v * SUB : (v + 1) * SUB, :] for v in range(16)])
        turned = jnp.transpose(jnp.concatenate(x, axis=0))
        for v in range(16):
            row = b * LANES + v * SUB
            key_ref[row : row + SUB, :] = pick(turned[v * SUB : (v + 1) * SUB, :], back)
        lower_ref[at, :] = jnp.transpose(jnp.concatenate(counts_below(x, 0), axis=0))
        if b * LANES >= skip:
            at = slice(b * LANES - skip, (b + 1) * LANES - skip)
            upper_ref[at, :] = jnp.transpose(jnp.concatenate(counts_below(x, LANES), axis=0))


def table_kernel(
    mine_ref, peer_ref, flow_ref,
    normal_ref, link_ref, order_ref, last_ref, lean_ref, coupling_ref,
    wide_ref, key_ref, beside_ref, joint_ref, flux_ref, sort_ref, lower_ref, upper_ref,
):
    tiles = normal_ref.shape[2]
    pairs = tiles // 2
    swapped = lax.axis_index("faces") == 1
    lane = lane_ids((pairs, LANES))
    half = LANES // 2
    for i in range(4):
        part = []
        for q in range(3):
            mine = mine_ref[i, q * pairs : (q + 1) * pairs, :]
            peer = peer_ref[i, q * pairs : (q + 1) * pairs, :]
            part.append((jnp.where(swapped, peer, mine), jnp.where(swapped, mine, peer)))
        (a0, b0), (a1, b1), (a2, b2) = part
        even = (a0, b0, jnp.where(lane < half, a1, pltpu.roll(b1, half, 1)))
        odd = (a2, b2, jnp.where(lane < half, pltpu.roll(a1, half, 1), b1))
        for r in range(3):
            target = normal_ref.at[i, r] if i < 3 else joint_ref.at[r]
            target[pl.ds(0, pairs, stride=2), :] = even[r]
            target[pl.ds(1, pairs, stride=2), :] = odd[r]
    lane = lane_ids()
    for r in range(3):
        for g in in_groups(tiles):
            joint = joint_ref[r, rows8(g), :].astype(I32)
            owner, code = joint >> 9, joint & 511
            link_ref[0, r, rows8(g), :] = owner
            link_ref[1, r, rows8(g), :] = code
            at = r * tiles + g * SUB
            key_ref[at : at + SUB, :] = (owner * LANES + lane).astype(F32)
            at += 3 * tiles
            key_ref[at : at + SUB, :] = (jnp.minimum(code, 256) * LANES + lane).astype(F32)
    sort_rows(key_ref, lower_ref, upper_ref)
    skip = lower_ref.shape[0] - upper_ref.shape[0]
    for r in range(3):
        for g in in_groups(tiles):
            at = r * tiles + g * SUB
            owned = key_ref[at : at + SUB, :]
            near = key_ref[at + 3 * tiles : at + 3 * tiles + SUB, :]
            order_ref[0, r, rows8(g), :] = owned.astype(I32) & (LANES - 1)
            order_ref[1, r, rows8(g), :] = near.astype(I32) & (LANES - 1)
            near = at + 3 * tiles
            for i, count in enumerate(
                (lower_ref[at : at + SUB, :], lower_ref[near : near + SUB, :], upper_ref[near - skip : near - skip + SUB, :])
            ):
                last_ref[i, r, rows8(g), :] = count.astype(I32) - 1
    for t in range(tiles):
        for c in range(3):
            wide_ref[c, t : t + 1, :] = flow_ref[c : c + 1, t * LANES : (t + 1) * LANES]
    widen(wide_ref, tiles, 3)
    for g in in_groups(tiles):
        for r in range(3):
            left, right = local_values(wide_ref, link_ref, g, r, 3)
            lean, size = zero(), zero()
            for i in range(3):
                normal = normal_ref[i, r, rows8(g), :]
                lean = lean + normal * (left[i] + right[i])
                size = size + normal * normal
                flux_ref[block_at((g * 3 + r) * 3 + i), :] = normal
            lean_ref[0, r, rows8(g), :] = lean
            lean_ref[1, r, rows8(g), :] = 2.0 * jnp.sqrt(size)
    to_cells(flux_ref, order_ref, last_ref, coupling_ref, beside_ref, sort_ref, (-1, -1, -1))
    for g in in_groups(tiles):
        for i in range(3):
            coupling_ref[i, rows8(g), :] = coupling_ref[i, rows8(g), :] - beside_ref[i, rows8(g), :]


def setup_kernel(
    in_ref, source_ref, volume_ref, normal_ref, link_ref, order_ref, last_ref, lean_ref, coupling_ref, send_ref,
    pair_ref, diag_ref, source_out, pre_ref, out_ref,
    stage_ref, halo_ref, here_ref, beside_ref, flux_ref, sort_ref, *, shifts,
):
    tiles = volume_ref.shape[0]
    lay_halo(got_halo(in_ref, shifts), halo_ref)
    for g in in_groups(tiles):
        for r in range(3):
            right = halo_values([zero() for _ in range(3)], halo_ref, link_ref, g, r, len(shifts))
            speed = lean_ref[0, r, rows8(g), :]
            for i in range(3):
                speed = speed + normal_ref[i, r, rows8(g), :] * right[i]
            wave = 0.5 * jnp.abs(speed) + lean_ref[1, r, rows8(g), :]
            for i, term in enumerate((0.5 * speed, wave)):
                pair_ref[i, r, rows8(g), :] = term
                flux_ref[block_at((g * 3 + r) * 2 + i), :] = term
    to_cells(flux_ref, order_ref, last_ref, here_ref, beside_ref, sort_ref, (-1, 1))
    for t in range(tiles):
        for c in range(BLOCK):
            source_out[c, t : t + 1, :] = source_ref[c : c + 1, t * LANES : (t + 1) * LANES]
    for g in in_groups(tiles):
        n0, n1, n2 = [coupling_ref[i, rows8(g), :] for i in range(3)]
        speed = here_ref[0, rows8(g), :] - beside_ref[0, rows8(g), :]
        pressure_diag = volume_ref[rows8(g), :] + (here_ref[1, rows8(g), :] + beside_ref[1, rows8(g), :])
        inverse = 1.0 / (pressure_diag + speed)
        schur = pressure_diag - (n0 * n0 + n1 * n1 + n2 * n2) * inverse
        for i, value in enumerate((inverse, n0, n1, n2, 1.0 / schur)):
            diag_ref[i, rows8(g), :] = value
        put(pre_ref, g, precondition(cell(source_out, g), diag_ref, g))
    send_halo(listed(tiled_rows(pre_ref), tiles, send_ref), stage_ref, out_ref, len(shifts) // 2)


def combine(scales, vectors):
    out = []
    for parts in zip(*vectors):
        acc = None
        for scale, part in zip(scales, parts):
            term = part if scale is None else scale * part
            acc = term if acc is None else acc + term
        out.append(acc)
    return out


def first_kernel(
    in_ref, pre_ref, source_ref, volume_ref, normal_ref, pair_ref, link_ref, order_ref, last_ref, diag_ref, send_ref,
    image_ref, mimage_ref, out_ref,
    stage_ref, halo_ref, wide_ref, here_ref, beside_ref, flux_ref, sort_ref, *, shifts,
):
    tiles = volume_ref.shape[0]
    groups = in_groups(tiles)
    for g in groups:
        put(wide_ref, g, cell(pre_ref, g))
    widen(wide_ref, tiles)
    lay_halo(got_halo(in_ref, shifts), halo_ref)
    faces = (normal_ref, pair_ref, link_ref, order_ref, last_ref)
    face_part(wide_ref, halo_ref, faces, here_ref, beside_ref, flux_ref, sort_ref, len(shifts))
    product, rho = zero(), zero()
    for g in groups:
        image = applied(g, volume_ref, wide_ref, here_ref, beside_ref)
        source = cell(source_ref, g)
        product = added(product, source, image)
        rho = added(rho, source, source)
        put(image_ref, g, image)
        put(mimage_ref, g, precondition(image, diag_ref, g))
    send_sums((product, rho), out_ref)
    send_halo(listed(tiled_rows(mimage_ref), tiles, send_ref), stage_ref, out_ref, len(shifts) // 2)


def second_kernel(
    in1_ref, in2_ref, pre_ref, mimage_ref, image_ref, source_ref,
    volume_ref, normal_ref, pair_ref, link_ref, order_ref, last_ref, diag_ref, send_ref,
    middle_ref, premid_ref, second_ref, msecond_ref, scale_ref, out_ref,
    stage_ref, halo_ref, wide_ref, here_ref, beside_ref, flux_ref, sort_ref, *, shifts,
):
    tiles = volume_ref.shape[0]
    groups = in_groups(tiles)
    sums = got_sums(in2_ref, len(shifts) // 2)
    rho = spread(sums, 1)
    alpha = rho / spread(sums, 0)
    scale_ref[0:1, :] = alpha[0:1, :]
    scale_ref[1:2, :] = rho[0:1, :]
    for g in groups:
        premid = combine((None, -alpha), (cell(pre_ref, g), cell(mimage_ref, g)))
        put(wide_ref, g, premid)
        put(premid_ref, g, premid)
    widen(wide_ref, tiles)
    lay_halo(combine((None, -alpha), (got_halo(in1_ref, shifts), got_halo(in2_ref, shifts))), halo_ref)
    faces = (normal_ref, pair_ref, link_ref, order_ref, last_ref)
    face_part(wide_ref, halo_ref, faces, here_ref, beside_ref, flux_ref, sort_ref, len(shifts))
    products = [zero() for _ in range(4)]
    for g in groups:
        second = applied(g, volume_ref, wide_ref, here_ref, beside_ref)
        source = cell(source_ref, g)
        middle = combine((None, -alpha), (source, cell(image_ref, g)))
        put(middle_ref, g, middle)
        put(second_ref, g, second)
        put(msecond_ref, g, precondition(second, diag_ref, g))
        for i, (a, b) in enumerate(((second, middle), (second, second), (source, middle), (source, second))):
            products[i] = added(products[i], a, b)
    send_sums(products, out_ref)
    send_halo(listed(tiled_rows(msecond_ref), tiles, send_ref), stage_ref, out_ref, len(shifts) // 2)


def third_kernel(
    in1_ref, in2_ref, in3_ref, scale_ref, pre_ref, mimage_ref, premid_ref, msecond_ref, middle_ref, second_ref, source_ref,
    volume_ref, normal_ref, pair_ref, link_ref, order_ref, last_ref, diag_ref, send_ref,
    field_ref, residual_ref, preres_ref, predir_ref, image_ref, mimage_out, scale_out, ghost_ref, out_ref,
    stage_ref, halo_ref, wide_ref, here_ref, beside_ref, flux_ref, sort_ref, *, shifts,
):
    tiles = volume_ref.shape[0]
    groups = in_groups(tiles)
    sums = got_sums(in3_ref, len(shifts) // 2)
    alpha, rho = row_of(scale_ref, 0), row_of(scale_ref, 1)
    omega = spread(sums, 0) / spread(sums, 1)
    rho_next = spread(sums, 2) - omega * spread(sums, 3)
    beta = rho_next / rho * (alpha / omega)
    scale_out[0:1, :] = rho_next[0:1, :]
    drop = -beta * omega
    for g in groups:
        predir, mimage, premid = cell(pre_ref, g), cell(mimage_ref, g), cell(premid_ref, g)
        put(field_ref, g, combine((alpha, omega), (predir, premid)))
        put(residual_ref, g, combine((None, -omega), (cell(middle_ref, g), cell(second_ref, g))))
        preres = combine((None, -omega), (premid, cell(msecond_ref, g)))
        put(preres_ref, g, preres)
        predir = combine((None, beta, drop), (preres, predir, mimage))
        put(predir_ref, g, predir)
        put(wide_ref, g, predir)
    widen(wide_ref, tiles)
    ghost1, ghost2, ghost3 = [got_halo(ref, shifts) for ref in (in1_ref, in2_ref, in3_ref)]
    preres = combine((None, -alpha, -omega), (ghost1, ghost2, ghost3))
    for k in range(len(shifts)):
        ghost_ref[k] = preres[k]
    lay_halo(combine((None, beta, drop), (preres, ghost1, ghost2)), halo_ref)
    faces = (normal_ref, pair_ref, link_ref, order_ref, last_ref)
    face_part(wide_ref, halo_ref, faces, here_ref, beside_ref, flux_ref, sort_ref, len(shifts))
    product = zero()
    for g in groups:
        image = applied(g, volume_ref, wide_ref, here_ref, beside_ref)
        product = added(product, cell(source_ref, g), image)
        put(image_ref, g, image)
        put(mimage_out, g, precondition(image, diag_ref, g))
    send_sums((product,), out_ref)
    send_halo(listed(tiled_rows(mimage_out), tiles, send_ref), stage_ref, out_ref, len(shifts) // 2)


def fourth_kernel(
    in4_ref, scale_ref, ghost_ref, field_ref, residual_ref, preres_ref, predir_ref, image_ref, mimage_ref,
    volume_ref, normal_ref, pair_ref, link_ref, order_ref, last_ref,
    field_out, premid_ref, middle_ref, second_ref, out_ref,
    halo_ref, wide_ref, here_ref, beside_ref, flux_ref, sort_ref, *, shifts,
):
    tiles = volume_ref.shape[0]
    groups = in_groups(tiles)
    alpha = row_of(scale_ref, 0) / spread(got_sums(in4_ref, len(shifts) // 2), 0)
    for g in groups:
        premid = combine((None, -alpha), (cell(preres_ref, g), cell(mimage_ref, g)))
        put(wide_ref, g, premid)
        put(premid_ref, g, premid)
        put(field_out, g, combine((None, alpha), (cell(field_ref, g), cell(predir_ref, g))))
        put(middle_ref, g, combine((None, -alpha), (cell(residual_ref, g), cell(image_ref, g))))
    widen(wide_ref, tiles)
    ghosts = [ghost_ref[k] for k in range(len(shifts))]
    lay_halo(combine((None, -alpha), (ghosts, got_halo(in4_ref, shifts))), halo_ref)
    faces = (normal_ref, pair_ref, link_ref, order_ref, last_ref)
    face_part(wide_ref, halo_ref, faces, here_ref, beside_ref, flux_ref, sort_ref, len(shifts))
    cross, square = zero(), zero()
    for g in groups:
        second = applied(g, volume_ref, wide_ref, here_ref, beside_ref)
        put(second_ref, g, second)
        cross = added(cross, second, cell(middle_ref, g))
        square = added(square, second, second)
    send_sums((cross, square), out_ref)


def last_kernel(in_ref, field_ref, premid_ref, middle_ref, second_ref, field_out, residual_out, stage_ref):
    tiles = field_ref.shape[1]
    sums = total_of([in_ref[d] for d in range(in_ref.shape[0])])
    omega = spread(sums, 0) / spread(sums, 1)
    for g in in_groups(tiles):
        field = combine((None, omega), (cell(field_ref, g), cell(premid_ref, g)))
        residual = combine((None, -omega), (cell(middle_ref, g), cell(second_ref, g)))
        put(stage_ref.at[0], g, field)
        put(stage_ref.at[1], g, residual)
        for i, out in enumerate((field_out, residual_out)):
            for t in range(g * SUB, g * SUB + SUB):
                for c in range(BLOCK):
                    out[c : c + 1, t * LANES : (t + 1) * LANES] = stage_ref[i, c, t : t + 1, :]


def run(kernel, outs, scratch, args, scalars=0, away=0):
    vmem = pl.BlockSpec(memory_space=pltpu.VMEM)
    smem = pl.BlockSpec(memory_space=pltpu.SMEM)
    hbm = pl.BlockSpec(memory_space=pltpu.HBM)
    far = range(scalars, scalars + away)
    args = [pltpu.with_memory_space_constraint(a, pltpu.HBM) if i in far else a for i, a in enumerate(args)]
    return pl.pallas_call(
        kernel,
        out_shape=[jax.ShapeDtypeStruct(shape, dtype) for shape, dtype in outs],
        in_specs=[smem] * scalars + [hbm] * away + [vmem] * (len(args) - scalars - away),
        out_specs=[vmem] * len(outs),
        scratch_shapes=[pltpu.VMEM(shape, F32) if isinstance(shape, tuple) else shape for shape in scratch],
        compiler_params=pltpu.CompilerParams(vmem_limit_bytes=24 << 20),
    )(*args)


def exchange(block):
    return lax.all_to_all(block, ("cells", "faces"), 0, 0)


def body(
    flow_state,
    source_term,
    volume_rate,
    face_normal,
    face_owner,
    face_neighbour,
    face_count,
    send_list,
    halo_count,
):
    count = lax.axis_size("cells")
    cells_here = flow_state.shape[1]
    lists, width = send_list.shape
    tiles = cells_here // LANES
    per_tile = face_owner.shape[0] // tiles
    shifts = offsets(lists // 2)
    assert per_tile * 2 == 3 * LANES and lax.axis_size("faces") == 2
    assert width == 2 * LANES and count > lists and lists % 2 == 0 and lists <= SUB
    assert tiles % SUB == 0 and cells_here & (cells_here - 1) == 0
    rows = 3
    span = -(-(lists + SUB - 1) // SUB) * SUB
    vector = (BLOCK, tiles, LANES)
    vec = (vector, F32)
    faces = (rows, tiles, LANES)
    scale = ((SUB, LANES), F32)
    sum_block = ((count, SUB, LANES), F32)
    full_block = ((2 * count, SUB, LANES), F32)
    flat_vec = (flow_state.shape, F32)
    stage = (SUB * SUB, LANES)
    halo = (SUB * span, LANES)
    flat = face_owner.shape[0] // LANES
    volume = volume_rate.reshape(tiles, LANES)

    def wide(parts):
        return (parts, tiles + SUB, LANES)

    def blocks(parts):
        return (rows * parts * tiles, LANES)

    ints = ((flat, LANES), I32)
    out0, send, flow, slopes, owner, neighbour, source = run(
        start_kernel,
        [full_block, ((2, SUB, LANES), I32), flat_vec, (face_normal.shape, F32), ints, ints, flat_vec],
        [stage, pltpu.VMEM(send_list.shape, I32), pltpu.SMEM((lists,), I32), pltpu.SemaphoreType.DMA((7,))],
        (
            halo_count, flow_state, send_list, face_normal,
            face_owner.reshape(flat, LANES), face_neighbour.reshape(flat, LANES), source_term,
        ),
        away=7,
    )
    in0 = exchange(out0)
    (pack,) = run(
        functools.partial(pack_kernel, lists=lists, width=width, cells_here=cells_here),
        [((4, flat, LANES), F32)],
        [],
        (face_count, slopes, owner, neighbour),
        scalars=1,
    )
    peer = lax.ppermute(pack, "faces", [(0, 1), (1, 0)])
    normal, link, order, last, lean, coupling = run(
        table_kernel,
        [
            ((3,) + faces, F32), ((2,) + faces, I32), ((2,) + faces, I32), ((3,) + faces, I32),
            ((2,) + faces, F32), ((3, tiles, LANES), F32),
        ],
        [
            wide(3), (6 * tiles, LANES), wide(3), faces,
            blocks(3), blocks(6), (6 * tiles, LANES), (4 * tiles, LANES),
        ],
        (pack, peer, flow),
    )
    pair, diag, source, predir, out1 = run(
        functools.partial(setup_kernel, shifts=shifts),
        [((2,) + faces, F32), ((5, tiles, LANES), F32), vec, vec, full_block],
        [stage, halo, (2, tiles, LANES), wide(2), blocks(2), blocks(4)],
        (in0, source, volume, normal, link, order, last, lean, coupling, send),
    )
    in1 = exchange(out1)
    work = [stage, halo, wide(BLOCK), vector, wide(BLOCK), blocks(BLOCK), blocks(2 * BLOCK)]
    fixed = (volume, normal, pair, link, order, last, diag, send)
    image, mimage, out2 = run(
        functools.partial(first_kernel, shifts=shifts), [vec, vec, full_block], work, (in1, predir, source) + fixed
    )
    in2 = exchange(out2)
    middle, premid, second, msecond, scales, out3 = run(
        functools.partial(second_kernel, shifts=shifts),
        [vec, vec, vec, vec, scale, full_block],
        work,
        (in1, in2, predir, mimage, image, source) + fixed,
    )
    in3 = exchange(out3)
    field, residual, preres, predir, image, mimage, scales, ghosts, out4 = run(
        functools.partial(third_kernel, shifts=shifts),
        [vec, vec, vec, vec, vec, vec, scale, ((lists, SUB, LANES), F32), full_block],
        work,
        (in1, in2, in3, scales, predir, mimage, premid, msecond, middle, second, source) + fixed,
    )
    in4 = exchange(out4)
    field, premid, middle, second, out5 = run(
        functools.partial(fourth_kernel, shifts=shifts),
        [vec, vec, vec, vec, sum_block],
        work[1:],
        (in4, scales, ghosts, field, residual, preres, predir, image, mimage) + fixed[:6],
    )
    in5 = lax.all_to_all(out5, "cells", 0, 0)
    field, residual = run(last_kernel, [flat_vec, flat_vec], [(2,) + vector], (in5, field, premid, middle, second))
    return (field, residual)


def solution(mesh):
    in_specs = (
        P(None, "cells"),
        P(None, "cells"),
        P("cells"),
        P(None, ("cells", "faces")),
        P(("cells", "faces")),
        P(("cells", "faces")),
        P(("cells", "faces")),
        P("cells", None),
        P("cells"),
    )
    out_specs = (P(None, "cells"), P(None, "cells"))
    return jax.shard_map(body, mesh=mesh, in_specs=in_specs, out_specs=out_specs, check_vma=False)
```

```python
import functools

import jax
import jax.numpy as jnp
from jax import lax
from jax.experimental import pallas as pl
from jax.experimental.pallas import tpu as pltpu
from jax.sharding import PartitionSpec as P

F32 = jnp.float32
I32 = jnp.int32
LANES = 128
SUB = 8
BLOCK = 4


def offsets(count):
    return [which + 1 for which in range(count)] + [-(which + 1) for which in range(count)]


ALONG_LANES = lax.GatherDimensionNumbers(
    offset_dims=(),
    collapsed_slice_dims=(1,),
    start_index_map=(1,),
    operand_batching_dims=(0,),
    start_indices_batching_dims=(0,),
)

ALONG_ROWS = lax.GatherDimensionNumbers(
    offset_dims=(),
    collapsed_slice_dims=(0,),
    start_index_map=(0,),
    operand_batching_dims=(1,),
    start_indices_batching_dims=(1,),
)


def pick(values, index):
    mode = lax.GatherScatterMode.PROMISE_IN_BOUNDS
    return lax.gather(values, index[..., None], ALONG_LANES, slice_sizes=(1, 1), mode=mode)


def pick_row(values, index):
    mode = lax.GatherScatterMode.PROMISE_IN_BOUNDS
    return lax.gather(values, index[..., None], ALONG_ROWS, slice_sizes=(1, 1), mode=mode)


def lane_ids(shape=(SUB, LANES)):
    return lax.broadcasted_iota(I32, shape, 1)


def sub_ids(shape=(SUB, LANES)):
    return lax.broadcasted_iota(I32, shape, 0)


def partition(distance, count):
    return lax.rem(lax.axis_index("cells") + distance + count, count)


def in_groups(tiles):
    return range(tiles // SUB)


def rows8(g):
    return slice(g * SUB, g * SUB + SUB)


def listed(row_of_tile, tiles, send_ref):
    row_at, lane_at = send_ref[0], send_ref[1]
    found = [jnp.zeros((SUB, LANES), F32) for _ in range(BLOCK)]
    for t in range(tiles):
        here = row_at == t
        for c in range(BLOCK):
            row = jnp.broadcast_to(row_of_tile(c, t), (SUB, LANES))
            found[c] = jnp.where(here, pick(row, lane_at), found[c])
    return found


def tiled_rows(ref):
    return lambda c, t: ref[c, t : t + 1, :]


def flat_rows(ref):
    return lambda c, t: ref[c : c + 1, t * LANES : (t + 1) * LANES]


def send_halo(found, stage_ref, out_ref, each):
    cores = lax.axis_size("faces")
    count = out_ref.shape[0] // cores
    halves = SUB // BLOCK
    for c in range(BLOCK):
        stage_ref[c * SUB : (c + 1) * SUB, :] = found[c]
    sign = 1 - 2 * lax.axis_index("faces")
    for j in range(each):
        place = partition(sign * (j + 1), count)
        for h in range(halves):
            rows = stage_ref[pl.ds(j * halves + h, BLOCK, stride=SUB), :]
            for core in range(cores):
                out_ref[place * cores + core, h * BLOCK : (h + 1) * BLOCK, :] = rows


def got_halo(in_ref, shifts):
    cores = lax.axis_size("faces")
    count = in_ref.shape[0] // cores
    each = len(shifts) // cores
    return [in_ref[partition(-shift, count) * cores + k // each] for k, shift in enumerate(shifts)]


def lay_halo(lists, halo_ref):
    total = len(lists)
    span = halo_ref.shape[0] // SUB
    for j in range(total + SUB - 1):
        halo_ref[pl.ds(j, SUB, stride=span), :] = lists[j % total]


def send_sums(sums, out_ref):
    rows = jnp.zeros((SUB, LANES), F32)
    sub = sub_ids()
    for i, acc in enumerate(sums):
        row = jnp.sum(acc, axis=0, keepdims=True)
        rows = jnp.where(sub == i, jnp.broadcast_to(row, (SUB, LANES)), rows)
    for d in range(out_ref.shape[0]):
        out_ref[d] = rows


def total_of(parts):
    while len(parts) > 1:
        parts = [a + b for a, b in zip(parts[::2], parts[1::2])] + parts[len(parts) & ~1 :]
    return jnp.sum(parts[0], axis=1, keepdims=True)


def got_sums(in_ref, each):
    cores = lax.axis_size("faces")
    count = in_ref.shape[0] // cores
    parts = []
    for q in range(count):
        ahead = partition(-q, count)
        core = jnp.where((ahead >= 1) & (ahead <= each), 1, 0)
        parts.append(in_ref[q * cores + core])
    return total_of(parts)


def spread(column, i):
    return jnp.broadcast_to(column[i : i + 1, :], (SUB, LANES))


def row_of(ref, i):
    return jnp.broadcast_to(ref[i : i + 1, :], (SUB, LANES))


def prefix_matrix():
    shape = (2 * LANES, LANES)
    upto = (lax.broadcasted_iota(I32, shape, 0) & (LANES - 1)) <= lax.broadcasted_iota(I32, shape, 1)
    return jnp.where(upto, 1.0, 0.0).astype(jnp.bfloat16)


def prefix_sums(values, matrix):
    high = values.astype(jnp.bfloat16)
    low = (values - high.astype(F32)).astype(jnp.bfloat16)
    return jnp.dot(jnp.concatenate([high, low], axis=1), matrix, preferred_element_type=F32)


def block_at(i):
    return slice(i * SUB, i * SUB + SUB)


def to_cells(flux_ref, order_ref, last_ref, here_ref, beside_ref, sort_ref, signs):
    parts = len(signs)
    tiles = here_ref.shape[1]
    rows = order_ref.shape[1]
    each = rows * parts
    sides = 1 if beside_ref is None else 2
    matrix = prefix_matrix()
    for g in in_groups(tiles):
        for side in range(sides):
            for r in range(rows):
                order = order_ref[side, r, rows8(g), :]
                for c in range(parts):
                    source = flux_ref[block_at(g * each + r * parts + c), :]
                    sort_ref[block_at((g * sides + side) * each + r * parts + c), :] = pick(source, order)
    for g in in_groups(tiles):
        at = slice(g * sides * each * SUB, (g + 1) * sides * each * SUB)
        sort_ref[at, :] = prefix_sums(sort_ref[at, :], matrix)
    lane = lane_ids()
    for g in in_groups(tiles):
        totals = []
        for side, of in ((0, 0), (1, 1), (1, 2))[: 2 * sides - 1]:
            acc = None
            for r in range(rows):
                last = last_ref[of, r, rows8(g), :]
                some = last >= 0
                at = last & (LANES - 1)
                got = [
                    jnp.where(some, pick(sort_ref[block_at((g * sides + side) * each + r * parts + c), :], at), 0.0)
                    for c in range(parts)
                ]
                acc = got if acc is None else [a + b for a, b in zip(acc, got)]
            totals.append(acc)
        for c in range(parts):
            if sides == 1:
                here_ref[c, rows8(g), :] = totals[0][c]
                continue
            owned, near, far = totals[0][c], totals[1][c], totals[2][c]
            here_ref[c, rows8(g), :] = owned + near if signs[c] > 0 else owned - near
            beside_ref[c, g * SUB + 1 : g * SUB + 1 + SUB, :] = jnp.where(lane == LANES - 1, near, far)
            sort_ref[block_at(g * sides * each + c), :] = far
    for g in in_groups(tiles):
        for c in range(parts):
            both = here_ref[c, rows8(g), :]
            here_ref[c, rows8(g), :] = both - jnp.where(lane == 0, 0.0, pltpu.roll(both, 1, 1))
            if sides == 2:
                at = slice(g * SUB + 1, g * SUB + 1 + SUB)
                before = pltpu.roll(beside_ref[c, at, :], 1, 1)
                beside_ref[c, at, :] = sort_ref[block_at(g * sides * each + c), :] - before
    if sides == 2:
        for c in range(parts):
            beside_ref[c, 0:1, :] = beside_ref[c, tiles : tiles + 1, :]


def local_values(wide_ref, link_ref, g, r, parts):
    owner, code = link_ref[0, r, rows8(g), :], link_ref[1, r, rows8(g), :]
    at = code & (LANES - 1)
    source = code >> 7
    own = [wide_ref[c, rows8(g), :] for c in range(parts)]
    left = [pick(v, owner) for v in own]
    right = [jnp.where(source == 0, pick(v, at), 0.0) for v in own]
    for c in range(parts):
        other = wide_ref[c, g * SUB + 1 : g * SUB + 1 + SUB, :]
        right[c] = jnp.where(source == 1, pick(other, at), right[c])
    return left, right


def halo_values(right, halo_ref, link_ref, g, r, lists):
    span = halo_ref.shape[0] // SUB
    code = link_ref[1, r, rows8(g), :]
    at = code & (LANES - 1)
    source = code >> 7
    first = (g * SUB) % lists
    right = list(right)
    for h in range(SUB // BLOCK):
        for c in range(len(right)):
            base = (h * BLOCK + c) * span + first
            right[c] = jnp.where(source == 2 + h, pick(halo_ref[base : base + SUB, :], at), right[c])
    return right


def widen(wide_ref, tiles, parts=BLOCK):
    for c in range(parts):
        wide_ref[c, tiles : tiles + 1, :] = wide_ref[c, 0:1, :]


def face_terms(normal_ref, pair_ref, g, r):
    normal = [normal_ref[i, r, rows8(g), :] for i in range(3)]
    return normal, pair_ref[0, r, rows8(g), :], pair_ref[1, r, rows8(g), :]


def put_flux(flux_ref, first, normal, speed, wave, both, gap):
    for i in range(3):
        flux_ref[block_at(first + i), :] = speed * both[i] + normal[i] * both[3] + wave * gap[i]
    last = normal[0] * both[0] + normal[1] * both[1] + normal[2] * both[2] + wave * gap[3]
    flux_ref[block_at(first + 3), :] = last


def face_part(wide_ref, halo_ref, faces, here_ref, beside_ref, flux_ref, sort_ref, lists):
    normal_ref, pair_ref, link_ref, order_ref, last_ref = faces
    rows = link_ref.shape[1]
    for g in in_groups(here_ref.shape[1]):
        for r in range(rows):
            left, right = local_values(wide_ref, link_ref, g, r, BLOCK)
            right = halo_values(right, halo_ref, link_ref, g, r, lists)
            normal, speed, wave = face_terms(normal_ref, pair_ref, g, r)
            both = [a + b for a, b in zip(left, right)]
            gap = [a - b for a, b in zip(left, right)]
            put_flux(flux_ref, (g * rows + r) * BLOCK, normal, speed, wave, both, gap)
    to_cells(flux_ref, order_ref, last_ref, here_ref, beside_ref, sort_ref, (-1,) * BLOCK)


def precondition(vector, diag_ref, g):
    inverse, n0, n1, n2, schur = [diag_ref[i, rows8(g), :] for i in range(5)]
    coupled = n0 * vector[0] + n1 * vector[1] + n2 * vector[2]
    pressure = (vector[3] - coupled * inverse) * schur
    return [(vector[i] - n * pressure) * inverse for i, n in enumerate((n0, n1, n2))] + [pressure]


def applied(g, volume_ref, wide_ref, here_ref, beside_ref):
    volume = volume_ref[rows8(g), :]
    return [
        volume * wide_ref[c, rows8(g), :] + (here_ref[c, rows8(g), :] - beside_ref[c, rows8(g), :])
        for c in range(BLOCK)
    ]


def cell(ref, g):
    return [ref[c, rows8(g), :] for c in range(BLOCK)]


def put(ref, g, vector):
    for c in range(BLOCK):
        ref[c, rows8(g), :] = vector[c]


def added(acc, a, b):
    for x, y in zip(a, b):
        acc = acc + x * y
    return acc


def zero():
    return jnp.zeros((SUB, LANES), F32)


def start_kernel(
    count_ref, used_any, flow_any, list_any, normal_any, owner_any, neighbour_any, source_any,
    pack_ref, out_ref, send_ref, flow_ref, source_ref,
    stage_ref, list_ref, used_ref, normal_ref, owner_ref, neighbour_ref, sems,
):
    pairs = (
        (used_any, used_ref), (flow_any, flow_ref), (list_any, list_ref), (normal_any, normal_ref),
        (owner_any, owner_ref), (neighbour_any, neighbour_ref), (source_any, source_ref),
    )
    copies = [pltpu.make_async_copy(a, b, sems.at[i]) for i, (a, b) in enumerate(pairs)]
    for copy in copies:
        copy.start()
    lists, width = list_ref.shape
    each = lists // 2
    halves = width // LANES
    sub = sub_ids()
    core = lax.axis_index("faces")
    used = jnp.zeros((SUB, LANES), I32)
    for copy in copies[:3]:
        copy.wait()
    for j in range(each):
        for h in range(halves):
            i = j * halves + h
            rows = [list_ref[k : k + 1, h * LANES : (h + 1) * LANES] for k in (j, each + j)]
            stage_ref[i : i + 1, :] = jnp.where(core == 0, *rows).astype(F32)
            used = jnp.where(sub == i, used_ref[core * each + j] - h * LANES, used)
    cells = stage_ref[0:SUB, :].astype(I32)
    alive = (lane_ids() < used) & (sub < each * halves)
    send_ref[0] = jnp.where(alive, cells >> 7, -1)
    send_ref[1] = jnp.where(alive, cells & (LANES - 1), 0)
    tiles = flow_ref.shape[1] // LANES
    send_halo(listed(flat_rows(flow_ref), tiles, send_ref), stage_ref, out_ref, each)
    for copy in copies[3:]:
        copy.wait()
    pack_faces(count_ref, normal_ref, owner_ref, neighbour_ref, pack_ref, lists, width, tiles * LANES)


def pack_faces(count_ref, normal_ref, owner_ref, neighbour_ref, pack_ref, lists, width, cells_here):
    tiles = cells_here // LANES
    pairs = tiles // 2
    shape = (pairs, LANES)
    pair, lane = sub_ids(shape), lane_ids(shape)
    for i in range(3 * pairs):
        for c in range(3):
            at = (i % 3) * pairs + i // 3
            pack_ref[c, at : at + 1, :] = normal_ref[c : c + 1, i * LANES : (i + 1) * LANES]
    for q in range(3):
        at = slice(q * pairs, (q + 1) * pairs)
        tile = 2 * pair + (0, jnp.where(lane >= LANES // 2, 1, 0), 1)[q]
        live = (3 * pair + q) * LANES + lane < count_ref[0]
        owner = owner_ref[pl.ds(q, pairs, stride=3), :] - tile * LANES
        neighbour = neighbour_ref[pl.ds(q, pairs, stride=3), :]
        near = (neighbour - tile * LANES) & (cells_here - 1)
        far = neighbour - cells_here - lax.rem(tile, lists) * width + 2 * LANES
        code = jnp.where(neighbour < cells_here, near, far)
        pack_ref[3, at, :] = (owner * 512 + code).astype(F32)
        for c in range(3):
            pack_ref[c, at, :] = jnp.where(live, 0.5 * pack_ref[c, at, :], 0.0)


def sorted_columns(x):
    sub = sub_ids()
    for k in range(1, 8):
        flip = None
        if 4 <= k <= 6:
            flip = ((sub >> (k - 4)) & 1) == 1
            x = [jnp.where(flip, -a, a) for a in x]
        for j in range(k - 1, -1, -1):
            if j < 4:
                new = list(x)
                for v in range(16):
                    w = v | (1 << j)
                    if w != v:
                        low, high = jnp.minimum(x[v], x[w]), jnp.maximum(x[v], x[w])
                        down = k < 4 and (v >> k) & 1
                        new[v], new[w] = (high, low) if down else (low, high)
                x = new
            else:
                d = 1 << (j - 4)
                first = ((sub >> (j - 4)) & 1) == 0
                x = [
                    jnp.where(
                        first,
                        jnp.minimum(a, pltpu.roll(a, SUB - d, 0)),
                        jnp.maximum(a, pltpu.roll(a, d, 0)),
                    )
                    for a in x
                ]
        if flip is not None:
            x = [jnp.where(flip, -a, a) for a in x]
    return x


def counts_below(x, first):
    sub = sub_ids()
    rows = []
    heads = [jnp.broadcast_to(x[15][s : s + 1, :], (SUB, LANES)) for s in range(SUB)]
    for w in range(LANES // SUB):
        bound = ((sub + (first + w * SUB + 1)) * LANES).astype(F32)
        block = jnp.zeros((SUB, LANES), I32)
        for s in range(SUB):
            block = jnp.where(heads[s] < bound, s + 1, block)
        at = jnp.minimum(block, SUB - 1)
        inside = jnp.zeros((SUB, LANES), I32)
        for v in range(15):
            inside = jnp.where(pick_row(x[v], at) < bound, v + 1, inside)
        rows.append((block * 16 + jnp.where(block < SUB, inside, 0)).astype(F32))
    return rows


def sort_rows(key_ref, lower_ref, upper_ref):
    lane = lane_ids()
    back = 8 * (lane & 15) + (lane >> 4)
    skip = lower_ref.shape[0] - upper_ref.shape[0]
    for b in range(key_ref.shape[0] // LANES):
        at = slice(b * LANES, (b + 1) * LANES)
        turned = jnp.transpose(key_ref[at, :])
        x = sorted_columns([turned[v * SUB : (v + 1) * SUB, :] for v in range(16)])
        turned = jnp.transpose(jnp.concatenate(x, axis=0))
        for v in range(16):
            row = b * LANES + v * SUB
            key_ref[row : row + SUB, :] = pick(turned[v * SUB : (v + 1) * SUB, :], back)
        lower_ref[at, :] = jnp.transpose(jnp.concatenate(counts_below(x, 0), axis=0))
        if b * LANES >= skip:
            at = slice(b * LANES - skip, (b + 1) * LANES - skip)
            upper_ref[at, :] = jnp.transpose(jnp.concatenate(counts_below(x, LANES), axis=0))


def table_kernel(
    mine_ref, peer_ref, flow_ref,
    normal_ref, link_ref, order_ref, last_ref, lean_ref, coupling_ref,
    wide_ref, key_ref, beside_ref, joint_ref, flux_ref, sort_ref, lower_ref, upper_ref,
):
    tiles = normal_ref.shape[2]
    pairs = tiles // 2
    swapped = lax.axis_index("faces") == 1
    lane = lane_ids((pairs, LANES))
    half = LANES // 2
    for i in range(4):
        part = []
        for q in range(3):
            mine = mine_ref[i, q * pairs : (q + 1) * pairs, :]
            peer = peer_ref[i, q * pairs : (q + 1) * pairs, :]
            part.append((jnp.where(swapped, peer, mine), jnp.where(swapped, mine, peer)))
        (a0, b0), (a1, b1), (a2, b2) = part
        even = (a0, b0, jnp.where(lane < half, a1, pltpu.roll(b1, half, 1)))
        odd = (a2, b2, jnp.where(lane < half, pltpu.roll(a1, half, 1), b1))
        for r in range(3):
            target = normal_ref.at[i, r] if i < 3 else joint_ref.at[r]
            target[pl.ds(0, pairs, stride=2), :] = even[r]
            target[pl.ds(1, pairs, stride=2), :] = odd[r]
    lane = lane_ids()
    for r in range(3):
        for g in in_groups(tiles):
            joint = joint_ref[r, rows8(g), :].astype(I32)
            owner, code = joint >> 9, joint & 511
            link_ref[0, r, rows8(g), :] = owner
            link_ref[1, r, rows8(g), :] = code
            at = r * tiles + g * SUB
            key_ref[at : at + SUB, :] = (owner * LANES + lane).astype(F32)
            at += 3 * tiles
            key_ref[at : at + SUB, :] = (jnp.minimum(code, 256) * LANES + lane).astype(F32)
    sort_rows(key_ref, lower_ref, upper_ref)
    skip = lower_ref.shape[0] - upper_ref.shape[0]
    for r in range(3):
        for g in in_groups(tiles):
            at = r * tiles + g * SUB
            owned = key_ref[at : at + SUB, :]
            near = key_ref[at + 3 * tiles : at + 3 * tiles + SUB, :]
            order_ref[0, r, rows8(g), :] = owned.astype(I32) & (LANES - 1)
            order_ref[1, r, rows8(g), :] = near.astype(I32) & (LANES - 1)
            near = at + 3 * tiles
            for i, count in enumerate(
                (lower_ref[at : at + SUB, :], lower_ref[near : near + SUB, :], upper_ref[near - skip : near - skip + SUB, :])
            ):
                last_ref[i, r, rows8(g), :] = count.astype(I32) - 1
    for t in range(tiles):
        for c in range(3):
            wide_ref[c, t : t + 1, :] = flow_ref[c : c + 1, t * LANES : (t + 1) * LANES]
    widen(wide_ref, tiles, 3)
    for g in in_groups(tiles):
        for r in range(3):
            left, right = local_values(wide_ref, link_ref, g, r, 3)
            lean, size = zero(), zero()
            for i in range(3):
                normal = normal_ref[i, r, rows8(g), :]
                lean = lean + normal * (left[i] + right[i])
                size = size + normal * normal
                flux_ref[block_at((g * 3 + r) * 3 + i), :] = normal
            lean_ref[0, r, rows8(g), :] = lean
            lean_ref[1, r, rows8(g), :] = 2.0 * jnp.sqrt(size)
    to_cells(flux_ref, order_ref, last_ref, coupling_ref, beside_ref, sort_ref, (-1, -1, -1))
    for g in in_groups(tiles):
        for i in range(3):
            coupling_ref[i, rows8(g), :] = coupling_ref[i, rows8(g), :] - beside_ref[i, rows8(g), :]


def setup_kernel(
    in_ref, source_ref, volume_ref, normal_ref, link_ref, order_ref, last_ref, lean_ref, coupling_ref, send_ref,
    pair_ref, diag_ref, source_out, pre_ref, out_ref,
    stage_ref, halo_ref, here_ref, beside_ref, flux_ref, sort_ref, *, shifts,
):
    tiles = volume_ref.shape[0]
    lay_halo(got_halo(in_ref, shifts), halo_ref)
    for g in in_groups(tiles):
        for r in range(3):
            right = halo_values([zero() for _ in range(3)], halo_ref, link_ref, g, r, len(shifts))
            speed = lean_ref[0, r, rows8(g), :]
            for i in range(3):
                speed = speed + normal_ref[i, r, rows8(g), :] * right[i]
            wave = 0.5 * jnp.abs(speed) + lean_ref[1, r, rows8(g), :]
            for i, term in enumerate((0.5 * speed, wave)):
                pair_ref[i, r, rows8(g), :] = term
                flux_ref[block_at((g * 3 + r) * 2 + i), :] = term
    to_cells(flux_ref, order_ref, last_ref, here_ref, beside_ref, sort_ref, (-1, 1))
    for t in range(tiles):
        for c in range(BLOCK):
            source_out[c, t : t + 1, :] = source_ref[c : c + 1, t * LANES : (t + 1) * LANES]
    for g in in_groups(tiles):
        n0, n1, n2 = [coupling_ref[i, rows8(g), :] for i in range(3)]
        speed = here_ref[0, rows8(g), :] - beside_ref[0, rows8(g), :]
        pressure_diag = volume_ref[rows8(g), :] + (here_ref[1, rows8(g), :] + beside_ref[1, rows8(g), :])
        inverse = 1.0 / (pressure_diag + speed)
        schur = pressure_diag - (n0 * n0 + n1 * n1 + n2 * n2) * inverse
        for i, value in enumerate((inverse, n0, n1, n2, 1.0 / schur)):
            diag_ref[i, rows8(g), :] = value
        put(pre_ref, g, precondition(cell(source_out, g), diag_ref, g))
    send_halo(listed(tiled_rows(pre_ref), tiles, send_ref), stage_ref, out_ref, len(shifts) // 2)


def combine(scales, vectors):
    out = []
    for parts in zip(*vectors):
        acc = None
        for scale, part in zip(scales, parts):
            term = part if scale is None else scale * part
            acc = term if acc is None else acc + term
        out.append(acc)
    return out


def apply_faces(in_ref, vector_ref, faces, here_ref, beside_ref, wide_ref, halo_ref, flux_ref, sort_ref, shifts):
    tiles = here_ref.shape[1]
    for g in in_groups(tiles):
        put(wide_ref, g, cell(vector_ref, g))
    widen(wide_ref, tiles)
    lay_halo(got_halo(in_ref, shifts), halo_ref)
    face_part(wide_ref, halo_ref, faces, here_ref, beside_ref, flux_ref, sort_ref, len(shifts))


def flatten(out_ref, ref, g):
    for t in range(g * SUB, g * SUB + SUB):
        for c in range(BLOCK):
            out_ref[c : c + 1, t * LANES : (t + 1) * LANES] = ref[c, t : t + 1, :]


def first_kernel(
    in_ref, vector_ref, source_ref, diag_ref, send_ref, volume_ref, *refs, shifts,
):
    faces, (image_ref, mimage_ref, out_ref), (stage_ref, *work) = refs[:5], refs[5:8], refs[8:]
    here_ref, beside_ref, wide_ref = work[:3]
    tiles = here_ref.shape[1]
    apply_faces(in_ref, vector_ref, faces, *work, shifts)
    product, rho = zero(), zero()
    for g in in_groups(tiles):
        image = applied(g, volume_ref, wide_ref, here_ref, beside_ref)
        source = cell(source_ref, g)
        product = added(product, source, image)
        rho = added(rho, source, source)
        put(image_ref, g, image)
        put(mimage_ref, g, precondition(image, diag_ref, g))
    send_sums((product, rho), out_ref)
    send_halo(listed(tiled_rows(mimage_ref), tiles, send_ref), stage_ref, out_ref, len(shifts) // 2)


def second_kernel(
    in_ref, vector_ref, source_ref, image_ref, diag_ref, send_ref, volume_ref, *refs, shifts,
):
    faces, outs, (stage_ref, *work) = refs[:5], refs[5:11], refs[11:]
    aimage_ref, second_ref, msecond_ref, middle_ref, scale_ref, out_ref = outs
    here_ref, beside_ref, wide_ref = work[:3]
    tiles = here_ref.shape[1]
    sums = got_sums(in_ref, len(shifts) // 2)
    rho = spread(sums, 1)
    alpha = rho / spread(sums, 0)
    scale_ref[0:1, :] = alpha[0:1, :]
    scale_ref[1:2, :] = rho[0:1, :]
    apply_faces(in_ref, vector_ref, faces, *work, shifts)
    products = [zero() for _ in range(4)]
    for g in in_groups(tiles):
        image, source = cell(image_ref, g), cell(source_ref, g)
        aimage = applied(g, volume_ref, wide_ref, here_ref, beside_ref)
        second = combine((None, -alpha), (image, aimage))
        middle = combine((None, -alpha), (source, image))
        put(aimage_ref, g, aimage)
        put(second_ref, g, second)
        put(middle_ref, g, middle)
        put(msecond_ref, g, precondition(second, diag_ref, g))
        for i, (a, b) in enumerate(((second, middle), (second, second), (source, middle), (source, second))):
            products[i] = added(products[i], a, b)
    send_sums(products, out_ref)
    send_halo(listed(tiled_rows(msecond_ref), tiles, send_ref), stage_ref, out_ref, len(shifts) // 2)


def third_kernel(
    in_ref, vector_ref, source_ref, image_ref, aimage_ref, second_ref, old_ref, diag_ref, send_ref, volume_ref, *refs, shifts,
):
    faces, outs, (stage_ref, *work) = refs[:5], refs[5:10], refs[10:]
    apreres_ref, next_ref, mnext_ref, scale_ref, out_ref = outs
    here_ref, beside_ref, wide_ref = work[:3]
    tiles = here_ref.shape[1]
    sums = got_sums(in_ref, len(shifts) // 2)
    alpha, rho = row_of(old_ref, 0), row_of(old_ref, 1)
    omega = spread(sums, 0) / spread(sums, 1)
    rho_next = spread(sums, 2) - omega * spread(sums, 3)
    beta = rho_next / rho * (alpha / omega)
    for i, value in enumerate((alpha, rho_next, omega, beta)):
        scale_ref[i : i + 1, :] = value[0:1, :]
    apply_faces(in_ref, vector_ref, faces, *work, shifts)
    drop = -beta * omega
    product = zero()
    for g in in_groups(tiles):
        asecond = applied(g, volume_ref, wide_ref, here_ref, beside_ref)
        apreres = combine((None, -omega), (cell(second_ref, g), asecond))
        image = combine((None, beta, drop), (apreres, cell(image_ref, g), cell(aimage_ref, g)))
        product = added(product, cell(source_ref, g), image)
        put(apreres_ref, g, apreres)
        put(next_ref, g, image)
        put(mnext_ref, g, precondition(image, diag_ref, g))
    send_sums((product,), out_ref)
    send_halo(listed(tiled_rows(mnext_ref), tiles, send_ref), stage_ref, out_ref, len(shifts) // 2)


def fourth_kernel(
    in_ref, vector_ref, apreres_ref, image_ref, middle_ref, second_ref, pre_ref, mimage_ref, msecond_ref, old_ref,
    volume_ref, *refs, shifts,
):
    faces, outs, (stage_ref, *work) = refs[:5], refs[5:10], refs[10:]
    field_out, premid_out, middle_out, second_out, out_ref = outs
    here_ref, beside_ref, wide_ref = work[:3]
    tiles = here_ref.shape[1]
    alpha2 = row_of(old_ref, 1) / spread(got_sums(in_ref, len(shifts) // 2), 0)
    alpha, omega, beta = [row_of(old_ref, i) for i in (0, 2, 3)]
    apply_faces(in_ref, vector_ref, faces, *work, shifts)
    cross, square = zero(), zero()
    for g in in_groups(tiles):
        pre, mimage = cell(pre_ref, g), cell(mimage_ref, g)
        premid = combine((None, -alpha), (pre, mimage))
        preres = combine((None, -omega), (premid, cell(msecond_ref, g)))
        predir = combine((None, beta, -beta * omega), (preres, pre, mimage))
        put(stage_ref.at[0], g, combine((alpha, omega, alpha2), (pre, premid, predir)))
        put(stage_ref.at[1], g, combine((None, -alpha2), (preres, cell(vector_ref, g))))
        flatten(field_out, stage_ref.at[0], g)
        flatten(premid_out, stage_ref.at[1], g)
        aimage = applied(g, volume_ref, wide_ref, here_ref, beside_ref)
        second = combine((None, -alpha2), (cell(apreres_ref, g), aimage))
        middle = combine((None, -omega, -alpha2), (cell(middle_ref, g), cell(second_ref, g), cell(image_ref, g)))
        put(stage_ref.at[2], g, second)
        put(stage_ref.at[3], g, middle)
        flatten(second_out, stage_ref.at[2], g)
        flatten(middle_out, stage_ref.at[3], g)
        cross = added(cross, second, middle)
        square = added(square, second, second)
    send_sums((cross, square), out_ref)


def last_kernel(in_ref, field_ref, premid_ref, middle_ref, second_ref, field_out, residual_out):
    sums = total_of([in_ref[d] for d in range(0, in_ref.shape[0], lax.axis_size("faces"))])
    omega = sums[0:1, :] / sums[1:2, :]
    field_out[...] = field_ref[...] + omega * premid_ref[...]
    residual_out[...] = middle_ref[...] - omega * second_ref[...]


def run(kernel, outs, scratch, args, scalars=0, away=0):
    vmem = pl.BlockSpec(memory_space=pltpu.VMEM)
    smem = pl.BlockSpec(memory_space=pltpu.SMEM)
    hbm = pl.BlockSpec(memory_space=pltpu.HBM)
    far = range(scalars, scalars + away)
    args = [pltpu.with_memory_space_constraint(a, pltpu.HBM) if i in far else a for i, a in enumerate(args)]
    return pl.pallas_call(
        kernel,
        out_shape=[jax.ShapeDtypeStruct(shape, dtype) for shape, dtype in outs],
        in_specs=[smem] * scalars + [hbm] * away + [vmem] * (len(args) - scalars - away),
        out_specs=[vmem] * len(outs),
        scratch_shapes=[pltpu.VMEM(shape, F32) if isinstance(shape, tuple) else shape for shape in scratch],
        compiler_params=pltpu.CompilerParams(vmem_limit_bytes=24 << 20),
    )(*args)


def exchange(block):
    return lax.all_to_all(block, ("cells", "faces"), 0, 0)


def body(
    flow_state,
    source_term,
    volume_rate,
    face_normal,
    face_owner,
    face_neighbour,
    face_count,
    send_list,
    halo_count,
):
    count = lax.axis_size("cells")
    cells_here = flow_state.shape[1]
    lists, width = send_list.shape
    tiles = cells_here // LANES
    per_tile = face_owner.shape[0] // tiles
    shifts = offsets(lists // 2)
    assert per_tile * 2 == 3 * LANES and lax.axis_size("faces") == 2
    assert width == 2 * LANES and count > lists and lists % 2 == 0 and lists <= SUB
    assert tiles % SUB == 0 and cells_here & (cells_here - 1) == 0
    rows = 3
    span = -(-(lists + SUB - 1) // SUB) * SUB
    vector = (BLOCK, tiles, LANES)
    vec = (vector, F32)
    faces = (rows, tiles, LANES)
    scale = ((SUB, LANES), F32)
    full_block = ((2 * count, SUB, LANES), F32)
    flat_vec = (flow_state.shape, F32)
    stage = (SUB * SUB, LANES)
    halo = (SUB * span, LANES)
    flat = face_owner.shape[0] // LANES
    volume = volume_rate.reshape(tiles, LANES)

    def wide(parts):
        return (parts, tiles + SUB, LANES)

    def blocks(parts):
        return (rows * parts * tiles, LANES)

    ints = pltpu.VMEM((flat, LANES), I32)
    pack, out0, send, flow, source = run(
        start_kernel,
        [((4, flat, LANES), F32), full_block, ((2, SUB, LANES), I32), flat_vec, flat_vec],
        [
            stage, pltpu.VMEM(send_list.shape, I32), pltpu.SMEM((lists,), I32),
            face_normal.shape, ints, ints, pltpu.SemaphoreType.DMA((7,)),
        ],
        (
            face_count, halo_count, flow_state, send_list, face_normal,
            face_owner.reshape(flat, LANES), face_neighbour.reshape(flat, LANES), source_term,
        ),
        scalars=1,
        away=7,
    )
    in0 = exchange(out0)
    peer = lax.ppermute(pack, "faces", [(0, 1), (1, 0)])
    normal, link, order, last, lean, coupling = run(
        table_kernel,
        [
            ((3,) + faces, F32), ((2,) + faces, I32), ((2,) + faces, I32), ((3,) + faces, I32),
            ((2,) + faces, F32), ((3, tiles, LANES), F32),
        ],
        [
            wide(3), (6 * tiles, LANES), wide(3), faces,
            blocks(3), blocks(6), (6 * tiles, LANES), (4 * tiles, LANES),
        ],
        (pack, peer, flow),
    )
    pair, diag, source, predir, out1 = run(
        functools.partial(setup_kernel, shifts=shifts),
        [((2,) + faces, F32), ((5, tiles, LANES), F32), vec, vec, full_block],
        [stage, halo, (2, tiles, LANES), wide(2), blocks(2), blocks(4)],
        (in0, source, volume, normal, link, order, last, lean, coupling, send),
    )
    tables = (volume, normal, pair, link, order, last)
    scratch = [vector, wide(BLOCK), wide(BLOCK), halo, blocks(BLOCK), blocks(2 * BLOCK)]

    def step(kernel, outs, args, stage=stage):
        return run(functools.partial(kernel, shifts=shifts), outs, [stage] + scratch, args + tables)

    in1 = exchange(out1)
    image, mimage, out2 = step(first_kernel, [vec, vec, full_block], (in1, predir, source, diag, send))
    in2 = exchange(out2)
    aimage, second, msecond, middle, scales, out3 = step(
        second_kernel, [vec, vec, vec, vec, scale, full_block], (in2, mimage, source, image, diag, send)
    )
    in3 = exchange(out3)
    apreres, image, mnext, scales, out4 = step(
        third_kernel,
        [vec, vec, vec, scale, full_block],
        (in3, msecond, source, image, aimage, second, scales, diag, send),
    )
    in4 = exchange(out4)
    field, premid, middle, second, out5 = step(
        fourth_kernel,
        [flat_vec] * 4 + [full_block],
        (in4, mnext, apreres, image, middle, second, predir, mimage, msecond, scales),
        (4,) + vector,
    )
    in5 = exchange(out5)
    field, residual = run(last_kernel, [flat_vec, flat_vec], [], (in5, field, premid, middle, second))
    return (field, residual)


def solution(mesh):
    in_specs = (
        P(None, "cells"),
        P(None, "cells"),
        P("cells"),
        P(None, ("cells", "faces")),
        P(("cells", "faces")),
        P(("cells", "faces")),
        P(("cells", "faces")),
        P("cells", None),
        P("cells"),
    )
    out_specs = (P(None, "cells"), P(None, "cells"))
    return jax.shard_map(body, mesh=mesh, in_specs=in_specs, out_specs=out_specs, check_vma=False)
```

```python
import functools

import jax
import jax.numpy as jnp
from jax import lax
from jax.experimental import pallas as pl
from jax.experimental.pallas import tpu as pltpu
from jax.sharding import PartitionSpec as P

F32 = jnp.float32
I32 = jnp.int32
LANES = 128
SUB = 8
BLOCK = 4


def offsets(count):
    return [which + 1 for which in range(count)] + [-(which + 1) for which in range(count)]


ALONG_LANES = lax.GatherDimensionNumbers(
    offset_dims=(),
    collapsed_slice_dims=(1,),
    start_index_map=(1,),
    operand_batching_dims=(0,),
    start_indices_batching_dims=(0,),
)

ALONG_ROWS = lax.GatherDimensionNumbers(
    offset_dims=(),
    collapsed_slice_dims=(0,),
    start_index_map=(0,),
    operand_batching_dims=(1,),
    start_indices_batching_dims=(1,),
)


def pick(values, index):
    mode = lax.GatherScatterMode.PROMISE_IN_BOUNDS
    return lax.gather(values, index[..., None], ALONG_LANES, slice_sizes=(1, 1), mode=mode)


def pick_row(values, index):
    mode = lax.GatherScatterMode.PROMISE_IN_BOUNDS
    return lax.gather(values, index[..., None], ALONG_ROWS, slice_sizes=(1, 1), mode=mode)


def lane_ids(shape=(SUB, LANES)):
    return lax.broadcasted_iota(I32, shape, 1)


def sub_ids(shape=(SUB, LANES)):
    return lax.broadcasted_iota(I32, shape, 0)


def partition(distance, count):
    return lax.rem(lax.axis_index("cells") + distance + count, count)


def in_groups(tiles):
    return range(tiles // SUB)


def rows8(g):
    return slice(g * SUB, g * SUB + SUB)


def listed(row_of_tile, tiles, send_ref, per):
    packed = send_ref.shape[0] // 2
    sub = sub_ids()
    found = []
    for v in range(packed):
        row_at, lane_at = send_ref[v], send_ref[packed + v]
        low, high = [min(n // per, BLOCK - 1) for n in (v * SUB, v * SUB + SUB - 1)]
        assert high - low <= 1
        values = jnp.zeros((SUB, LANES), F32)
        for t in range(tiles):
            row = jnp.broadcast_to(row_of_tile(low, t), (SUB, LANES))
            if high > low:
                other = jnp.broadcast_to(row_of_tile(high, t), (SUB, LANES))
                row = jnp.where(sub < high * per - v * SUB, row, other)
            values = jnp.where(row_at == t, pick(row, lane_at), values)
        found.append(values)
    return found


def tiled_rows(ref):
    return lambda c, t: ref[c, t : t + 1, :]


def flat_rows(ref):
    return lambda c, t: ref[c : c + 1, t * LANES : (t + 1) * LANES]


def send_halo(found, stage_ref, out_ref, each):
    cores = lax.axis_size("faces")
    count = out_ref.shape[0] // cores
    halves = SUB // BLOCK
    for v, values in enumerate(found):
        stage_ref[v * SUB : (v + 1) * SUB, :] = values
    sign = 1 - 2 * lax.axis_index("faces")
    for j in range(each):
        place = partition(sign * (j + 1), count)
        for h in range(halves):
            rows = stage_ref[pl.ds(j * halves + h, BLOCK, stride=each * halves), :]
            for core in range(cores):
                out_ref[place * cores + core, h * BLOCK : (h + 1) * BLOCK, :] = rows


def got_halo(in_ref, shifts):
    cores = lax.axis_size("faces")
    count = in_ref.shape[0] // cores
    each = len(shifts) // cores
    return [in_ref[partition(-shift, count) * cores + k // each] for k, shift in enumerate(shifts)]


def lay_halo(lists, halo_ref):
    total = len(lists)
    span = halo_ref.shape[0] // SUB
    for j in range(total + SUB - 1):
        halo_ref[pl.ds(j, SUB, stride=span), :] = lists[j % total]


def send_sums(sums, out_ref):
    rows = jnp.zeros((SUB, LANES), F32)
    sub = sub_ids()
    for i, acc in enumerate(sums):
        row = jnp.sum(acc, axis=0, keepdims=True)
        rows = jnp.where(sub == i, jnp.broadcast_to(row, (SUB, LANES)), rows)
    for d in range(out_ref.shape[0]):
        out_ref[d] = rows


def total_of(parts):
    while len(parts) > 1:
        parts = [a + b for a, b in zip(parts[::2], parts[1::2])] + parts[len(parts) & ~1 :]
    return jnp.sum(parts[0], axis=1, keepdims=True)


def got_sums(in_ref, each):
    cores = lax.axis_size("faces")
    count = in_ref.shape[0] // cores
    parts = []
    for q in range(count):
        ahead = partition(-q, count)
        core = jnp.where((ahead >= 1) & (ahead <= each), 1, 0)
        parts.append(in_ref[q * cores + core])
    return total_of(parts)


def spread(column, i):
    return jnp.broadcast_to(column[i : i + 1, :], (SUB, LANES))


def row_of(ref, i):
    return jnp.broadcast_to(ref[i : i + 1, :], (SUB, LANES))


def prefix_matrix():
    shape = (2 * LANES, LANES)
    upto = (lax.broadcasted_iota(I32, shape, 0) & (LANES - 1)) <= lax.broadcasted_iota(I32, shape, 1)
    return jnp.where(upto, 1.0, 0.0).astype(jnp.bfloat16)


def prefix_sums(values, matrix):
    high = values.astype(jnp.bfloat16)
    low = (values - high.astype(F32)).astype(jnp.bfloat16)
    return jnp.dot(jnp.concatenate([high, low], axis=1), matrix, preferred_element_type=F32)


def block_at(i):
    return slice(i * SUB, i * SUB + SUB)


def to_cells(flux_ref, order_ref, last_ref, here_ref, beside_ref, sort_ref, signs):
    parts = len(signs)
    tiles = here_ref.shape[1]
    rows = order_ref.shape[1]
    each = rows * parts
    sides = 1 if beside_ref is None else 2
    matrix = prefix_matrix()
    for g in in_groups(tiles):
        for side in range(sides):
            for r in range(rows):
                order = order_ref[side, r, rows8(g), :]
                for c in range(parts):
                    source = flux_ref[block_at(g * each + r * parts + c), :]
                    sort_ref[block_at((g * sides + side) * each + r * parts + c), :] = pick(source, order)
    for g in in_groups(tiles):
        at = slice(g * sides * each * SUB, (g + 1) * sides * each * SUB)
        sort_ref[at, :] = prefix_sums(sort_ref[at, :], matrix)
    lane = lane_ids()
    for g in in_groups(tiles):
        totals = []
        for side, of in ((0, 0), (1, 1), (1, 2))[: 2 * sides - 1]:
            acc = None
            for r in range(rows):
                last = last_ref[of, r, rows8(g), :]
                some = last >= 0
                at = last & (LANES - 1)
                got = [
                    jnp.where(some, pick(sort_ref[block_at((g * sides + side) * each + r * parts + c), :], at), 0.0)
                    for c in range(parts)
                ]
                acc = got if acc is None else [a + b for a, b in zip(acc, got)]
            totals.append(acc)
        for c in range(parts):
            if sides == 1:
                here_ref[c, rows8(g), :] = totals[0][c]
                continue
            owned, near, far = totals[0][c], totals[1][c], totals[2][c]
            here_ref[c, rows8(g), :] = owned + near if signs[c] > 0 else owned - near
            beside_ref[c, g * SUB + 1 : g * SUB + 1 + SUB, :] = jnp.where(lane == LANES - 1, near, far)
            sort_ref[block_at(g * sides * each + c), :] = far
    for g in in_groups(tiles):
        for c in range(parts):
            both = here_ref[c, rows8(g), :]
            here_ref[c, rows8(g), :] = both - jnp.where(lane == 0, 0.0, pltpu.roll(both, 1, 1))
            if sides == 2:
                at = slice(g * SUB + 1, g * SUB + 1 + SUB)
                before = pltpu.roll(beside_ref[c, at, :], 1, 1)
                beside_ref[c, at, :] = sort_ref[block_at(g * sides * each + c), :] - before
    if sides == 2:
        for c in range(parts):
            beside_ref[c, 0:1, :] = beside_ref[c, tiles : tiles + 1, :]


def local_values(wide_ref, link_ref, g, r, parts):
    owner, code = link_ref[0, r, rows8(g), :], link_ref[1, r, rows8(g), :]
    at = code & (LANES - 1)
    source = code >> 7
    own = [wide_ref[c, rows8(g), :] for c in range(parts)]
    left = [pick(v, owner) for v in own]
    right = [jnp.where(source == 0, pick(v, at), 0.0) for v in own]
    for c in range(parts):
        other = wide_ref[c, g * SUB + 1 : g * SUB + 1 + SUB, :]
        right[c] = jnp.where(source == 1, pick(other, at), right[c])
    return left, right


def halo_values(right, halo_ref, link_ref, g, r, lists):
    span = halo_ref.shape[0] // SUB
    code = link_ref[1, r, rows8(g), :]
    at = code & (LANES - 1)
    source = code >> 7
    first = (g * SUB) % lists
    right = list(right)
    for h in range(SUB // BLOCK):
        for c in range(len(right)):
            base = (h * BLOCK + c) * span + first
            right[c] = jnp.where(source == 2 + h, pick(halo_ref[base : base + SUB, :], at), right[c])
    return right


def widen(wide_ref, tiles, parts=BLOCK):
    for c in range(parts):
        wide_ref[c, tiles : tiles + 1, :] = wide_ref[c, 0:1, :]


def face_terms(normal_ref, pair_ref, g, r):
    normal = [normal_ref[i, r, rows8(g), :] for i in range(3)]
    return normal, pair_ref[0, r, rows8(g), :], pair_ref[1, r, rows8(g), :]


def put_flux(flux_ref, first, normal, speed, wave, both, gap):
    for i in range(3):
        flux_ref[block_at(first + i), :] = speed * both[i] + normal[i] * both[3] + wave * gap[i]
    last = normal[0] * both[0] + normal[1] * both[1] + normal[2] * both[2] + wave * gap[3]
    flux_ref[block_at(first + 3), :] = last


def face_part(wide_ref, halo_ref, faces, here_ref, beside_ref, flux_ref, sort_ref, lists):
    normal_ref, pair_ref, link_ref, order_ref, last_ref = faces
    rows = link_ref.shape[1]
    for g in in_groups(here_ref.shape[1]):
        for r in range(rows):
            left, right = local_values(wide_ref, link_ref, g, r, BLOCK)
            right = halo_values(right, halo_ref, link_ref, g, r, lists)
            normal, speed, wave = face_terms(normal_ref, pair_ref, g, r)
            both = [a + b for a, b in zip(left, right)]
            gap = [a - b for a, b in zip(left, right)]
            put_flux(flux_ref, (g * rows + r) * BLOCK, normal, speed, wave, both, gap)
    to_cells(flux_ref, order_ref, last_ref, here_ref, beside_ref, sort_ref, (-1,) * BLOCK)


def precondition(vector, diag_ref, g):
    inverse, n0, n1, n2, schur = [diag_ref[i, rows8(g), :] for i in range(5)]
    coupled = n0 * vector[0] + n1 * vector[1] + n2 * vector[2]
    pressure = (vector[3] - coupled * inverse) * schur
    return [(vector[i] - n * pressure) * inverse for i, n in enumerate((n0, n1, n2))] + [pressure]


def applied(g, volume_ref, wide_ref, here_ref, beside_ref):
    volume = volume_ref[rows8(g), :]
    return [
        volume * wide_ref[c, rows8(g), :] + (here_ref[c, rows8(g), :] - beside_ref[c, rows8(g), :])
        for c in range(BLOCK)
    ]


def cell(ref, g):
    return [ref[c, rows8(g), :] for c in range(BLOCK)]


def put(ref, g, vector):
    for c in range(BLOCK):
        ref[c, rows8(g), :] = vector[c]


def added(acc, a, b):
    for x, y in zip(a, b):
        acc = acc + x * y
    return acc


def zero():
    return jnp.zeros((SUB, LANES), F32)


def start_kernel(
    count_ref, used_any, flow_any, list_any, normal_any, owner_any, neighbour_any, source_any,
    pack_ref, out_ref, send_ref, flow_ref, source_ref,
    stage_ref, list_ref, used_ref, normal_ref, owner_ref, neighbour_ref, sems,
):
    pairs = (
        (used_any, used_ref), (flow_any, flow_ref), (list_any, list_ref), (normal_any, normal_ref),
        (owner_any, owner_ref), (neighbour_any, neighbour_ref), (source_any, source_ref),
    )
    copies = [pltpu.make_async_copy(a, b, sems.at[i]) for i, (a, b) in enumerate(pairs)]
    for copy in copies:
        copy.start()
    lists, width = list_ref.shape
    each = lists // 2
    halves = width // LANES
    sub = sub_ids()
    core = lax.axis_index("faces")
    per = each * halves
    packed = send_ref.shape[0] // 2
    for copy in copies[:3]:
        copy.wait()
    rows = []
    for i in range(per):
        j, h = i // halves, i % halves
        two = [list_ref[k : k + 1, h * LANES : (h + 1) * LANES] for k in (j, each + j)]
        rows.append(jnp.where(core == 0, *two))
    for v in range(packed):
        cells = jnp.zeros((SUB, LANES), I32)
        used = jnp.zeros((SUB, LANES), I32)
        for s in range(min(SUB, BLOCK * per - v * SUB)):
            i = (v * SUB + s) % per
            cells = jnp.where(sub == s, jnp.broadcast_to(rows[i], (SUB, LANES)), cells)
            used = jnp.where(sub == s, used_ref[core * each + i // halves] - i % halves * LANES, used)
        alive = lane_ids() < used
        send_ref[v] = jnp.where(alive, cells >> 7, -1)
        send_ref[packed + v] = jnp.where(alive, cells & (LANES - 1), 0)
    tiles = flow_ref.shape[1] // LANES
    send_halo(listed(flat_rows(flow_ref), tiles, send_ref, per), stage_ref, out_ref, each)
    for copy in copies[3:]:
        copy.wait()
    pack_faces(count_ref, normal_ref, owner_ref, neighbour_ref, pack_ref, lists, width, tiles * LANES)


def pack_faces(count_ref, normal_ref, owner_ref, neighbour_ref, pack_ref, lists, width, cells_here):
    tiles = cells_here // LANES
    pairs = tiles // 2
    shape = (pairs, LANES)
    pair, lane = sub_ids(shape), lane_ids(shape)
    for i in range(3 * pairs):
        for c in range(3):
            at = (i % 3) * pairs + i // 3
            pack_ref[c, at : at + 1, :] = normal_ref[c : c + 1, i * LANES : (i + 1) * LANES]
    for q in range(3):
        at = slice(q * pairs, (q + 1) * pairs)
        tile = 2 * pair + (0, jnp.where(lane >= LANES // 2, 1, 0), 1)[q]
        live = (3 * pair + q) * LANES + lane < count_ref[0]
        owner = owner_ref[pl.ds(q, pairs, stride=3), :] - tile * LANES
        neighbour = neighbour_ref[pl.ds(q, pairs, stride=3), :]
        near = (neighbour - tile * LANES) & (cells_here - 1)
        far = neighbour - cells_here - lax.rem(tile, lists) * width + 2 * LANES
        code = jnp.where(neighbour < cells_here, near, far)
        pack_ref[3, at, :] = (owner * 512 + code).astype(F32)
        for c in range(3):
            pack_ref[c, at, :] = jnp.where(live, 0.5 * pack_ref[c, at, :], 0.0)


def sorted_columns(x):
    sub = sub_ids()
    for k in range(1, 8):
        flip = None
        if 4 <= k <= 6:
            flip = ((sub >> (k - 4)) & 1) == 1
            x = [jnp.where(flip, -a, a) for a in x]
        for j in range(k - 1, -1, -1):
            if j < 4:
                new = list(x)
                for v in range(16):
                    w = v | (1 << j)
                    if w != v:
                        low, high = jnp.minimum(x[v], x[w]), jnp.maximum(x[v], x[w])
                        down = k < 4 and (v >> k) & 1
                        new[v], new[w] = (high, low) if down else (low, high)
                x = new
            else:
                d = 1 << (j - 4)
                first = ((sub >> (j - 4)) & 1) == 0
                x = [
                    jnp.where(
                        first,
                        jnp.minimum(a, pltpu.roll(a, SUB - d, 0)),
                        jnp.maximum(a, pltpu.roll(a, d, 0)),
                    )
                    for a in x
                ]
        if flip is not None:
            x = [jnp.where(flip, -a, a) for a in x]
    return x


def counts_below(x, first):
    sub = sub_ids()
    rows = []
    heads = [jnp.broadcast_to(x[15][s : s + 1, :], (SUB, LANES)) for s in range(SUB)]
    for w in range(LANES // SUB):
        bound = ((sub + (first + w * SUB + 1)) * LANES).astype(F32)
        block = jnp.zeros((SUB, LANES), I32)
        for s in range(SUB):
            block = jnp.where(heads[s] < bound, s + 1, block)
        at = jnp.minimum(block, SUB - 1)
        inside = jnp.zeros((SUB, LANES), I32)
        for v in range(15):
            inside = jnp.where(pick_row(x[v], at) < bound, v + 1, inside)
        rows.append((block * 16 + jnp.where(block < SUB, inside, 0)).astype(F32))
    return rows


def sort_rows(key_ref, lower_ref, upper_ref):
    lane = lane_ids()
    back = 8 * (lane & 15) + (lane >> 4)
    skip = lower_ref.shape[0] - upper_ref.shape[0]
    for b in range(key_ref.shape[0] // LANES):
        at = slice(b * LANES, (b + 1) * LANES)
        turned = jnp.transpose(key_ref[at, :])
        x = sorted_columns([turned[v * SUB : (v + 1) * SUB, :] for v in range(16)])
        turned = jnp.transpose(jnp.concatenate(x, axis=0))
        for v in range(16):
            row = b * LANES + v * SUB
            key_ref[row : row + SUB, :] = pick(turned[v * SUB : (v + 1) * SUB, :], back)
        lower_ref[at, :] = jnp.transpose(jnp.concatenate(counts_below(x, 0), axis=0))
        if b * LANES >= skip:
            at = slice(b * LANES - skip, (b + 1) * LANES - skip)
            upper_ref[at, :] = jnp.transpose(jnp.concatenate(counts_below(x, LANES), axis=0))


def table_kernel(
    mine_ref, peer_ref, flow_ref,
    normal_ref, link_ref, order_ref, last_ref, lean_ref, coupling_ref,
    wide_ref, key_ref, beside_ref, joint_ref, flux_ref, sort_ref, lower_ref, upper_ref,
):
    tiles = normal_ref.shape[2]
    pairs = tiles // 2
    swapped = lax.axis_index("faces") == 1
    lane = lane_ids((pairs, LANES))
    half = LANES // 2
    for i in range(4):
        part = []
        for q in range(3):
            mine = mine_ref[i, q * pairs : (q + 1) * pairs, :]
            peer = peer_ref[i, q * pairs : (q + 1) * pairs, :]
            part.append((jnp.where(swapped, peer, mine), jnp.where(swapped, mine, peer)))
        (a0, b0), (a1, b1), (a2, b2) = part
        even = (a0, b0, jnp.where(lane < half, a1, pltpu.roll(b1, half, 1)))
        odd = (a2, b2, jnp.where(lane < half, pltpu.roll(a1, half, 1), b1))
        for r in range(3):
            target = normal_ref.at[i, r] if i < 3 else joint_ref.at[r]
            target[pl.ds(0, pairs, stride=2), :] = even[r]
            target[pl.ds(1, pairs, stride=2), :] = odd[r]
    lane = lane_ids()
    for r in range(3):
        for g in in_groups(tiles):
            joint = joint_ref[r, rows8(g), :].astype(I32)
            owner, code = joint >> 9, joint & 511
            link_ref[0, r, rows8(g), :] = owner
            link_ref[1, r, rows8(g), :] = code
            at = r * tiles + g * SUB
            key_ref[at : at + SUB, :] = (owner * LANES + lane).astype(F32)
            at += 3 * tiles
            key_ref[at : at + SUB, :] = (jnp.minimum(code, 256) * LANES + lane).astype(F32)
    sort_rows(key_ref, lower_ref, upper_ref)
    skip = lower_ref.shape[0] - upper_ref.shape[0]
    for r in range(3):
        for g in in_groups(tiles):
            at = r * tiles + g * SUB
            owned = key_ref[at : at + SUB, :]
            near = key_ref[at + 3 * tiles : at + 3 * tiles + SUB, :]
            order_ref[0, r, rows8(g), :] = owned.astype(I32) & (LANES - 1)
            order_ref[1, r, rows8(g), :] = near.astype(I32) & (LANES - 1)
            near = at + 3 * tiles
            for i, count in enumerate(
                (lower_ref[at : at + SUB, :], lower_ref[near : near + SUB, :], upper_ref[near - skip : near - skip + SUB, :])
            ):
                last_ref[i, r, rows8(g), :] = count.astype(I32) - 1
    for t in range(tiles):
        for c in range(3):
            wide_ref[c, t : t + 1, :] = flow_ref[c : c + 1, t * LANES : (t + 1) * LANES]
    widen(wide_ref, tiles, 3)
    for g in in_groups(tiles):
        for r in range(3):
            left, right = local_values(wide_ref, link_ref, g, r, 3)
            lean, size = zero(), zero()
            for i in range(3):
                normal = normal_ref[i, r, rows8(g), :]
                lean = lean + normal * (left[i] + right[i])
                size = size + normal * normal
                flux_ref[block_at((g * 3 + r) * 3 + i), :] = normal
            lean_ref[0, r, rows8(g), :] = lean
            lean_ref[1, r, rows8(g), :] = 2.0 * jnp.sqrt(size)
    to_cells(flux_ref, order_ref, last_ref, coupling_ref, beside_ref, sort_ref, (-1, -1, -1))
    for g in in_groups(tiles):
        for i in range(3):
            coupling_ref[i, rows8(g), :] = coupling_ref[i, rows8(g), :] - beside_ref[i, rows8(g), :]


def setup_kernel(
    in_ref, source_ref, volume_ref, normal_ref, link_ref, order_ref, last_ref, lean_ref, coupling_ref, send_ref,
    pair_ref, diag_ref, source_out, pre_ref, out_ref,
    stage_ref, halo_ref, here_ref, beside_ref, flux_ref, sort_ref, *, shifts,
):
    tiles = volume_ref.shape[0]
    lay_halo(got_halo(in_ref, shifts), halo_ref)
    for g in in_groups(tiles):
        for r in range(3):
            right = halo_values([zero() for _ in range(3)], halo_ref, link_ref, g, r, len(shifts))
            speed = lean_ref[0, r, rows8(g), :]
            for i in range(3):
                speed = speed + normal_ref[i, r, rows8(g), :] * right[i]
            wave = 0.5 * jnp.abs(speed) + lean_ref[1, r, rows8(g), :]
            for i, term in enumerate((0.5 * speed, wave)):
                pair_ref[i, r, rows8(g), :] = term
                flux_ref[block_at((g * 3 + r) * 2 + i), :] = term
    to_cells(flux_ref, order_ref, last_ref, here_ref, beside_ref, sort_ref, (-1, 1))
    for t in range(tiles):
        for c in range(BLOCK):
            source_out[c, t : t + 1, :] = source_ref[c : c + 1, t * LANES : (t + 1) * LANES]
    for g in in_groups(tiles):
        n0, n1, n2 = [coupling_ref[i, rows8(g), :] for i in range(3)]
        speed = here_ref[0, rows8(g), :] - beside_ref[0, rows8(g), :]
        pressure_diag = volume_ref[rows8(g), :] + (here_ref[1, rows8(g), :] + beside_ref[1, rows8(g), :])
        inverse = 1.0 / (pressure_diag + speed)
        schur = pressure_diag - (n0 * n0 + n1 * n1 + n2 * n2) * inverse
        for i, value in enumerate((inverse, n0, n1, n2, 1.0 / schur)):
            diag_ref[i, rows8(g), :] = value
        put(pre_ref, g, precondition(cell(source_out, g), diag_ref, g))
    send_halo(listed(tiled_rows(pre_ref), tiles, send_ref, len(shifts) // 2 * (SUB // BLOCK)), stage_ref, out_ref, len(shifts) // 2)


def combine(scales, vectors):
    out = []
    for parts in zip(*vectors):
        acc = None
        for scale, part in zip(scales, parts):
            term = part if scale is None else scale * part
            acc = term if acc is None else acc + term
        out.append(acc)
    return out


def first_kernel(
    in_ref, pre_ref, source_ref, volume_ref, normal_ref, pair_ref, link_ref, order_ref, last_ref, diag_ref, send_ref,
    image_ref, mimage_ref, out_ref,
    stage_ref, halo_ref, wide_ref, here_ref, beside_ref, flux_ref, sort_ref, *, shifts,
):
    tiles = volume_ref.shape[0]
    groups = in_groups(tiles)
    for g in groups:
        put(wide_ref, g, cell(pre_ref, g))
    widen(wide_ref, tiles)
    lay_halo(got_halo(in_ref, shifts), halo_ref)
    faces = (normal_ref, pair_ref, link_ref, order_ref, last_ref)
    face_part(wide_ref, halo_ref, faces, here_ref, beside_ref, flux_ref, sort_ref, len(shifts))
    product, rho = zero(), zero()
    for g in groups:
        image = applied(g, volume_ref, wide_ref, here_ref, beside_ref)
        source = cell(source_ref, g)
        product = added(product, source, image)
        rho = added(rho, source, source)
        put(image_ref, g, image)
        put(mimage_ref, g, precondition(image, diag_ref, g))
    send_sums((product, rho), out_ref)
    send_halo(listed(tiled_rows(mimage_ref), tiles, send_ref, len(shifts) // 2 * (SUB // BLOCK)), stage_ref, out_ref, len(shifts) // 2)


def second_kernel(
    in1_ref, in2_ref, pre_ref, mimage_ref, image_ref, source_ref,
    volume_ref, normal_ref, pair_ref, link_ref, order_ref, last_ref, diag_ref, send_ref,
    middle_ref, premid_ref, second_ref, msecond_ref, scale_ref, out_ref,
    stage_ref, halo_ref, wide_ref, here_ref, beside_ref, flux_ref, sort_ref, *, shifts,
):
    tiles = volume_ref.shape[0]
    groups = in_groups(tiles)
    sums = got_sums(in2_ref, len(shifts) // 2)
    rho = spread(sums, 1)
    alpha = rho / spread(sums, 0)
    scale_ref[0:1, :] = alpha[0:1, :]
    scale_ref[1:2, :] = rho[0:1, :]
    for g in groups:
        premid = combine((None, -alpha), (cell(pre_ref, g), cell(mimage_ref, g)))
        put(wide_ref, g, premid)
        put(premid_ref, g, premid)
    widen(wide_ref, tiles)
    lay_halo(combine((None, -alpha), (got_halo(in1_ref, shifts), got_halo(in2_ref, shifts))), halo_ref)
    faces = (normal_ref, pair_ref, link_ref, order_ref, last_ref)
    face_part(wide_ref, halo_ref, faces, here_ref, beside_ref, flux_ref, sort_ref, len(shifts))
    products = [zero() for _ in range(4)]
    for g in groups:
        second = applied(g, volume_ref, wide_ref, here_ref, beside_ref)
        source = cell(source_ref, g)
        middle = combine((None, -alpha), (source, cell(image_ref, g)))
        put(middle_ref, g, middle)
        put(second_ref, g, second)
        put(msecond_ref, g, precondition(second, diag_ref, g))
        for i, (a, b) in enumerate(((second, middle), (second, second), (source, middle), (source, second))):
            products[i] = added(products[i], a, b)
    send_sums(products, out_ref)
    send_halo(listed(tiled_rows(msecond_ref), tiles, send_ref, len(shifts) // 2 * (SUB // BLOCK)), stage_ref, out_ref, len(shifts) // 2)


def third_kernel(
    in1_ref, in2_ref, in3_ref, scale_ref, pre_ref, mimage_ref, premid_ref, msecond_ref, middle_ref, second_ref, source_ref,
    volume_ref, normal_ref, pair_ref, link_ref, order_ref, last_ref, diag_ref, send_ref,
    field_ref, residual_ref, preres_ref, predir_ref, image_ref, mimage_out, scale_out, ghost_ref, out_ref,
    stage_ref, halo_ref, wide_ref, here_ref, beside_ref, flux_ref, sort_ref, *, shifts,
):
    tiles = volume_ref.shape[0]
    groups = in_groups(tiles)
    sums = got_sums(in3_ref, len(shifts) // 2)
    alpha, rho = row_of(scale_ref, 0), row_of(scale_ref, 1)
    omega = spread(sums, 0) / spread(sums, 1)
    rho_next = spread(sums, 2) - omega * spread(sums, 3)
    beta = rho_next / rho * (alpha / omega)
    scale_out[0:1, :] = rho_next[0:1, :]
    drop = -beta * omega
    for g in groups:
        predir, mimage, premid = cell(pre_ref, g), cell(mimage_ref, g), cell(premid_ref, g)
        put(field_ref, g, combine((alpha, omega), (predir, premid)))
        put(residual_ref, g, combine((None, -omega), (cell(middle_ref, g), cell(second_ref, g))))
        preres = combine((None, -omega), (premid, cell(msecond_ref, g)))
        put(preres_ref, g, preres)
        predir = combine((None, beta, drop), (preres, predir, mimage))
        put(predir_ref, g, predir)
        put(wide_ref, g, predir)
    widen(wide_ref, tiles)
    ghost1, ghost2, ghost3 = [got_halo(ref, shifts) for ref in (in1_ref, in2_ref, in3_ref)]
    preres = combine((None, -alpha, -omega), (ghost1, ghost2, ghost3))
    for k in range(len(shifts)):
        ghost_ref[k] = preres[k]
    lay_halo(combine((None, beta, drop), (preres, ghost1, ghost2)), halo_ref)
    faces = (normal_ref, pair_ref, link_ref, order_ref, last_ref)
    face_part(wide_ref, halo_ref, faces, here_ref, beside_ref, flux_ref, sort_ref, len(shifts))
    product = zero()
    for g in groups:
        image = applied(g, volume_ref, wide_ref, here_ref, beside_ref)
        product = added(product, cell(source_ref, g), image)
        put(image_ref, g, image)
        put(mimage_out, g, precondition(image, diag_ref, g))
    send_sums((product,), out_ref)
    send_halo(listed(tiled_rows(mimage_out), tiles, send_ref, len(shifts) // 2 * (SUB // BLOCK)), stage_ref, out_ref, len(shifts) // 2)


def fourth_kernel(
    in4_ref, scale_ref, ghost_ref, field_ref, residual_ref, preres_ref, predir_ref, image_ref, mimage_ref,
    volume_ref, normal_ref, pair_ref, link_ref, order_ref, last_ref,
    field_out, premid_ref, middle_ref, second_ref, out_ref,
    halo_ref, wide_ref, here_ref, beside_ref, flux_ref, sort_ref, *, shifts,
):
    tiles = volume_ref.shape[0]
    groups = in_groups(tiles)
    alpha = row_of(scale_ref, 0) / spread(got_sums(in4_ref, len(shifts) // 2), 0)
    for g in groups:
        premid = combine((None, -alpha), (cell(preres_ref, g), cell(mimage_ref, g)))
        put(wide_ref, g, premid)
        put(premid_ref, g, premid)
        put(field_out, g, combine((None, alpha), (cell(field_ref, g), cell(predir_ref, g))))
        put(middle_ref, g, combine((None, -alpha), (cell(residual_ref, g), cell(image_ref, g))))
    widen(wide_ref, tiles)
    ghosts = [ghost_ref[k] for k in range(len(shifts))]
    lay_halo(combine((None, -alpha), (ghosts, got_halo(in4_ref, shifts))), halo_ref)
    faces = (normal_ref, pair_ref, link_ref, order_ref, last_ref)
    face_part(wide_ref, halo_ref, faces, here_ref, beside_ref, flux_ref, sort_ref, len(shifts))
    cross, square = zero(), zero()
    for g in groups:
        second = applied(g, volume_ref, wide_ref, here_ref, beside_ref)
        put(second_ref, g, second)
        cross = added(cross, second, cell(middle_ref, g))
        square = added(square, second, second)
    send_sums((cross, square), out_ref)


def last_kernel(in_ref, field_ref, premid_ref, middle_ref, second_ref, field_out, residual_out, stage_ref):
    tiles = field_ref.shape[1]
    sums = total_of([in_ref[d] for d in range(0, in_ref.shape[0], lax.axis_size("faces"))])
    omega = spread(sums, 0) / spread(sums, 1)
    for g in in_groups(tiles):
        field = combine((None, omega), (cell(field_ref, g), cell(premid_ref, g)))
        residual = combine((None, -omega), (cell(middle_ref, g), cell(second_ref, g)))
        put(stage_ref.at[0], g, field)
        put(stage_ref.at[1], g, residual)
        for i, out in enumerate((field_out, residual_out)):
            for t in range(g * SUB, g * SUB + SUB):
                for c in range(BLOCK):
                    out[c : c + 1, t * LANES : (t + 1) * LANES] = stage_ref[i, c, t : t + 1, :]


def run(kernel, outs, scratch, args, scalars=0, away=0):
    vmem = pl.BlockSpec(memory_space=pltpu.VMEM)
    smem = pl.BlockSpec(memory_space=pltpu.SMEM)
    hbm = pl.BlockSpec(memory_space=pltpu.HBM)
    far = range(scalars, scalars + away)
    args = [pltpu.with_memory_space_constraint(a, pltpu.HBM) if i in far else a for i, a in enumerate(args)]
    return pl.pallas_call(
        kernel,
        out_shape=[jax.ShapeDtypeStruct(shape, dtype) for shape, dtype in outs],
        in_specs=[smem] * scalars + [hbm] * away + [vmem] * (len(args) - scalars - away),
        out_specs=[vmem] * len(outs),
        scratch_shapes=[pltpu.VMEM(shape, F32) if isinstance(shape, tuple) else shape for shape in scratch],
        compiler_params=pltpu.CompilerParams(vmem_limit_bytes=24 << 20),
    )(*args)


def exchange(block):
    return lax.all_to_all(block, ("cells", "faces"), 0, 0)


def body(
    flow_state,
    source_term,
    volume_rate,
    face_normal,
    face_owner,
    face_neighbour,
    face_count,
    send_list,
    halo_count,
):
    count = lax.axis_size("cells")
    cells_here = flow_state.shape[1]
    lists, width = send_list.shape
    tiles = cells_here // LANES
    per_tile = face_owner.shape[0] // tiles
    shifts = offsets(lists // 2)
    assert per_tile * 2 == 3 * LANES and lax.axis_size("faces") == 2
    assert width == 2 * LANES and count > lists and lists % 2 == 0 and lists <= SUB
    assert tiles % SUB == 0 and cells_here & (cells_here - 1) == 0
    rows = 3
    span = -(-(lists + SUB - 1) // SUB) * SUB
    vector = (BLOCK, tiles, LANES)
    vec = (vector, F32)
    faces = (rows, tiles, LANES)
    scale = ((SUB, LANES), F32)
    full_block = ((2 * count, SUB, LANES), F32)
    flat_vec = (flow_state.shape, F32)
    stage = (SUB * SUB, LANES)
    halo = (SUB * span, LANES)
    flat = face_owner.shape[0] // LANES
    volume = volume_rate.reshape(tiles, LANES)

    def wide(parts):
        return (parts, tiles + SUB, LANES)

    def blocks(parts):
        return (rows * parts * tiles, LANES)

    ints = pltpu.VMEM((flat, LANES), I32)
    packed = -(-BLOCK * (lists // 2) * (width // LANES) // SUB)
    pack, out0, send, flow, source = run(
        start_kernel,
        [((4, flat, LANES), F32), full_block, ((2 * packed, SUB, LANES), I32), flat_vec, flat_vec],
        [
            stage, pltpu.VMEM(send_list.shape, I32), pltpu.SMEM((lists,), I32),
            face_normal.shape, ints, ints, pltpu.SemaphoreType.DMA((7,)),
        ],
        (
            face_count, halo_count, flow_state, send_list, face_normal,
            face_owner.reshape(flat, LANES), face_neighbour.reshape(flat, LANES), source_term,
        ),
        scalars=1,
        away=7,
    )
    in0 = exchange(out0)
    peer = lax.ppermute(pack, "faces", [(0, 1), (1, 0)])
    normal, link, order, last, lean, coupling = run(
        table_kernel,
        [
            ((3,) + faces, F32), ((2,) + faces, I32), ((2,) + faces, I32), ((3,) + faces, I32),
            ((2,) + faces, F32), ((3, tiles, LANES), F32),
        ],
        [
            wide(3), (6 * tiles, LANES), wide(3), faces,
            blocks(3), blocks(6), (6 * tiles, LANES), (4 * tiles, LANES),
        ],
        (pack, peer, flow),
    )
    pair, diag, source, predir, out1 = run(
        functools.partial(setup_kernel, shifts=shifts),
        [((2,) + faces, F32), ((5, tiles, LANES), F32), vec, vec, full_block],
        [stage, halo, (2, tiles, LANES), wide(2), blocks(2), blocks(4)],
        (in0, source, volume, normal, link, order, last, lean, coupling, send),
    )
    in1 = exchange(out1)
    work = [stage, halo, wide(BLOCK), vector, wide(BLOCK), blocks(BLOCK), blocks(2 * BLOCK)]
    fixed = (volume, normal, pair, link, order, last, diag, send)
    image, mimage, out2 = run(
        functools.partial(first_kernel, shifts=shifts), [vec, vec, full_block], work, (in1, predir, source) + fixed
    )
    in2 = exchange(out2)
    middle, premid, second, msecond, scales, out3 = run(
        functools.partial(second_kernel, shifts=shifts),
        [vec, vec, vec, vec, scale, full_block],
        work,
        (in1, in2, predir, mimage, image, source) + fixed,
    )
    in3 = exchange(out3)
    field, residual, preres, predir, image, mimage, scales, ghosts, out4 = run(
        functools.partial(third_kernel, shifts=shifts),
        [vec, vec, vec, vec, vec, vec, scale, ((lists, SUB, LANES), F32), full_block],
        work,
        (in1, in2, in3, scales, predir, mimage, premid, msecond, middle, second, source) + fixed,
    )
    in4 = exchange(out4)
    field, premid, middle, second, out5 = run(
        functools.partial(fourth_kernel, shifts=shifts),
        [vec, vec, vec, vec, full_block],
        work[1:],
        (in4, scales, ghosts, field, residual, preres, predir, image, mimage) + fixed[:6],
    )
    in5 = exchange(out5)
    field, residual = run(last_kernel, [flat_vec, flat_vec], [(2,) + vector], (in5, field, premid, middle, second))
    return (field, residual)


def solution(mesh):
    in_specs = (
        P(None, "cells"),
        P(None, "cells"),
        P("cells"),
        P(None, ("cells", "faces")),
        P(("cells", "faces")),
        P(("cells", "faces")),
        P(("cells", "faces")),
        P("cells", None),
        P("cells"),
    )
    out_specs = (P(None, "cells"), P(None, "cells"))
    return jax.shard_map(body, mesh=mesh, in_specs=in_specs, out_specs=out_specs, check_vma=False)
```

```python
import functools

import jax
import jax.numpy as jnp
from jax import lax
from jax.experimental import pallas as pl
from jax.experimental.pallas import tpu as pltpu
from jax.sharding import PartitionSpec as P

F32 = jnp.float32
I32 = jnp.int32
LANES = 128
SUB = 8
BLOCK = 4


def offsets(count):
    return [which + 1 for which in range(count)] + [-(which + 1) for which in range(count)]


ALONG_LANES = lax.GatherDimensionNumbers(
    offset_dims=(),
    collapsed_slice_dims=(1,),
    start_index_map=(1,),
    operand_batching_dims=(0,),
    start_indices_batching_dims=(0,),
)

ALONG_ROWS = lax.GatherDimensionNumbers(
    offset_dims=(),
    collapsed_slice_dims=(0,),
    start_index_map=(0,),
    operand_batching_dims=(1,),
    start_indices_batching_dims=(1,),
)


def pick(values, index):
    mode = lax.GatherScatterMode.PROMISE_IN_BOUNDS
    return lax.gather(values, index[..., None], ALONG_LANES, slice_sizes=(1, 1), mode=mode)


def pick_row(values, index):
    mode = lax.GatherScatterMode.PROMISE_IN_BOUNDS
    return lax.gather(values, index[..., None], ALONG_ROWS, slice_sizes=(1, 1), mode=mode)


def lane_ids(shape=(SUB, LANES)):
    return lax.broadcasted_iota(I32, shape, 1)


def sub_ids(shape=(SUB, LANES)):
    return lax.broadcasted_iota(I32, shape, 0)


def partition(distance, count):
    return lax.rem(lax.axis_index("cells") + distance + count, count)


def in_groups(tiles):
    return range(tiles // SUB)


def rows8(g):
    return slice(g * SUB, g * SUB + SUB)


def listed(row_of_tile, tiles, send_ref, per):
    packed = send_ref.shape[0] // 2
    sub = sub_ids()
    found = []
    for v in range(packed):
        row_at, lane_at = send_ref[v], send_ref[packed + v]
        low, high = [min(n // per, BLOCK - 1) for n in (v * SUB, v * SUB + SUB - 1)]
        assert high - low <= 1
        values = jnp.zeros((SUB, LANES), F32)
        for t in range(tiles):
            row = jnp.broadcast_to(row_of_tile(low, t), (SUB, LANES))
            if high > low:
                other = jnp.broadcast_to(row_of_tile(high, t), (SUB, LANES))
                row = jnp.where(sub < high * per - v * SUB, row, other)
            values = jnp.where(row_at == t, pick(row, lane_at), values)
        found.append(values)
    return found


def tiled_rows(ref):
    return lambda c, t: ref[c, t : t + 1, :]


def flat_rows(ref):
    return lambda c, t: ref[c : c + 1, t * LANES : (t + 1) * LANES]


def send_halo(found, stage_ref, out_ref, each):
    cores = lax.axis_size("faces")
    count = out_ref.shape[0] // cores
    halves = SUB // BLOCK
    for v, values in enumerate(found):
        stage_ref[v * SUB : (v + 1) * SUB, :] = values
    sign = 1 - 2 * lax.axis_index("faces")
    for j in range(each):
        place = partition(sign * (j + 1), count)
        for h in range(halves):
            rows = stage_ref[pl.ds(j * halves + h, BLOCK, stride=each * halves), :]
            for core in range(cores):
                out_ref[place * cores + core, h * BLOCK : (h + 1) * BLOCK, :] = rows


def got_halo(in_ref, shifts):
    cores = lax.axis_size("faces")
    count = in_ref.shape[0] // cores
    each = len(shifts) // cores
    return [in_ref[partition(-shift, count) * cores + k // each] for k, shift in enumerate(shifts)]


def lay_halo(lists, halo_ref):
    total = len(lists)
    span = halo_ref.shape[0] // SUB
    for j in range(total + SUB - 1):
        halo_ref[pl.ds(j, SUB, stride=span), :] = lists[j % total]


def send_sums(sums, out_ref):
    rows = jnp.zeros((SUB, LANES), F32)
    sub = sub_ids()
    for i, acc in enumerate(sums):
        row = jnp.sum(acc, axis=0, keepdims=True)
        rows = jnp.where(sub == i, jnp.broadcast_to(row, (SUB, LANES)), rows)
    for d in range(out_ref.shape[0]):
        out_ref[d] = rows


def total_of(parts):
    while len(parts) > 1:
        parts = [a + b for a, b in zip(parts[::2], parts[1::2])] + parts[len(parts) & ~1 :]
    return jnp.sum(parts[0], axis=1, keepdims=True)


def got_sums(in_ref, each):
    cores = lax.axis_size("faces")
    count = in_ref.shape[0] // cores
    parts = []
    for q in range(count):
        ahead = partition(-q, count)
        core = jnp.where((ahead >= 1) & (ahead <= each), 1, 0)
        parts.append(in_ref[q * cores + core])
    return total_of(parts)


def spread(column, i):
    return jnp.broadcast_to(column[i : i + 1, :], (SUB, LANES))


def row_of(ref, i):
    return jnp.broadcast_to(ref[i : i + 1, :], (SUB, LANES))


def prefix_matrix():
    shape = (2 * LANES, LANES)
    upto = (lax.broadcasted_iota(I32, shape, 0) & (LANES - 1)) <= lax.broadcasted_iota(I32, shape, 1)
    return jnp.where(upto, 1.0, 0.0).astype(jnp.bfloat16)


def prefix_sums(values, matrix):
    high = values.astype(jnp.bfloat16)
    low = (values - high.astype(F32)).astype(jnp.bfloat16)
    return jnp.dot(jnp.concatenate([high, low], axis=1), matrix, preferred_element_type=F32)


def block_at(i):
    return slice(i * SUB, i * SUB + SUB)


def to_cells(flux_ref, order_ref, last_ref, here_ref, beside_ref, sort_ref, signs):
    parts = len(signs)
    tiles = here_ref.shape[1]
    rows = order_ref.shape[1]
    each = rows * parts
    sides = 1 if beside_ref is None else 2
    matrix = prefix_matrix()
    for g in in_groups(tiles):
        for side in range(sides):
            for r in range(rows):
                order = order_ref[side, r, rows8(g), :]
                for c in range(parts):
                    source = flux_ref[block_at(g * each + r * parts + c), :]
                    sort_ref[block_at((g * sides + side) * each + r * parts + c), :] = pick(source, order)
    for g in in_groups(tiles):
        at = slice(g * sides * each * SUB, (g + 1) * sides * each * SUB)
        sort_ref[at, :] = prefix_sums(sort_ref[at, :], matrix)
    lane = lane_ids()
    for g in in_groups(tiles):
        totals = []
        for side, of in ((0, 0), (1, 1), (1, 2))[: 2 * sides - 1]:
            acc = None
            for r in range(rows):
                last = last_ref[of, r, rows8(g), :]
                some = last >= 0
                at = last & (LANES - 1)
                got = [
                    jnp.where(some, pick(sort_ref[block_at((g * sides + side) * each + r * parts + c), :], at), 0.0)
                    for c in range(parts)
                ]
                acc = got if acc is None else [a + b for a, b in zip(acc, got)]
            totals.append(acc)
        for c in range(parts):
            if sides == 1:
                here_ref[c, rows8(g), :] = totals[0][c]
                continue
            owned, near, far = totals[0][c], totals[1][c], totals[2][c]
            here_ref[c, rows8(g), :] = owned + near if signs[c] > 0 else owned - near
            beside_ref[c, g * SUB + 1 : g * SUB + 1 + SUB, :] = jnp.where(lane == LANES - 1, near, far)
            sort_ref[block_at(g * sides * each + c), :] = far
    for g in in_groups(tiles):
        for c in range(parts):
            both = here_ref[c, rows8(g), :]
            here_ref[c, rows8(g), :] = both - jnp.where(lane == 0, 0.0, pltpu.roll(both, 1, 1))
            if sides == 2:
                at = slice(g * SUB + 1, g * SUB + 1 + SUB)
                before = pltpu.roll(beside_ref[c, at, :], 1, 1)
                beside_ref[c, at, :] = sort_ref[block_at(g * sides * each + c), :] - before
    if sides == 2:
        for c in range(parts):
            beside_ref[c, 0:1, :] = beside_ref[c, tiles : tiles + 1, :]


def local_values(wide_ref, link_ref, g, r, parts):
    owner, code = link_ref[0, r, rows8(g), :], link_ref[1, r, rows8(g), :]
    at = code & (LANES - 1)
    source = code >> 7
    own = [wide_ref[c, rows8(g), :] for c in range(parts)]
    left = [pick(v, owner) for v in own]
    right = [jnp.where(source == 0, pick(v, at), 0.0) for v in own]
    for c in range(parts):
        other = wide_ref[c, g * SUB + 1 : g * SUB + 1 + SUB, :]
        right[c] = jnp.where(source == 1, pick(other, at), right[c])
    return left, right


def halo_values(right, halo_ref, link_ref, g, r, lists):
    span = halo_ref.shape[0] // SUB
    code = link_ref[1, r, rows8(g), :]
    at = code & (LANES - 1)
    source = code >> 7
    first = (g * SUB) % lists
    right = list(right)
    for h in range(SUB // BLOCK):
        for c in range(len(right)):
            base = (h * BLOCK + c) * span + first
            right[c] = jnp.where(source == 2 + h, pick(halo_ref[base : base + SUB, :], at), right[c])
    return right


def widen(wide_ref, tiles, parts=BLOCK):
    for c in range(parts):
        wide_ref[c, tiles : tiles + 1, :] = wide_ref[c, 0:1, :]


def face_terms(normal_ref, pair_ref, g, r):
    normal = [normal_ref[i, r, rows8(g), :] for i in range(3)]
    return normal, pair_ref[0, r, rows8(g), :], pair_ref[1, r, rows8(g), :]


def put_flux(flux_ref, first, normal, speed, wave, both, gap):
    for i in range(3):
        flux_ref[block_at(first + i), :] = speed * both[i] + normal[i] * both[3] + wave * gap[i]
    last = normal[0] * both[0] + normal[1] * both[1] + normal[2] * both[2] + wave * gap[3]
    flux_ref[block_at(first + 3), :] = last


def face_part(wide_ref, halo_ref, faces, here_ref, beside_ref, flux_ref, sort_ref, lists):
    normal_ref, pair_ref, link_ref, order_ref, last_ref = faces
    rows = link_ref.shape[1]
    for g in in_groups(here_ref.shape[1]):
        for r in range(rows):
            left, right = local_values(wide_ref, link_ref, g, r, BLOCK)
            right = halo_values(right, halo_ref, link_ref, g, r, lists)
            normal, speed, wave = face_terms(normal_ref, pair_ref, g, r)
            both = [a + b for a, b in zip(left, right)]
            gap = [a - b for a, b in zip(left, right)]
            put_flux(flux_ref, (g * rows + r) * BLOCK, normal, speed, wave, both, gap)
    to_cells(flux_ref, order_ref, last_ref, here_ref, beside_ref, sort_ref, (-1,) * BLOCK)


def precondition(vector, diag_ref, g):
    inverse, n0, n1, n2, schur = [diag_ref[i, rows8(g), :] for i in range(5)]
    coupled = n0 * vector[0] + n1 * vector[1] + n2 * vector[2]
    pressure = (vector[3] - coupled * inverse) * schur
    return [(vector[i] - n * pressure) * inverse for i, n in enumerate((n0, n1, n2))] + [pressure]


def applied(g, volume_ref, wide_ref, here_ref, beside_ref):
    volume = volume_ref[rows8(g), :]
    return [
        volume * wide_ref[c, rows8(g), :] + (here_ref[c, rows8(g), :] - beside_ref[c, rows8(g), :])
        for c in range(BLOCK)
    ]


def cell(ref, g):
    return [ref[c, rows8(g), :] for c in range(BLOCK)]


def put(ref, g, vector):
    for c in range(BLOCK):
        ref[c, rows8(g), :] = vector[c]


def added(acc, a, b):
    for x, y in zip(a, b):
        acc = acc + x * y
    return acc


def zero():
    return jnp.zeros((SUB, LANES), F32)


def start_kernel(
    count_ref, used_any, flow_any, list_any, normal_any, owner_any, neighbour_any, source_any,
    pack_ref, out_ref, send_ref, flow_ref, source_ref,
    stage_ref, list_ref, used_ref, normal_ref, owner_ref, neighbour_ref, sems,
):
    pairs = (
        (used_any, used_ref), (flow_any, flow_ref), (list_any, list_ref), (normal_any, normal_ref),
        (owner_any, owner_ref), (neighbour_any, neighbour_ref), (source_any, source_ref),
    )
    copies = [pltpu.make_async_copy(a, b, sems.at[i]) for i, (a, b) in enumerate(pairs)]
    for copy in copies:
        copy.start()
    lists, width = list_ref.shape
    each = lists // 2
    halves = width // LANES
    sub = sub_ids()
    core = lax.axis_index("faces")
    per = each * halves
    packed = send_ref.shape[0] // 2
    for copy in copies[:3]:
        copy.wait()
    rows = []
    for i in range(per):
        j, h = i // halves, i % halves
        two = [list_ref[k : k + 1, h * LANES : (h + 1) * LANES] for k in (j, each + j)]
        rows.append(jnp.where(core == 0, *two))
    for v in range(packed):
        cells = jnp.zeros((SUB, LANES), I32)
        used = jnp.zeros((SUB, LANES), I32)
        for s in range(min(SUB, BLOCK * per - v * SUB)):
            i = (v * SUB + s) % per
            cells = jnp.where(sub == s, jnp.broadcast_to(rows[i], (SUB, LANES)), cells)
            used = jnp.where(sub == s, used_ref[core * each + i // halves] - i % halves * LANES, used)
        alive = lane_ids() < used
        send_ref[v] = jnp.where(alive, cells >> 7, -1)
        send_ref[packed + v] = jnp.where(alive, cells & (LANES - 1), 0)
    tiles = flow_ref.shape[1] // LANES
    send_halo(listed(flat_rows(flow_ref), tiles, send_ref, per), stage_ref, out_ref, each)
    for copy in copies[3:]:
        copy.wait()
    pack_faces(count_ref, normal_ref, owner_ref, neighbour_ref, pack_ref, lists, width, tiles * LANES)


def pack_faces(count_ref, normal_ref, owner_ref, neighbour_ref, pack_ref, lists, width, cells_here):
    tiles = cells_here // LANES
    pairs = tiles // 2
    shape = (pairs, LANES)
    pair, lane = sub_ids(shape), lane_ids(shape)
    for i in range(3 * pairs):
        for c in range(3):
            at = (i % 3) * pairs + i // 3
            pack_ref[c, at : at + 1, :] = normal_ref[c : c + 1, i * LANES : (i + 1) * LANES]
    for q in range(3):
        at = slice(q * pairs, (q + 1) * pairs)
        tile = 2 * pair + (0, jnp.where(lane >= LANES // 2, 1, 0), 1)[q]
        live = (3 * pair + q) * LANES + lane < count_ref[0]
        owner = owner_ref[pl.ds(q, pairs, stride=3), :] - tile * LANES
        neighbour = neighbour_ref[pl.ds(q, pairs, stride=3), :]
        near = (neighbour - tile * LANES) & (cells_here - 1)
        far = neighbour - cells_here - lax.rem(tile, lists) * width + 2 * LANES
        code = jnp.where(neighbour < cells_here, near, far)
        pack_ref[3, at, :] = (owner * 512 + code).astype(F32)
        for c in range(3):
            pack_ref[c, at, :] = jnp.where(live, 0.5 * pack_ref[c, at, :], 0.0)


def sorted_columns(x):
    sub = sub_ids()
    for k in range(1, 8):
        flip = None
        if 4 <= k <= 6:
            flip = ((sub >> (k - 4)) & 1) == 1
            x = [jnp.where(flip, -a, a) for a in x]
        for j in range(k - 1, -1, -1):
            if j < 4:
                new = list(x)
                for v in range(16):
                    w = v | (1 << j)
                    if w != v:
                        low, high = jnp.minimum(x[v], x[w]), jnp.maximum(x[v], x[w])
                        down = k < 4 and (v >> k) & 1
                        new[v], new[w] = (high, low) if down else (low, high)
                x = new
            else:
                d = 1 << (j - 4)
                first = ((sub >> (j - 4)) & 1) == 0
                x = [
                    jnp.where(
                        first,
                        jnp.minimum(a, pltpu.roll(a, SUB - d, 0)),
                        jnp.maximum(a, pltpu.roll(a, d, 0)),
                    )
                    for a in x
                ]
        if flip is not None:
            x = [jnp.where(flip, -a, a) for a in x]
    return x


def counts_below(x, first):
    sub = sub_ids()
    rows = []
    heads = [jnp.broadcast_to(x[15][s : s + 1, :], (SUB, LANES)) for s in range(SUB)]
    for w in range(LANES // SUB):
        bound = ((sub + (first + w * SUB + 1)) * LANES).astype(F32)
        block = jnp.zeros((SUB, LANES), I32)
        for s in range(SUB):
            block = jnp.where(heads[s] < bound, s + 1, block)
        at = jnp.minimum(block, SUB - 1)
        inside = jnp.zeros((SUB, LANES), I32)
        for v in range(15):
            inside = jnp.where(pick_row(x[v], at) < bound, v + 1, inside)
        rows.append((block * 16 + jnp.where(block < SUB, inside, 0)).astype(F32))
    return rows


def sort_rows(key_ref, lower_ref, upper_ref):
    lane = lane_ids()
    back = 8 * (lane & 15) + (lane >> 4)
    skip = lower_ref.shape[0] - upper_ref.shape[0]
    for b in range(key_ref.shape[0] // LANES):
        at = slice(b * LANES, (b + 1) * LANES)
        turned = jnp.transpose(key_ref[at, :])
        x = sorted_columns([turned[v * SUB : (v + 1) * SUB, :] for v in range(16)])
        turned = jnp.transpose(jnp.concatenate(x, axis=0))
        for v in range(16):
            row = b * LANES + v * SUB
            key_ref[row : row + SUB, :] = pick(turned[v * SUB : (v + 1) * SUB, :], back)
        lower_ref[at, :] = jnp.transpose(jnp.concatenate(counts_below(x, 0), axis=0))
        if b * LANES >= skip:
            at = slice(b * LANES - skip, (b + 1) * LANES - skip)
            upper_ref[at, :] = jnp.transpose(jnp.concatenate(counts_below(x, LANES), axis=0))


def table_kernel(
    mine_ref, peer_ref, flow_ref,
    normal_ref, link_ref, order_ref, last_ref, lean_ref, coupling_ref,
    wide_ref, key_ref, beside_ref, joint_ref, flux_ref, sort_ref, lower_ref, upper_ref,
):
    tiles = normal_ref.shape[2]
    pairs = tiles // 2
    swapped = lax.axis_index("faces") == 1
    lane = lane_ids((pairs, LANES))
    half = LANES // 2
    for i in range(4):
        part = []
        for q in range(3):
            mine = mine_ref[i, q * pairs : (q + 1) * pairs, :]
            peer = peer_ref[i, q * pairs : (q + 1) * pairs, :]
            part.append((jnp.where(swapped, peer, mine), jnp.where(swapped, mine, peer)))
        (a0, b0), (a1, b1), (a2, b2) = part
        even = (a0, b0, jnp.where(lane < half, a1, pltpu.roll(b1, half, 1)))
        odd = (a2, b2, jnp.where(lane < half, pltpu.roll(a1, half, 1), b1))
        for r in range(3):
            target = normal_ref.at[i, r] if i < 3 else joint_ref.at[r]
            target[pl.ds(0, pairs, stride=2), :] = even[r]
            target[pl.ds(1, pairs, stride=2), :] = odd[r]
    lane = lane_ids()
    for r in range(3):
        for g in in_groups(tiles):
            joint = joint_ref[r, rows8(g), :].astype(I32)
            owner, code = joint >> 9, joint & 511
            link_ref[0, r, rows8(g), :] = owner
            link_ref[1, r, rows8(g), :] = code
            at = r * tiles + g * SUB
            key_ref[at : at + SUB, :] = (owner * LANES + lane).astype(F32)
            at += 3 * tiles
            key_ref[at : at + SUB, :] = (jnp.minimum(code, 256) * LANES + lane).astype(F32)
    sort_rows(key_ref, lower_ref, upper_ref)
    skip = lower_ref.shape[0] - upper_ref.shape[0]
    for r in range(3):
        for g in in_groups(tiles):
            at = r * tiles + g * SUB
            owned = key_ref[at : at + SUB, :]
            near = key_ref[at + 3 * tiles : at + 3 * tiles + SUB, :]
            order_ref[0, r, rows8(g), :] = owned.astype(I32) & (LANES - 1)
            order_ref[1, r, rows8(g), :] = near.astype(I32) & (LANES - 1)
            near = at + 3 * tiles
            for i, count in enumerate(
                (lower_ref[at : at + SUB, :], lower_ref[near : near + SUB, :], upper_ref[near - skip : near - skip + SUB, :])
            ):
                last_ref[i, r, rows8(g), :] = count.astype(I32) - 1
    for t in range(tiles):
        for c in range(3):
            wide_ref[c, t : t + 1, :] = flow_ref[c : c + 1, t * LANES : (t + 1) * LANES]
    widen(wide_ref, tiles, 3)
    for g in in_groups(tiles):
        for r in range(3):
            left, right = local_values(wide_ref, link_ref, g, r, 3)
            lean, size = zero(), zero()
            for i in range(3):
                normal = normal_ref[i, r, rows8(g), :]
                lean = lean + normal * (left[i] + right[i])
                size = size + normal * normal
                flux_ref[block_at((g * 3 + r) * 3 + i), :] = normal
            lean_ref[0, r, rows8(g), :] = lean
            lean_ref[1, r, rows8(g), :] = 2.0 * jnp.sqrt(size)
    to_cells(flux_ref, order_ref, last_ref, coupling_ref, beside_ref, sort_ref, (-1, -1, -1))
    for g in in_groups(tiles):
        for i in range(3):
            coupling_ref[i, rows8(g), :] = coupling_ref[i, rows8(g), :] - beside_ref[i, rows8(g), :]


def setup_kernel(
    in_ref, source_ref, volume_ref, normal_ref, link_ref, order_ref, last_ref, lean_ref, coupling_ref, send_ref,
    pair_ref, diag_ref, source_out, pre_ref, out_ref,
    stage_ref, halo_ref, here_ref, beside_ref, flux_ref, sort_ref, *, shifts,
):
    tiles = volume_ref.shape[0]
    lay_halo(got_halo(in_ref, shifts), halo_ref)
    for g in in_groups(tiles):
        for r in range(3):
            right = halo_values([zero() for _ in range(3)], halo_ref, link_ref, g, r, len(shifts))
            speed = lean_ref[0, r, rows8(g), :]
            for i in range(3):
                speed = speed + normal_ref[i, r, rows8(g), :] * right[i]
            wave = 0.5 * jnp.abs(speed) + lean_ref[1, r, rows8(g), :]
            for i, term in enumerate((0.5 * speed, wave)):
                pair_ref[i, r, rows8(g), :] = term
                flux_ref[block_at((g * 3 + r) * 2 + i), :] = term
    to_cells(flux_ref, order_ref, last_ref, here_ref, beside_ref, sort_ref, (-1, 1))
    for t in range(tiles):
        for c in range(BLOCK):
            source_out[c, t : t + 1, :] = source_ref[c : c + 1, t * LANES : (t + 1) * LANES]
    for g in in_groups(tiles):
        n0, n1, n2 = [coupling_ref[i, rows8(g), :] for i in range(3)]
        speed = here_ref[0, rows8(g), :] - beside_ref[0, rows8(g), :]
        pressure_diag = volume_ref[rows8(g), :] + (here_ref[1, rows8(g), :] + beside_ref[1, rows8(g), :])
        inverse = 1.0 / (pressure_diag + speed)
        schur = pressure_diag - (n0 * n0 + n1 * n1 + n2 * n2) * inverse
        for i, value in enumerate((inverse, n0, n1, n2, 1.0 / schur)):
            diag_ref[i, rows8(g), :] = value
        put(pre_ref, g, precondition(cell(source_out, g), diag_ref, g))
    send_halo(listed(tiled_rows(pre_ref), tiles, send_ref, len(shifts) // 2 * (SUB // BLOCK)), stage_ref, out_ref, len(shifts) // 2)


def combine(scales, vectors):
    out = []
    for parts in zip(*vectors):
        acc = None
        for scale, part in zip(scales, parts):
            term = part if scale is None else scale * part
            acc = term if acc is None else acc + term
        out.append(acc)
    return out


def first_kernel(
    in_ref, pre_ref, source_ref, volume_ref, normal_ref, pair_ref, link_ref, order_ref, last_ref, diag_ref, send_ref,
    image_ref, mimage_ref, out_ref,
    stage_ref, halo_ref, wide_ref, here_ref, beside_ref, flux_ref, sort_ref, *, shifts,
):
    tiles = volume_ref.shape[0]
    groups = in_groups(tiles)
    for g in groups:
        put(wide_ref, g, cell(pre_ref, g))
    widen(wide_ref, tiles)
    lay_halo(got_halo(in_ref, shifts), halo_ref)
    faces = (normal_ref, pair_ref, link_ref, order_ref, last_ref)
    face_part(wide_ref, halo_ref, faces, here_ref, beside_ref, flux_ref, sort_ref, len(shifts))
    product, rho = zero(), zero()
    for g in groups:
        image = applied(g, volume_ref, wide_ref, here_ref, beside_ref)
        source = cell(source_ref, g)
        product = added(product, source, image)
        rho = added(rho, source, source)
        put(image_ref, g, image)
        put(mimage_ref, g, precondition(image, diag_ref, g))
    send_sums((product, rho), out_ref)
    send_halo(listed(tiled_rows(mimage_ref), tiles, send_ref, len(shifts) // 2 * (SUB // BLOCK)), stage_ref, out_ref, len(shifts) // 2)


def second_kernel(
    in1_ref, in2_ref, pre_ref, mimage_ref, image_ref, source_ref,
    volume_ref, normal_ref, pair_ref, link_ref, order_ref, last_ref, diag_ref, send_ref,
    middle_ref, premid_ref, second_ref, msecond_ref, scale_ref, out_ref,
    stage_ref, halo_ref, wide_ref, here_ref, beside_ref, flux_ref, sort_ref, *, shifts,
):
    tiles = volume_ref.shape[0]
    groups = in_groups(tiles)
    sums = got_sums(in2_ref, len(shifts) // 2)
    rho = spread(sums, 1)
    alpha = rho / spread(sums, 0)
    scale_ref[0:1, :] = alpha[0:1, :]
    scale_ref[1:2, :] = rho[0:1, :]
    for g in groups:
        premid = combine((None, -alpha), (cell(pre_ref, g), cell(mimage_ref, g)))
        put(wide_ref, g, premid)
        put(premid_ref, g, premid)
    widen(wide_ref, tiles)
    lay_halo(combine((None, -alpha), (got_halo(in1_ref, shifts), got_halo(in2_ref, shifts))), halo_ref)
    faces = (normal_ref, pair_ref, link_ref, order_ref, last_ref)
    face_part(wide_ref, halo_ref, faces, here_ref, beside_ref, flux_ref, sort_ref, len(shifts))
    products = [zero() for _ in range(4)]
    for g in groups:
        second = applied(g, volume_ref, wide_ref, here_ref, beside_ref)
        source = cell(source_ref, g)
        middle = combine((None, -alpha), (source, cell(image_ref, g)))
        put(middle_ref, g, middle)
        put(second_ref, g, second)
        put(msecond_ref, g, precondition(second, diag_ref, g))
        for i, (a, b) in enumerate(((second, middle), (second, second), (source, middle), (source, second))):
            products[i] = added(products[i], a, b)
    send_sums(products, out_ref)
    send_halo(listed(tiled_rows(msecond_ref), tiles, send_ref, len(shifts) // 2 * (SUB // BLOCK)), stage_ref, out_ref, len(shifts) // 2)


def third_kernel(
    in1_ref, in2_ref, in3_ref, scale_ref, pre_ref, mimage_ref, premid_ref, msecond_ref, middle_ref, second_ref, source_ref,
    volume_ref, normal_ref, pair_ref, link_ref, order_ref, last_ref, diag_ref, send_ref,
    field_ref, residual_ref, preres_ref, predir_ref, image_ref, mimage_out, scale_out, ghost_ref, out_ref,
    stage_ref, halo_ref, wide_ref, here_ref, beside_ref, flux_ref, sort_ref, *, shifts,
):
    tiles = volume_ref.shape[0]
    groups = in_groups(tiles)
    sums = got_sums(in3_ref, len(shifts) // 2)
    alpha, rho = row_of(scale_ref, 0), row_of(scale_ref, 1)
    omega = spread(sums, 0) / spread(sums, 1)
    rho_next = spread(sums, 2) - omega * spread(sums, 3)
    beta = rho_next / rho * (alpha / omega)
    scale_out[0:1, :] = rho_next[0:1, :]
    drop = -beta * omega
    for g in groups:
        predir, mimage, premid = cell(pre_ref, g), cell(mimage_ref, g), cell(premid_ref, g)
        put(field_ref, g, combine((alpha, omega), (predir, premid)))
        put(residual_ref, g, combine((None, -omega), (cell(middle_ref, g), cell(second_ref, g))))
        preres = combine((None, -omega), (premid, cell(msecond_ref, g)))
        put(preres_ref, g, preres)
        predir = combine((None, beta, drop), (preres, predir, mimage))
        put(predir_ref, g, predir)
        put(wide_ref, g, predir)
    widen(wide_ref, tiles)
    ghost1, ghost2, ghost3 = [got_halo(ref, shifts) for ref in (in1_ref, in2_ref, in3_ref)]
    preres = combine((None, -alpha, -omega), (ghost1, ghost2, ghost3))
    for k in range(len(shifts)):
        ghost_ref[k] = preres[k]
    lay_halo(combine((None, beta, drop), (preres, ghost1, ghost2)), halo_ref)
    faces = (normal_ref, pair_ref, link_ref, order_ref, last_ref)
    face_part(wide_ref, halo_ref, faces, here_ref, beside_ref, flux_ref, sort_ref, len(shifts))
    product = zero()
    for g in groups:
        image = applied(g, volume_ref, wide_ref, here_ref, beside_ref)
        product = added(product, cell(source_ref, g), image)
        put(image_ref, g, image)
        put(mimage_out, g, precondition(image, diag_ref, g))
    send_sums((product,), out_ref)
    send_halo(listed(tiled_rows(mimage_out), tiles, send_ref, len(shifts) // 2 * (SUB // BLOCK)), stage_ref, out_ref, len(shifts) // 2)


def flatten(out_ref, ref, g):
    for t in range(g * SUB, g * SUB + SUB):
        for c in range(BLOCK):
            out_ref[c : c + 1, t * LANES : (t + 1) * LANES] = ref[c, t : t + 1, :]


def fourth_kernel(
    in4_ref, scale_ref, ghost_ref, field_ref, residual_ref, preres_ref, predir_ref, image_ref, mimage_ref,
    volume_ref, normal_ref, pair_ref, link_ref, order_ref, last_ref,
    field_flat, premid_flat, middle_flat, second_flat, out_ref,
    stage_ref, halo_ref, wide_ref, here_ref, beside_ref, flux_ref, sort_ref, *, shifts,
):
    tiles = volume_ref.shape[0]
    field_out, premid_ref, middle_ref, second_ref = [stage_ref.at[i] for i in range(4)]
    groups = in_groups(tiles)
    alpha = row_of(scale_ref, 0) / spread(got_sums(in4_ref, len(shifts) // 2), 0)
    for g in groups:
        premid = combine((None, -alpha), (cell(preres_ref, g), cell(mimage_ref, g)))
        put(wide_ref, g, premid)
        put(premid_ref, g, premid)
        put(field_out, g, combine((None, alpha), (cell(field_ref, g), cell(predir_ref, g))))
        put(middle_ref, g, combine((None, -alpha), (cell(residual_ref, g), cell(image_ref, g))))
        flatten(field_flat, field_out, g)
        flatten(premid_flat, premid_ref, g)
        flatten(middle_flat, middle_ref, g)
    widen(wide_ref, tiles)
    ghosts = [ghost_ref[k] for k in range(len(shifts))]
    lay_halo(combine((None, -alpha), (ghosts, got_halo(in4_ref, shifts))), halo_ref)
    faces = (normal_ref, pair_ref, link_ref, order_ref, last_ref)
    face_part(wide_ref, halo_ref, faces, here_ref, beside_ref, flux_ref, sort_ref, len(shifts))
    cross, square = zero(), zero()
    for g in groups:
        second = applied(g, volume_ref, wide_ref, here_ref, beside_ref)
        put(second_ref, g, second)
        flatten(second_flat, second_ref, g)
        cross = added(cross, second, cell(middle_ref, g))
        square = added(square, second, second)
    send_sums((cross, square), out_ref)


def last_kernel(in_ref, field_ref, premid_ref, middle_ref, second_ref, field_out, residual_out):
    sums = total_of([in_ref[d] for d in range(0, in_ref.shape[0], lax.axis_size("faces"))])
    omega = sums[0:1, :] / sums[1:2, :]
    field_out[...] = field_ref[...] + omega * premid_ref[...]
    residual_out[...] = middle_ref[...] - omega * second_ref[...]


def run(kernel, outs, scratch, args, scalars=0, away=0):
    vmem = pl.BlockSpec(memory_space=pltpu.VMEM)
    smem = pl.BlockSpec(memory_space=pltpu.SMEM)
    hbm = pl.BlockSpec(memory_space=pltpu.HBM)
    far = range(scalars, scalars + away)
    args = [pltpu.with_memory_space_constraint(a, pltpu.HBM) if i in far else a for i, a in enumerate(args)]
    return pl.pallas_call(
        kernel,
        out_shape=[jax.ShapeDtypeStruct(shape, dtype) for shape, dtype in outs],
        in_specs=[smem] * scalars + [hbm] * away + [vmem] * (len(args) - scalars - away),
        out_specs=[vmem] * len(outs),
        scratch_shapes=[pltpu.VMEM(shape, F32) if isinstance(shape, tuple) else shape for shape in scratch],
        compiler_params=pltpu.CompilerParams(vmem_limit_bytes=24 << 20),
    )(*args)


def exchange(block):
    return lax.all_to_all(block, ("cells", "faces"), 0, 0)


def body(
    flow_state,
    source_term,
    volume_rate,
    face_normal,
    face_owner,
    face_neighbour,
    face_count,
    send_list,
    halo_count,
):
    count = lax.axis_size("cells")
    cells_here = flow_state.shape[1]
    lists, width = send_list.shape
    tiles = cells_here // LANES
    per_tile = face_owner.shape[0] // tiles
    shifts = offsets(lists // 2)
    assert per_tile * 2 == 3 * LANES and lax.axis_size("faces") == 2
    assert width == 2 * LANES and count > lists and lists % 2 == 0 and lists <= SUB
    assert tiles % SUB == 0 and cells_here & (cells_here - 1) == 0
    rows = 3
    span = -(-(lists + SUB - 1) // SUB) * SUB
    vector = (BLOCK, tiles, LANES)
    vec = (vector, F32)
    faces = (rows, tiles, LANES)
    scale = ((SUB, LANES), F32)
    full_block = ((2 * count, SUB, LANES), F32)
    flat_vec = (flow_state.shape, F32)
    stage = (SUB * SUB, LANES)
    halo = (SUB * span, LANES)
    flat = face_owner.shape[0] // LANES
    volume = volume_rate.reshape(tiles, LANES)

    def wide(parts):
        return (parts, tiles + SUB, LANES)

    def blocks(parts):
        return (rows * parts * tiles, LANES)

    ints = pltpu.VMEM((flat, LANES), I32)
    packed = -(-BLOCK * (lists // 2) * (width // LANES) // SUB)
    pack, out0, send, flow, source = run(
        start_kernel,
        [((4, flat, LANES), F32), full_block, ((2 * packed, SUB, LANES), I32), flat_vec, flat_vec],
        [
            stage, pltpu.VMEM(send_list.shape, I32), pltpu.SMEM((lists,), I32),
            face_normal.shape, ints, ints, pltpu.SemaphoreType.DMA((7,)),
        ],
        (
            face_count, halo_count, flow_state, send_list, face_normal,
            face_owner.reshape(flat, LANES), face_neighbour.reshape(flat, LANES), source_term,
        ),
        scalars=1,
        away=7,
    )
    in0 = exchange(out0)
    peer = lax.ppermute(pack, "faces", [(0, 1), (1, 0)])
    normal, link, order, last, lean, coupling = run(
        table_kernel,
        [
            ((3,) + faces, F32), ((2,) + faces, I32), ((2,) + faces, I32), ((3,) + faces, I32),
            ((2,) + faces, F32), ((3, tiles, LANES), F32),
        ],
        [
            wide(3), (6 * tiles, LANES), wide(3), faces,
            blocks(3), blocks(6), (6 * tiles, LANES), (4 * tiles, LANES),
        ],
        (pack, peer, flow),
    )
    pair, diag, source, predir, out1 = run(
        functools.partial(setup_kernel, shifts=shifts),
        [((2,) + faces, F32), ((5, tiles, LANES), F32), vec, vec, full_block],
        [stage, halo, (2, tiles, LANES), wide(2), blocks(2), blocks(4)],
        (in0, source, volume, normal, link, order, last, lean, coupling, send),
    )
    in1 = exchange(out1)
    work = [stage, halo, wide(BLOCK), vector, wide(BLOCK), blocks(BLOCK), blocks(2 * BLOCK)]
    fixed = (volume, normal, pair, link, order, last, diag, send)
    image, mimage, out2 = run(
        functools.partial(first_kernel, shifts=shifts), [vec, vec, full_block], work, (in1, predir, source) + fixed
    )
    in2 = exchange(out2)
    middle, premid, second, msecond, scales, out3 = run(
        functools.partial(second_kernel, shifts=shifts),
        [vec, vec, vec, vec, scale, full_block],
        work,
        (in1, in2, predir, mimage, image, source) + fixed,
    )
    in3 = exchange(out3)
    field, residual, preres, predir, image, mimage, scales, ghosts, out4 = run(
        functools.partial(third_kernel, shifts=shifts),
        [vec, vec, vec, vec, vec, vec, scale, ((lists, SUB, LANES), F32), full_block],
        work,
        (in1, in2, in3, scales, predir, mimage, premid, msecond, middle, second, source) + fixed,
    )
    in4 = exchange(out4)
    field, premid, middle, second, out5 = run(
        functools.partial(fourth_kernel, shifts=shifts),
        [flat_vec] * 4 + [full_block],
        [(4,) + vector] + work[1:],
        (in4, scales, ghosts, field, residual, preres, predir, image, mimage) + fixed[:6],
    )
    in5 = exchange(out5)
    field, residual = run(last_kernel, [flat_vec, flat_vec], [], (in5, field, premid, middle, second))
    return (field, residual)


def solution(mesh):
    in_specs = (
        P(None, "cells"),
        P(None, "cells"),
        P("cells"),
        P(None, ("cells", "faces")),
        P(("cells", "faces")),
        P(("cells", "faces")),
        P(("cells", "faces")),
        P("cells", None),
        P("cells"),
    )
    out_specs = (P(None, "cells"), P(None, "cells"))
    return jax.shard_map(body, mesh=mesh, in_specs=in_specs, out_specs=out_specs, check_vma=False)
```
